8 devices in a mesh: member: 1 (over z), ty: 2 (over y), tx: 2 (over x), panel: 2 (over core).
Axes of the slice: x: 2, y: 2, z: 1, core: 2. Of those that a mesh axis runs over, the one named last changes fastest.
Arguments:
- tracer: float32 [6, 180, 180], P(('member', 'panel'), 'tx', 'ty')
- wind_a: float32 [6, 180, 180], P('panel', 'tx', 'ty')
- wind_b: float32 [6, 180, 180], P('panel', 'tx', 'ty')
- wind_scale: float32 [256], replicated
Outputs:
- output: float32 [6, 180, 180], P(('member', 'panel'), 'tx', 'ty')
All inputs are finite; a program needn't handle non-finite values.
Results may differ from the reference program's by a relative error of at most 0.001.
Values sent between devices are 32-bit elements.
A program may use at most 1 GiB of HBM per device.

```python
import math
import jax
import jax.numpy as jnp
from jax import lax

N = 180
STEPS = 256

C_SPEED = 2.5
CFL_STEP = 0.12
DALPHA = 0.5 * math.pi / N
DT = CFL_STEP * DALPHA
EDGE_TABLE = (
    ((3, 1, 0), (1, 0, 0), (5, 3, 0), (4, 2, 0)),
    ((0, 1, 0), (2, 0, 0), (5, 1, 1), (4, 1, 0)),
    ((1, 1, 0), (3, 0, 0), (5, 2, 1), (4, 3, 1)),
    ((2, 1, 0), (0, 0, 0), (5, 0, 0), (4, 0, 1)),
    ((3, 3, 1), (1, 3, 0), (0, 3, 0), (2, 3, 1)),
    ((3, 2, 0), (1, 2, 1), (2, 2, 1), (0, 2, 0)),
)
TANGENT_A = ((0.0, 1.0, 0.0), (-1.0, 0.0, 0.0), (0.0, -1.0, 0.0), (1.0, 0.0, 0.0), (0.0, 1.0, 0.0), (0.0, 1.0, 0.0))
TANGENT_B = ((0.0, 0.0, 1.0), (0.0, 0.0, 1.0), (0.0, 0.0, 1.0), (0.0, 0.0, 1.0), (-1.0, 0.0, 0.0), (1.0, 0.0, 0.0))


def edge_sign(side_id, edge_id):
    out_sign = 1.0 if edge_id in (1, 3) else -1.0
    return out_sign if side_id in (0, 2) else -out_sign


def out_strips(field_a, field_b):
    return (field_a[:, 0:2, :],
            jnp.flip(field_a[:, -2:, :], axis=1),
            jnp.swapaxes(field_b[:, :, 0:2], 1, 2),
            jnp.swapaxes(jnp.flip(field_b[:, :, -2:], axis=2), 1, 2))


def to_blocks(ghosts):
    return (jnp.flip(ghosts[0], axis=1), ghosts[1],
            jnp.swapaxes(jnp.flip(ghosts[2], axis=1), 1, 2), jnp.swapaxes(ghosts[3], 1, 2))


def sphere_blocks(field_a, field_b, signed):
    strips = out_strips(field_a, field_b)
    ghosts = []
    for side_id in range(4):
        per_panel = []
        for panel_id in range(6):
            src_panel, edge_id, flipped = EDGE_TABLE[panel_id][side_id]
            one_strip = strips[edge_id][src_panel]
            if flipped:
                one_strip = jnp.flip(one_strip, axis=1)
            if signed:
                one_strip = edge_sign(side_id, edge_id) * one_strip
            per_panel.append(one_strip)
        ghosts.append(jnp.stack(per_panel))
    return to_blocks(ghosts)


def extend_field(field_now, blocks):
    return (jnp.concatenate([blocks[0], field_now, blocks[1]], axis=1),
            jnp.concatenate([blocks[2], field_now, blocks[3]], axis=2))


def wind_faces(blocks, wind_a, wind_b):
    ext_a = jnp.concatenate([blocks[0][:, 1:2, :], wind_a, blocks[1][:, 0:1, :]], axis=1)
    ext_b = jnp.concatenate([blocks[2][:, :, 1:2], wind_b, blocks[3][:, :, 0:1]], axis=2)
    return 0.5 * (ext_a[:, :-1, :] + ext_a[:, 1:, :]), 0.5 * (ext_b[:, :, :-1] + ext_b[:, :, 1:])


def face_flux_div(ext_arr, wind_face, step_scale, axis_id):
    face_count = ext_arr.shape[axis_id] - 3
    far_left = lax.slice_in_dim(ext_arr, 0, face_count, axis=axis_id)
    near_left = lax.slice_in_dim(ext_arr, 1, face_count + 1, axis=axis_id)
    near_right = lax.slice_in_dim(ext_arr, 2, face_count + 2, axis=axis_id)
    far_right = lax.slice_in_dim(ext_arr, 3, face_count + 3, axis=axis_id)
    face_val = (7.0 * (near_left + near_right) - (far_left + far_right)) / 12.0
    face_flux = step_scale * wind_face * face_val - (0.5 * C_SPEED) * (near_right - near_left)
    return (lax.slice_in_dim(face_flux, 1, face_count, axis=axis_id)
            - lax.slice_in_dim(face_flux, 0, face_count - 1, axis=axis_id))


def tendency(ext_a, ext_b, face_a, face_b, step_scale, inv_area):
    div_total = face_flux_div(ext_a, face_a, step_scale, 1) + face_flux_div(ext_b, face_b, step_scale, 2)
    return -div_total * inv_area


def inverse_area(row_ids, col_ids, cells):
    dalpha = 0.5 * math.pi / cells
    tan_a = jnp.tan((row_ids.astype(jnp.float32) + 0.5) * dalpha - 0.25 * math.pi)[:, None]
    tan_b = jnp.tan((col_ids.astype(jnp.float32) + 0.5) * dalpha - 0.25 * math.pi)[None, :]
    r_sq = 1.0 + tan_a * tan_a + tan_b * tan_b
    sqrt_g = (1.0 + tan_a * tan_a) * (1.0 + tan_b * tan_b) / (r_sq * jnp.sqrt(r_sq))
    return 1.0 / (dalpha * sqrt_g)


def sphere_points():
    centre_tan = jnp.tan((jnp.arange(N, dtype=jnp.float32) + 0.5) * DALPHA - 0.25 * math.pi)
    tan_a = jnp.broadcast_to(centre_tan[:, None], (N, N))
    tan_b = jnp.broadcast_to(centre_tan[None, :], (N, N))
    ones_grid = jnp.ones((N, N), jnp.float32)
    comp_x = jnp.stack([ones_grid, -tan_a, -ones_grid, tan_a, -tan_b, tan_b])
    comp_y = jnp.stack([tan_a, ones_grid, -tan_a, -ones_grid, tan_a, tan_a])
    comp_z = jnp.stack([tan_b, tan_b, tan_b, tan_b, ones_grid, -ones_grid])
    cube_pts = jnp.stack([comp_x, comp_y, comp_z], axis=-1)
    return tan_a, tan_b, cube_pts / jnp.linalg.norm(cube_pts, axis=-1, keepdims=True)


def flux_winds(tan_a, tan_b, velocity):
    along_a = jnp.sum(velocity * jnp.array(TANGENT_A, jnp.float32)[:, None, None, :], axis=-1)
    along_b = jnp.sum(velocity * jnp.array(TANGENT_B, jnp.float32)[:, None, None, :], axis=-1)
    sq_a = tan_a * tan_a
    sq_b = tan_b * tan_b
    r_sq = 1.0 + sq_a + sq_b
    cross_ab = tan_a * tan_b
    wind_a = (1.0 + sq_b) * ((1.0 + sq_a) * along_a + cross_ab * along_b) / r_sq
    wind_b = (1.0 + sq_a) * (cross_ab * along_a + (1.0 + sq_b) * along_b) / r_sq
    return wind_a, wind_b


def random_unit(key_vec):
    raw_vec = jax.random.normal(key_vec, (3,), jnp.float32)
    return raw_vec / jnp.linalg.norm(raw_vec)


def setup_inputs(seed: int = 0, part: int = 0) -> dict:
    base_key = jax.random.key(seed)
    shared_key, part_key = jax.random.split(base_key)
    part_key = jax.random.fold_in(part_key, part)
    tan_a, tan_b, sphere_pts = sphere_points()
    key_axis, key_rate, key_scale = jax.random.split(shared_key, 3)
    rot_axis = random_unit(key_axis) * jax.random.uniform(key_rate, (), jnp.float32, 0.6, 1.0)
    velocity = jnp.cross(rot_axis, sphere_pts)
    wind_a, wind_b = flux_winds(tan_a, tan_b, velocity)
    wind_scale = jax.random.uniform(key_scale, (STEPS,), jnp.float32, -0.2, 1.0)
    key_front, key_wave, key_phase = jax.random.split(part_key, 3)
    front_part = jnp.tanh((N / 12.0) * (sphere_pts @ random_unit(key_front)))
    wave_phase = jax.random.uniform(key_phase, (), jnp.float32, 0.0, 2.0 * math.pi)
    wave_part = jnp.sin((N / 6.0) * (sphere_pts @ random_unit(key_wave)) + wave_phase)
    tracer = 0.8 * front_part + 0.5 * wave_part
    return {'tracer': tracer.astype(jnp.float32), 'wind_a': wind_a.astype(jnp.float32),
            'wind_b': wind_b.astype(jnp.float32), 'wind_scale': wind_scale}


def reference(tracer, wind_a, wind_b, wind_scale):
    cell_ids = jnp.arange(N)
    inv_area = inverse_area(cell_ids, cell_ids, N)
    face_a, face_b = wind_faces(sphere_blocks(wind_a, wind_b, True), wind_a, wind_b)

    def tend_of(tracer_now, step_scale):
        ext_a, ext_b = extend_field(tracer_now, sphere_blocks(tracer_now, tracer_now, False))
        return tendency(ext_a, ext_b, face_a, face_b, step_scale, inv_area)

    def one_step(tracer_now, step_scale):
        stage_one = tracer_now + DT * tend_of(tracer_now, step_scale)
        stage_two = stage_one + DT * tend_of(stage_one, step_scale)
        return 0.5 * (tracer_now + stage_two), None

    return lax.scan(one_step, tracer, wind_scale)[0]
```

```python
import functools
import math

import jax
import jax.numpy as jnp
import numpy as np
from jax import lax
from jax.experimental import pallas as pl
from jax.experimental.pallas import tpu as pltpu
from jax.sharding import PartitionSpec as P

C_SPEED = 2.5
CFL_STEP = 0.12
MESH = pl.DeviceIdType.MESH
HIGHEST = lax.Precision.HIGHEST

TWIN = (1, 0, 3, 2, 5, 4)
ACROSS = (2, 4, 0, 5, 1, 3)
PRIMARY = (0, 2, 4)

SIZE = 128
TILES = 16
LOW = 6
OWN = 90
BLOCK_STEPS = 8


def pos_idx(pos):
    return TILES * (pos % 8) + pos // 8


def tiles_of(arr):
    return [arr[8 * i:8 * i + 8] for i in range(TILES)]


def join(tiles):
    return jnp.concatenate(tiles, axis=0)


def roll_rows(tile, shift):
    return pltpu.roll(tile, shift % 8, 0)


def solution(mesh):
    axis_names = mesh.axis_names

    def local_run(tracer, wind_a, wind_b, wind_scale):
        own = tracer.shape[1]
        cells = 2 * own
        steps = wind_scale.shape[0]
        dalpha = 0.5 * math.pi / cells
        tan_u = np.tan((pos_idx(np.arange(SIZE)) - LOW + 0.5) * dalpha - 0.25 * math.pi)
        tan_a, tan_b = tan_u[:, None], tan_u[None, :]
        r_sq = 1.0 + tan_a * tan_a + tan_b * tan_b
        inv_sqrt_g = r_sq * np.sqrt(r_sq) / ((1.0 + tan_a * tan_a) * (1.0 + tan_b * tan_b))
        gain = (0.5 * C_SPEED * CFL_STEP * inv_sqrt_g).astype(np.float32)
        out = pl.pallas_call(
            functools.partial(kernel, own, steps, axis_names),
            out_shape=jax.ShapeDtypeStruct(tracer.shape, jnp.float32),
            in_specs=[pl.BlockSpec(memory_space=pltpu.SMEM)] + [pl.BlockSpec(memory_space=pltpu.VMEM)] * 4,
            out_specs=pl.BlockSpec(memory_space=pltpu.VMEM),
            scratch_shapes=[
                pltpu.VMEM((6, SIZE, SIZE), jnp.float32),
                pltpu.VMEM((6, SIZE, SIZE), jnp.float32),
                pltpu.VMEM((6, SIZE, SIZE), jnp.float32),
                pltpu.VMEM((6, SIZE, SIZE), jnp.float32),
                pltpu.VMEM((SIZE, SIZE), jnp.float32),
                pltpu.VMEM((3, 3, own, own), jnp.float32),
                pltpu.VMEM((3, own, own), jnp.float32),
                pltpu.VMEM((6, 32, SIZE), jnp.float32),
                pltpu.VMEM((2, 6, 32, SIZE), jnp.float32),
                pltpu.VMEM((3, 8, SIZE), jnp.float32),
                pltpu.VMEM((2, 3, 8, SIZE), jnp.float32),
                pltpu.SemaphoreType.DMA((2, 9)),
                pltpu.SemaphoreType.DMA((2, 9)),
                pltpu.SemaphoreType.DMA((3, 3)),
                pltpu.SemaphoreType.DMA((3, 3)),
                pltpu.SemaphoreType.DMA((3,)),
                pltpu.SemaphoreType.DMA((3,)),
            ],
            name="advect",
        )(wind_scale, tracer, wind_a, wind_b, gain)
        return out

    field_spec = P(('member', 'panel'), 'tx', 'ty')
    wind_spec = P('panel', 'tx', 'ty')
    return jax.shard_map(local_run, mesh=mesh, in_specs=(field_spec, wind_spec, wind_spec, P()),
                         out_specs=field_spec, check_vma=False)


def kernel(own, steps, axis_names, ws_ref, q_in, wa_in, wb_in, gain_ref, out_ref,
           qa, qb, wl, wf, keep, tiles, result, send, recv, csend, crecv,
           ssem, rsem, tsend, trecv, osend, orecv):
    tx, ty, core = lax.axis_index('tx'), lax.axis_index('ty'), lax.axis_index('panel')

    def at(bx, by, bz):
        place = {'tx': bx, 'ty': by, 'panel': lax.rem(bz + bx, 2)}
        return {name: place.get(name, 0) for name in axis_names}

    bx, by, bz = tx, ty, lax.rem(core + tx, 2)
    is_first = core == 0

    def pick(first, second):
        return jnp.where(is_first, first, second)

    homes = (
        (pick(1, tx), pick(tx, 0), ty, pick(0, 1)),
        (pick(1 - tx, 1 - ty), pick(1, tx), pick(ty, 1), pick(1, 2)),
        (pick(0, ty), pick(1 - tx, tx), pick(ty, 0), pick(0, 2)),
    )
    fields = (q_in, wa_in, wb_in)
    for slot in range(3):
        ox, oy, oz, quad = homes[slot]
        mine = (ox == bx) & (oy == by) & (oz == bz)

        @pl.when(mine)
        def _():
            for f in range(3):
                tiles[f, quad] = fields[f][slot]

        @pl.when(jnp.logical_not(mine))
        def _():
            for f in range(3):
                pltpu.make_async_remote_copy(
                    fields[f].at[slot], tiles.at[f, quad], tsend.at[f, slot], trecv.at[f, quad],
                    device_id=at(ox, oy, oz), device_id_type=MESH).start()

    def owner(kx, ky, kc):
        return {name: {'tx': kx, 'ty': ky, 'panel': kc}.get(name, 0) for name in axis_names}

    flip_a = (1 - lax.rem(bx + by, 2), lax.rem(bx + by, 2), by)
    flip_b = (bz, bz, jnp.where(bz == 1, 1 - bx, bx))
    panel = (jnp.where(bx == 1, 0, 2), jnp.where(by == 1, 1, 3), jnp.where(bz == 1, 4, 5))
    for slot in range(3):
        ox, oy, oz, quad = homes[slot]
        mine = (ox == bx) & (oy == by) & (oz == bz)

        @pl.when(jnp.logical_not(mine))
        def _():
            for f in range(3):
                pltpu.make_async_remote_copy(
                    fields[f].at[slot], tiles.at[f, quad], tsend.at[f, slot], trecv.at[f, quad],
                    device_id=at(ox, oy, oz), device_id_type=MESH).wait_send()
    for quad in range(3):
        from_core = panel[quad] // 3
        stays = (flip_a[quad] == tx) & (flip_b[quad] == ty) & (from_core == core)

        @pl.when(jnp.logical_not(stays))
        def _():
            for f in range(3):
                pltpu.make_async_remote_copy(
                    fields[f].at[0], tiles.at[f, quad], tsend.at[f, 0], trecv.at[f, quad],
                    device_id=owner(flip_a[quad], flip_b[quad], from_core), device_id_type=MESH).wait_recv()

    pos_r = lax.broadcasted_iota(jnp.int32, (SIZE, own), 0)
    cell_c = lax.broadcasted_iota(jnp.int32, (SIZE, own), 1)
    cell_r = lax.broadcasted_iota(jnp.int32, (own, SIZE), 0)
    pos_c = lax.broadcasted_iota(jnp.int32, (own, SIZE), 1)

    def spot(pos, flip):
        dist = TILES * lax.rem(pos, 8) + pos // 8 - LOW
        inside = (dist >= 0) & (dist < own)
        return jnp.where(inside, jnp.where(flip == 1, own - 1 - dist, dist), -1)

    def place_rows(flip):
        return jnp.where(spot(pos_r, flip) == cell_c, 1.0, 0.0)

    def place_cols(flip):
        return jnp.where(spot(pos_c, flip) == cell_r, 1.0, 0.0)

    def dot(lhs, rhs):
        return jnp.dot(lhs, rhs, precision=HIGHEST, preferred_element_type=jnp.float32)

    for quad in range(3):
        rows, cols = place_rows(flip_a[quad]), place_cols(flip_b[quad])
        plain = (0, 2, 5)[quad]
        turned = TWIN[plain]
        sign_a = jnp.where(flip_a[quad] == 1, -1.0, 1.0)
        sign_b = jnp.where(flip_b[quad] == 1, -1.0, 1.0)
        q_loc = dot(dot(rows, tiles[0, quad]), cols)
        a_loc = sign_a * dot(dot(rows, tiles[1, quad]), cols)
        b_loc = sign_b * dot(dot(rows, tiles[2, quad]), cols)
        qa[plain] = q_loc
        qa[turned] = q_loc.T
        qb[plain] = a_loc
        qb[turned] = b_loc.T
        wl[plain] = b_loc
        wl[turned] = a_loc.T

    sub = lax.broadcasted_iota(jnp.int32, (8, SIZE), 0)
    lane = lax.broadcasted_iota(jnp.int32, (8, SIZE), 1)
    halo_rows = sub >= 6
    halo_lanes = lax.rem(lane, 8) >= 6
    first_row = sub == 0

    def take(tile, idx, axis):
        return jnp.take_along_axis(tile, idx, axis=axis, mode="promise_in_bounds")

    sides = ((0, 0, 1), (1, 0, 0), (0, 1, 0), (1, 0, 1), (0, 1, 1), (1, 1, 0))
    strip_axis = (1, 2, 0, 2, 0, 1)
    place_in = (2, 4, 0, 5, 1, 3)
    axis_first = (0, 2, 4)
    axis_flip = ((1, 0, 0), (0, 1, 0), (0, 0, 1))
    corner_flip = {0: (0, 1, 1), 2: (1, 0, 1), 4: (1, 1, 0)}

    def peer(flip):
        return at(*(1 - b if f else b for b, f in zip((bx, by, bz), flip)))

    def copies(slot):
        made = []
        for axis in (1, 0, 2):
            first = axis_first[axis]
            made.append(pltpu.make_async_remote_copy(
                send.at[pl.ds(first, 2)], recv.at[slot, pl.ds(first, 2)], ssem.at[slot, axis], rsem.at[slot, axis],
                device_id=peer(axis_flip[axis]), device_id_type=MESH))
        for n, arr in enumerate(PRIMARY):
            made.append(pltpu.make_async_remote_copy(
                csend.at[n], crecv.at[slot, n], ssem.at[slot, 3 + n], rsem.at[slot, 3 + n],
                device_id=peer(corner_flip[arr]), device_id_type=MESH))
        return made

    row_perm = 5 - lax.rem(sub, 2)
    lane_perm = 125 - 8 * (lane // 8) - lax.rem(lane, 2)
    row_pair = sub // 2
    lane_pair = lax.rem(lane, 8) // 2

    def by_pair(pair, parts):
        res = parts[3]
        for m in (2, 1, 0):
            res = jnp.where(pair == m, parts[m], res)
        return res

    def exchange(arrs, twins, slot, row_sign, corner_sign):
        for k in range(6):
            a = tiles_of(arrs[k])
            msg = [by_pair(row_pair, [take(a[15 - 4 * j - m], row_perm, 0) for m in range(4)]) for j in range(4)]
            send[place_in[k]] = row_sign * jnp.concatenate(msg, axis=0)
            if k in PRIMARY:
                csend[PRIMARY.index(k)] = corner_sign * by_pair(lane_pair, [take(t, lane_perm, 1) for t in msg])
        made = copies(slot)
        for c in made:
            c.start()
        for c in made:
            c.wait()
        for k in range(6):
            a = tiles_of(arrs[k])
            msg = tiles_of_strip(recv[slot, place_in[k]])
            if k in PRIMARY:
                corner = crecv[slot, PRIMARY.index(k)]
                msg = [jnp.where(halo_lanes, pltpu.roll(corner, (6 - 2 * j) % 128, 1), msg[j]) for j in range(4)]
            arrs[k] = join([jnp.where(halo_rows, roll_rows(msg[i // 4], 6 - 2 * (i % 4)), a[i]) for i in range(TILES)])

    def tiles_of_strip(arr):
        return [arr[8 * j:8 * j + 8] for j in range(4)]

    own_rows_halo_lanes = halo_lanes & jnp.logical_not(halo_rows)

    def fill_lanes(arrs, twins):
        for k in PRIMARY:
            t = TWIN[k]
            from_twin = tiles_of(twins[t].T)
            from_self = tiles_of(twins[k].T) if twins is not arrs else tiles_of(arrs[k].T)
            mine, other = tiles_of(arrs[k]), tiles_of(arrs[t])
            new_mine = join([jnp.where(own_rows_halo_lanes, from_twin[i], mine[i]) for i in range(TILES)])
            new_other = join([jnp.where(halo_lanes, from_self[i], other[i]) for i in range(TILES)])
            arrs[k] = new_mine
            arrs[t] = new_other

    def set_ghosts(arrs, new):
        for k in range(6):
            near = new[ACROSS[k]]
            arrs[k, 32:33] = near[56:57]
            arrs[k, 40:41] = near[48:49]

    exchange(qb, wl, 0, -1.0, -1.0)
    exchange(wl, qb, 1, 1.0, -1.0)
    for k in PRIMARY:
        t = TWIN[k]
        lane_k, lane_t = tiles_of(wl[t].T), tiles_of(wl[k].T)
        mine, other = tiles_of(qb[k]), tiles_of(qb[t])
        qb[k] = join([jnp.where(own_rows_halo_lanes, lane_k[i], mine[i]) for i in range(TILES)])
        qb[t] = join([jnp.where(halo_lanes, lane_t[i], other[i]) for i in range(TILES)])
    for k in range(6):
        qb[k, 40:41] = -qb[ACROSS[k], 48:49]
    for k in range(6):
        a = tiles_of(qb[k])
        nxt = a[1:] + [roll_rows(a[0], -1)]
        wf[k] = (0.5 / (6.0 * C_SPEED)) * (qb[k] + join(nxt))
    keep[...] = 1.0 - 4.0 * gain_ref[...]

    def x_part(a_ref, k, faces):
        a = a_ref[k]
        before = jnp.concatenate([a_ref[k, 119:127], a[:120]], axis=0)
        after = jnp.concatenate([a[8:], a_ref[k, 1:9]], axis=0)
        m = before + after
        v = 8.0 * a - m
        v_after = jnp.concatenate([v[8:], roll_rows(v[:8], -1)], axis=0)
        flux = faces * (v + v_after)
        flux_before = jnp.concatenate([roll_rows(flux[120:], 1), flux[:120]], axis=0)
        return (m - flux) + flux_before

    def stage(src, dst, second, scale):
        gain = gain_ref[...]
        ready = []
        for k in PRIMARY:
            t = TWIN[k]
            parts = []
            for j in (k, t):
                if second:
                    faces = wl[j]
                else:
                    faces = scale * wf[j]
                    wl[j] = faces
                x = x_part(src, j, faces)
                if second:
                    x = (0.5 * gain) * x
                else:
                    x = gain * x
                if j == k:
                    if second:
                        x = (0.5 * dst[k] + (0.5 * keep[...]) * src[k]) + x
                    else:
                        x = keep[...] * src[k] + x
                parts.append(x)
            ready.append(parts)
        new = [None] * 6
        for k, (zk, zt) in zip(PRIMARY, ready):
            new[k] = zk + zt.T
            new[TWIN[k]] = zt + zk.T
        for k in range(6):
            dst[k] = new[k]
        set_ghosts(dst, new)

    block_count = steps // BLOCK_STEPS

    def block(blk, carry):
        slot = lax.rem(blk, 2)
        exchange(qa, qa, slot, 1.0, 1.0)
        fill_lanes(qa, qa)
        for k in range(6):
            near = ACROSS[k]
            qa[k, 32:33] = qa[near, 56:57]
            qa[k, 40:41] = qa[near, 48:49]

        def one_step(step, inner):
            scale = ws_ref[blk * BLOCK_STEPS + step]
            stage(qa, qb, False, scale)
            stage(qb, qa, True, scale)
            return inner

        lax.fori_loop(0, BLOCK_STEPS, one_step, 0)
        return carry

    lax.fori_loop(0, block_count, block, 0)

    for quad in range(3):
        plain = (0, 2, 5)[quad]
        rows, cols = place_cols(flip_a[quad]), place_rows(flip_b[quad])
        result[quad] = dot(dot(rows, qa[plain]), cols)
    for quad in range(3):
        from_core, from_slot = panel[quad] // 3, lax.rem(panel[quad], 3)
        stays = (flip_a[quad] == tx) & (flip_b[quad] == ty) & (from_core == core)

        @pl.when(stays)
        def _():
            out_ref[from_slot] = result[quad]

        @pl.when(jnp.logical_not(stays))
        def _():
            pltpu.make_async_remote_copy(
                result.at[quad], out_ref.at[from_slot], osend.at[quad], orecv.at[from_slot],
                device_id=owner(flip_a[quad], flip_b[quad], from_core), device_id_type=MESH).start()
    for quad in range(3):
        from_core, from_slot = panel[quad] // 3, lax.rem(panel[quad], 3)
        stays = (flip_a[quad] == tx) & (flip_b[quad] == ty) & (from_core == core)

        @pl.when(jnp.logical_not(stays))
        def _():
            pltpu.make_async_remote_copy(
                result.at[quad], out_ref.at[from_slot], osend.at[quad], orecv.at[from_slot],
                device_id=owner(flip_a[quad], flip_b[quad], from_core), device_id_type=MESH).wait_send()
    for slot in range(3):
        ox, oy, oz, quad = homes[slot]
        mine = (ox == bx) & (oy == by) & (oz == bz)

        @pl.when(jnp.logical_not(mine))
        def _():
            pltpu.make_async_remote_copy(
                result.at[0], out_ref.at[slot], osend.at[0], orecv.at[slot],
                device_id=at(ox, oy, oz), device_id_type=MESH).wait_recv()
```

```python
import functools
import math

import jax
import jax.numpy as jnp
import numpy as np
from jax import lax
from jax.experimental import pallas as pl
from jax.experimental.pallas import tpu as pltpu
from jax.sharding import PartitionSpec as P

C_SPEED = 2.5
CFL_STEP = 0.12
MESH = pl.DeviceIdType.MESH
HIGHEST = lax.Precision.HIGHEST

TWIN = (1, 0, 3, 2, 5, 4)
ACROSS = (2, 4, 0, 5, 1, 3)
PRIMARY = (0, 2, 4)
STRIPS = ((2, 4), (0, 5), (1, 3))
CORNERS = {0: ((0, 1, 1), 1, 0), 2: ((1, 0, 1), 0, 0), 4: ((1, 1, 0), 0, 1)}

SIZE = 128
TILES = 16
LOW = 2
OWN = 90
BLOCK_STEPS = 9


def pos_idx(pos):
    return TILES * (pos % 8) + pos // 8


def tiles_of(arr):
    return [arr[8 * i:8 * i + 8] for i in range(arr.shape[0] // 8)]


def join(tiles):
    return jnp.concatenate(tiles, axis=0)


def roll_rows(tile, shift):
    return pltpu.roll(tile, shift % 8, 0)


def solution(mesh):
    axis_names = mesh.axis_names

    def local_run(tracer, wind_a, wind_b, wind_scale):
        own = tracer.shape[1]
        cells = 2 * own
        steps = wind_scale.shape[0]
        dalpha = 0.5 * math.pi / cells
        tan_u = np.tan((pos_idx(np.arange(SIZE)) - LOW + 0.5) * dalpha - 0.25 * math.pi)
        tan_a, tan_b = tan_u[:, None], tan_u[None, :]
        r_sq = 1.0 + tan_a * tan_a + tan_b * tan_b
        inv_sqrt_g = r_sq * np.sqrt(r_sq) / ((1.0 + tan_a * tan_a) * (1.0 + tan_b * tan_b))
        gain = (0.5 * C_SPEED * CFL_STEP * inv_sqrt_g).astype(np.float32)
        out = pl.pallas_call(
            functools.partial(kernel, own, steps, axis_names),
            out_shape=jax.ShapeDtypeStruct(tracer.shape, jnp.float32),
            in_specs=[pl.BlockSpec(memory_space=pltpu.SMEM)] + [pl.BlockSpec(memory_space=pltpu.VMEM)] * 4,
            out_specs=pl.BlockSpec(memory_space=pltpu.VMEM),
            scratch_shapes=[
                pltpu.VMEM((6, SIZE, SIZE), jnp.float32),
                pltpu.VMEM((6, SIZE, SIZE), jnp.float32),
                pltpu.VMEM((BLOCK_STEPS, 6, SIZE, SIZE), jnp.float32),
                pltpu.VMEM((6, SIZE, SIZE), jnp.float32),
                pltpu.VMEM((4, SIZE, SIZE), jnp.float32),
                pltpu.VMEM((3, 3, own, own), jnp.float32),
                pltpu.VMEM((3, own, own), jnp.float32),
                pltpu.VMEM((3, 3, 72, SIZE), jnp.float32),
                pltpu.VMEM((4, 3, 72, SIZE), jnp.float32),
                pltpu.VMEM((3, 3, 16, SIZE), jnp.float32),
                pltpu.VMEM((4, 3, 16, SIZE), jnp.float32),
                pltpu.SemaphoreType.DMA((4, 6)),
                pltpu.SemaphoreType.DMA((4, 6)),
                pltpu.SemaphoreType.DMA((3, 3)),
                pltpu.SemaphoreType.DMA((3, 3)),
                pltpu.SemaphoreType.DMA((3,)),
                pltpu.SemaphoreType.DMA((3,)),
            ],
            name="advect",
        )(wind_scale, tracer, wind_a, wind_b, gain)
        return out

    field_spec = P(('member', 'panel'), 'tx', 'ty')
    wind_spec = P('panel', 'tx', 'ty')
    return jax.shard_map(local_run, mesh=mesh, in_specs=(field_spec, wind_spec, wind_spec, P()),
                         out_specs=field_spec, check_vma=False)


def kernel(own, steps, axis_names, ws_ref, q_in, wa_in, wb_in, gain_ref, out_ref,
           qa, qb, sw, wf, coef, tiles, result, send, recv, csend, crecv,
           ssem, rsem, tsend, trecv, osend, orecv):
    tx, ty, core = lax.axis_index('tx'), lax.axis_index('ty'), lax.axis_index('panel')
    by, bz, bx = tx, ty, lax.rem(core + tx + 1, 2)

    def place(kx, ky, kc):
        return {name: {'tx': kx, 'ty': ky, 'panel': kc}.get(name, 0) for name in axis_names}

    def at(ox, oy, oz):
        return place(oy, oz, lax.rem(ox + oy + 1, 2))

    def pick(first, second):
        return jnp.where(core == 0, first, second)

    homes = (
        (pick(1, tx), pick(tx, 0), ty, pick(0, 1)),
        (pick(1 - tx, 1 - ty), pick(1, tx), pick(ty, 1), pick(1, 2)),
        (pick(0, ty), pick(1 - tx, tx), pick(ty, 0), pick(0, 2)),
    )
    leaves = [jnp.logical_not((ox == bx) & (oy == by) & (oz == bz)) for ox, oy, oz, _ in homes]
    flip_a = (1 - lax.rem(bx + by, 2), lax.rem(bx + by, 2), by)
    flip_b = (bz, bz, jnp.where(bz == 1, 1 - bx, bx))
    panel = (jnp.where(bx == 1, 0, 2), jnp.where(by == 1, 1, 3), jnp.where(bz == 1, 4, 5))
    holder = [place(flip_a[n], flip_b[n], panel[n] // 3) for n in range(3)]
    slot_of = [lax.rem(panel[n], 3) for n in range(3)]
    comes = [jnp.logical_not((flip_a[n] == tx) & (flip_b[n] == ty) & (panel[n] // 3 == core)) for n in range(3)]

    fields = (q_in, wa_in, wb_in)

    def tile_copy(f, slot, quad, device):
        return pltpu.make_async_remote_copy(
            fields[f].at[slot], tiles.at[f, quad], tsend.at[f, slot], trecv.at[f, quad],
            device_id=device, device_id_type=MESH)

    for f in (1, 2, 0):
        for slot in range(3):
            ox, oy, oz, quad = homes[slot]

            @pl.when(leaves[slot])
            def _():
                tile_copy(f, slot, quad, at(ox, oy, oz)).start()

            @pl.when(jnp.logical_not(leaves[slot]))
            def _():
                tiles[f, quad] = fields[f][slot]

    pos_r = lax.broadcasted_iota(jnp.int32, (SIZE, own), 0)
    cell_c = lax.broadcasted_iota(jnp.int32, (SIZE, own), 1)
    cell_r = lax.broadcasted_iota(jnp.int32, (own, SIZE), 0)
    pos_c = lax.broadcasted_iota(jnp.int32, (own, SIZE), 1)

    def spot(pos, flip):
        dist = TILES * lax.rem(pos, 8) + pos // 8 - LOW
        inside = (dist >= 0) & (dist < own)
        return jnp.where(inside, jnp.where(flip == 1, own - 1 - dist, dist), -1)

    def place_rows(flip):
        return jnp.where(spot(pos_r, flip) == cell_c, 1.0, 0.0)

    def place_cols(flip):
        return jnp.where(spot(pos_c, flip) == cell_r, 1.0, 0.0)

    def dot(lhs, rhs):
        return jnp.dot(lhs, rhs, precision=HIGHEST, preferred_element_type=jnp.float32)

    PLAIN = (0, 2, 5)

    sub = lax.broadcasted_iota(jnp.int32, (8, SIZE), 0)
    lane = lax.broadcasted_iota(jnp.int32, (8, SIZE), 1)
    lane_s, lane_i = lax.rem(lane, 8), lane // 8
    halo_lane = (lane_s >= 6) | ((lane_s == 5) & (lane_i >= 12))
    mirror = jnp.where(lane_i < 8, 67, 194)
    pair_src = mirror - (8 * lane_i + 6 + lax.rem(lane, 2))
    edge_src = jnp.where(lane_i >= 12, 189 - 8 * lane_i, 0)
    halo_src = jnp.where(halo_lane, mirror - lane, 0)
    row_even, row_odd = 5 - lax.rem(sub, 2), 4 - lax.rem(sub, 2)
    row_pair, lane_pair = sub // 2, lane_s // 2

    def take(tile, idx, axis):
        return jnp.take_along_axis(tile, idx, axis=axis, mode="promise_in_bounds")

    def by_number(number, parts):
        res = parts[3]
        for m in (2, 1, 0):
            res = jnp.where(number == m, parts[m], res)
        return res

    def peer(mirrored):
        return at(*(1 - b if m else b for b, m in zip((bx, by, bz), mirrored)))

    def strip_copy(axis, out, slot):
        return pltpu.make_async_remote_copy(
            send.at[out, axis], recv.at[slot, axis], ssem.at[slot, axis], rsem.at[slot, axis],
            device_id=peer(tuple(int(n == axis) for n in range(3))), device_id_type=MESH)

    def corner_copy(k, out, slot):
        n = PRIMARY.index(k)
        return pltpu.make_async_remote_copy(
            csend.at[out, n], crecv.at[slot, n], ssem.at[slot, 3 + n], rsem.at[slot, 3 + n],
            device_id=peer(CORNERS[k][0]), device_id_type=MESH)

    def pack_strip(get, axis, out, sign):
        for n, k in enumerate(STRIPS[axis]):
            a = [get(k, i) for i in range(TILES)]
            for j in range(4):
                first, perm = (7, row_even) if j < 2 else (23, row_odd)
                part = by_number(row_pair, [take(a[first - 4 * j - m], perm, 0) for m in range(4)])
                send[out, axis, 32 * n + 8 * j:32 * n + 8 * j + 8] = sign * part if sign != 1.0 else part
            tail = by_number(lax.rem(sub, 4), [take(a[11 - m], row_even * 0 + 5, 0) for m in range(4)])
            tail = sign * tail if sign != 1.0 else tail
            send[out, axis, 64 + 4 * n:68 + 4 * n] = tail[4 * n:4 * n + 4]

    def pack_corner(k, out, sign):
        _, axis, n = CORNERS[k]
        msg = [send[out, axis, 32 * n + 8 * j:32 * n + 8 * j + 8] for j in range(4)]
        tail = send[out, axis, 64:72]
        pairs = by_number(lane_pair, [take(m, pair_src, 1) for m in msg])
        edges = by_number(lane_s, [take(m, edge_src, 1) for m in msg])
        rest = jnp.where(halo_lane, take(tail, halo_src, 1), edges)
        slot = PRIMARY.index(k)
        csend[out, slot, 0:8] = sign * pairs if sign != 1.0 else pairs
        csend[out, slot, 8:16] = sign * rest if sign != 1.0 else rest

    def start_all(arrs, out, slot, row_sign, corner_sign):
        def get(k, i):
            return arrs[k, 8 * i:8 * i + 8]
        pack_strip(get, 2, out, row_sign)
        strip_copy(2, out, slot).start()
        pack_strip(get, 1, out, row_sign)
        pack_corner(0, out, corner_sign)
        corner_copy(0, out, slot).start()
        pack_strip(get, 0, out, row_sign)
        pack_corner(4, out, corner_sign)
        corner_copy(4, out, slot).start()
        strip_copy(1, out, slot).start()
        pack_corner(2, out, corner_sign)
        corner_copy(2, out, slot).start()
        strip_copy(0, out, slot).start()

    def merge_corner(k, slot):
        _, axis, n = CORNERS[k]
        pairs, rest = crecv[slot, PRIMARY.index(k), 0:8], crecv[slot, PRIMARY.index(k), 8:16]
        for j in range(4):
            rows = pl.ds(32 * n + 8 * j, 8)
            mixed = jnp.where(lane_s >= 6, pltpu.roll(pairs, (6 - 2 * j) % SIZE, 1), recv[slot, axis, rows])
            recv[slot, axis, rows] = jnp.where((lane_s == 5) & (lane_i >= 12), pltpu.roll(rest, (5 - j) % SIZE, 1), mixed)
        mine = halo_lane & (sub // 4 == n)
        recv[slot, axis, 64:72] = jnp.where(mine, rest, recv[slot, axis, 64:72])

    def unpack_strip(arrs, axis, slot):
        for n, k in enumerate(STRIPS[axis]):
            for i in range(TILES):
                arrs[k, 8 * i + 6:8 * i + 8] = recv[slot, axis, 32 * n + 2 * i:32 * n + 2 * i + 2]
            for i in range(12, TILES):
                arrs[k, 8 * i + 5:8 * i + 6] = recv[slot, axis, 52 + 4 * n + i:53 + 4 * n + i]

    def own_rows(i):
        return sub < (6 if i < 12 else 5)

    def lanes_from(arrs, k, source):
        turned = tiles_of(source.T)
        for i in range(TILES):
            mask = halo_lane & own_rows(i) if k in PRIMARY else halo_lane
            arrs[k, 8 * i:8 * i + 8] = jnp.where(mask, turned[i], arrs[k, 8 * i:8 * i + 8])

    def ghosts(arrs):
        for k in range(6):
            near = ACROSS[k]
            arrs[k, 0:1] = arrs[near, 24:25]
            arrs[k, 8:9] = arrs[near, 16:17]

    def early_rows(arrs, out, slot):
        strip_copy(0, out, slot).wait()
        corner_copy(2, out, slot).wait()
        merge_corner(2, slot)
        corner_copy(4, out, slot).wait()
        merge_corner(4, slot)
        unpack_strip(arrs, 0, slot)
        strip_copy(1, out, slot).wait()
        corner_copy(0, out, slot).wait()
        merge_corner(0, slot)
        unpack_strip(arrs, 1, slot)

    def late_rows(arrs, out, slot):
        strip_copy(2, out, slot).wait()
        for n, k in enumerate(STRIPS[2]):
            for i in range(TILES):
                rows = pl.ds(8 * i + 6, 2)
                arrs[k, rows] = jnp.where(halo_lane[0:2], arrs[k, rows], recv[slot, 2, 32 * n + 2 * i:32 * n + 2 * i + 2])
            for i in range(12, TILES):
                rows = pl.ds(8 * i + 5, 1)
                arrs[k, rows] = jnp.where(halo_lane[0:1], arrs[k, rows], recv[slot, 2, 52 + 4 * n + i:53 + 4 * n + i])

    def scale_faces(first_step):
        def one(step, carry):
            scale = ws_ref[lax.rem(first_step + step, steps)]
            sw[step] = scale * wf[...]
            return carry
        lax.fori_loop(0, BLOCK_STEPS, one, 0)

    for f in (1, 2, 0):
        for slot in range(3):
            ox, oy, oz, quad = homes[slot]

            @pl.when(leaves[slot])
            def _():
                tile_copy(f, slot, quad, at(ox, oy, oz)).wait_send()
        for quad in range(3):
            @pl.when(comes[quad])
            def _():
                tile_copy(f, 0, quad, holder[quad]).wait_recv()
        for quad in range(3):
            loc = dot(dot(place_rows(flip_a[quad]), tiles[f, quad]), place_cols(flip_b[quad]))
            plain, turned = PLAIN[quad], TWIN[PLAIN[quad]]
            if f == 0:
                qa[plain] = loc
                qa[turned] = loc.T
            elif f == 1:
                loc = jnp.where(flip_a[quad] == 1, -1.0, 1.0) * loc
                qb[plain] = loc
                sw[0, turned] = loc.T
            else:
                loc = jnp.where(flip_b[quad] == 1, -1.0, 1.0) * loc
                sw[0, plain] = loc
                qb[turned] = loc.T
        if f == 2:
            start_all(qb, 1, 2, -1.0, 1.0)
            start_all(sw.at[0], 2, 3, 1.0, -1.0)
    start_all(qa, 0, 0, 1.0, 1.0)

    coef[0] = gain_ref[...]
    coef[1] = 1.0 - 4.0 * gain_ref[...]
    coef[2] = 0.5 * gain_ref[...]
    coef[3] = 0.5 - 2.0 * gain_ref[...]

    early_rows(qb, 1, 2)
    late_rows(qb, 1, 2)
    early_rows(sw.at[0], 2, 3)
    late_rows(sw.at[0], 2, 3)
    for k in range(6):
        lanes_from(qb, k, sw[0, TWIN[k]])
    for k in range(6):
        qb[k, 8:9] = -qb[ACROSS[k], 16:17]
    for k in range(6):
        here = qb[k]
        after = jnp.concatenate([here[8:], roll_rows(here[:8], -1)], axis=0)
        wf[k] = (0.5 / (6.0 * C_SPEED)) * (here + after)
    scale_faces(0)

    def lanes_and_ghosts(out, slot):
        for k in (1, 3, 4, 5):
            lanes_from(qa, k, qa[TWIN[k]])
        late_rows(qa, out, slot)
        for k in (0, 2):
            lanes_from(qa, k, qa[TWIN[k]])
        ghosts(qa)

    early_rows(qa, 0, 0)
    lanes_and_ghosts(0, 0)

    def x_part(a_ref, k, faces):
        a = a_ref[k]
        before = jnp.concatenate([a_ref[k, 119:127], a[:120]], axis=0)
        after = jnp.concatenate([a[8:], a_ref[k, 1:9]], axis=0)
        m = before + after
        v = 8.0 * a - m
        v_after = jnp.concatenate([v[8:], roll_rows(v[:8], -1)], axis=0)
        flux = faces * (v + v_after)
        flux_before = jnp.concatenate([roll_rows(flux[120:], 1), flux[:120]], axis=0)
        return (m - flux) + flux_before

    def stage(src, dst, second, step):
        ready = []
        for k in PRIMARY:
            t = TWIN[k]
            gain = coef[2 if second else 0]
            zk = gain * x_part(src, k, sw[step, k])
            own_part = coef[3 if second else 1] * src[k]
            if second:
                own_part = 0.5 * dst[k] + own_part
            zk = own_part + zk
            zt = gain * x_part(src, t, sw[step, t])
            ready.append((zk, zt))
        new = [None] * 6
        for k, (zk, zt) in zip(PRIMARY, ready):
            new[k] = zk + zt.T
            new[TWIN[k]] = zt + zk.T
        for k in range(6):
            dst[k] = new[k]
        for k in range(6):
            near = new[ACROSS[k]]
            dst[k, 0:1] = near[24:25]
            dst[k, 8:9] = near[16:17]

    def one_step(step, carry):
        stage(qa, qb, False, step)
        stage(qb, qa, True, step)
        return carry

    def run_steps(count):
        lax.fori_loop(0, count, one_step, 0, unroll=True)

    full_blocks = (steps - 1) // BLOCK_STEPS

    def block(blk, carry):
        run_steps(BLOCK_STEPS)
        slot = lax.rem(blk + 1, 2)
        start_all(qa, 0, slot, 1.0, 1.0)
        scale_faces((blk + 1) * BLOCK_STEPS)
        early_rows(qa, 0, slot)
        lanes_and_ghosts(0, slot)
        return carry

    lax.fori_loop(0, full_blocks, block, 0)
    run_steps(steps - full_blocks * BLOCK_STEPS)

    def result_copy(quad, slot, device, number):
        return pltpu.make_async_remote_copy(
            result.at[quad], out_ref.at[slot], osend.at[number], orecv.at[slot],
            device_id=device, device_id_type=MESH)

    for quad in range(3):
        result[quad] = dot(dot(place_cols(flip_a[quad]), qa[PLAIN[quad]]), place_rows(flip_b[quad]))

        @pl.when(comes[quad])
        def _():
            result_copy(quad, slot_of[quad], holder[quad], quad).start()

        @pl.when(jnp.logical_not(comes[quad]))
        def _():
            out_ref[slot_of[quad]] = result[quad]

    for quad in range(3):
        @pl.when(comes[quad])
        def _():
            result_copy(quad, slot_of[quad], holder[quad], quad).wait_send()
    for slot in range(3):
        ox, oy, oz, _ = homes[slot]

        @pl.when(leaves[slot])
        def _():
            result_copy(0, slot, at(ox, oy, oz), 0).wait_recv()
```

```python
import functools
import math

import jax
import jax.numpy as jnp
import numpy as np
from jax import lax
from jax.experimental import pallas as pl
from jax.experimental.pallas import tpu as pltpu
from jax.sharding import PartitionSpec as P

C_SPEED = 2.5
CFL_STEP = 0.12
MESH = pl.DeviceIdType.MESH
HIGHEST = lax.Precision.HIGHEST

TWIN = (1, 0, 3, 2, 5, 4)
ACROSS = (2, 4, 0, 5, 1, 3)
PRIMARY = (0, 2, 4)
STRIPS = ((2, 4), (0, 5), (1, 3))
CORNERS = {0: ((0, 1, 1), 1, 0), 2: ((1, 0, 1), 0, 0), 4: ((1, 1, 0), 0, 1)}

SIZE = 128
TILES = 16
LOW = 2
OWN = 90
BLOCK_STEPS = 9
LANE_ORDER = (8, 7, 9, 6, 10, 5, 11, 4, 12, 3, 13, 2, 14, 1, 15, 0)
GROUPS = ((0, 2), (1, 3), (4, 5))


def row_idx(row):
    return TILES * (row % 8) + row // 8


def lane_group(b):
    half = (b + 1) // 2
    return 8 - half + 2 * half * (1 - b % 2)


def turn(arr):
    turned = jnp.concatenate([arr[8 * i:8 * i + 8] for i in LANE_ORDER], axis=0).T
    return jnp.concatenate([turned[8 * b:8 * b + 8] for b in map(LANE_ORDER.index, range(TILES))], axis=0)


def tiles_of(arr):
    return [arr[8 * i:8 * i + 8] for i in range(arr.shape[0] // 8)]


def join(tiles):
    return jnp.concatenate(tiles, axis=0)


def roll_rows(tile, shift):
    return pltpu.roll(tile, shift % 8, 0)


def solution(mesh):
    axis_names = mesh.axis_names

    def local_run(tracer, wind_a, wind_b, wind_scale):
        own = tracer.shape[1]
        cells = 2 * own
        steps = wind_scale.shape[0]
        dalpha = 0.5 * math.pi / cells
        place = np.arange(SIZE)
        lane_idx = TILES * (place % 8) + lane_group(place // 8)
        tan_a = np.tan((row_idx(place) - LOW + 0.5) * dalpha - 0.25 * math.pi)[:, None]
        tan_b = np.tan((lane_idx - LOW + 0.5) * dalpha - 0.25 * math.pi)[None, :]
        r_sq = 1.0 + tan_a * tan_a + tan_b * tan_b
        inv_sqrt_g = r_sq * np.sqrt(r_sq) / ((1.0 + tan_a * tan_a) * (1.0 + tan_b * tan_b))
        gain = (0.5 * C_SPEED * CFL_STEP * inv_sqrt_g).astype(np.float32)
        out = pl.pallas_call(
            functools.partial(kernel, own, steps, axis_names),
            out_shape=jax.ShapeDtypeStruct(tracer.shape, jnp.float32),
            in_specs=[pl.BlockSpec(memory_space=pltpu.SMEM)] + [pl.BlockSpec(memory_space=pltpu.VMEM)] * 4,
            out_specs=pl.BlockSpec(memory_space=pltpu.VMEM),
            scratch_shapes=[
                pltpu.VMEM((6, SIZE, SIZE), jnp.float32),
                pltpu.VMEM((6, SIZE, SIZE), jnp.float32),
                pltpu.VMEM((BLOCK_STEPS, 6, SIZE, SIZE), jnp.float32),
                pltpu.VMEM((6, SIZE, SIZE), jnp.float32),
                pltpu.VMEM((4, SIZE, SIZE), jnp.float32),
                pltpu.VMEM((3, 3, own, own), jnp.float32),
                pltpu.VMEM((3, own, own), jnp.float32),
                pltpu.VMEM((3, 3, 72, SIZE), jnp.float32),
                pltpu.VMEM((4, 3, 72, SIZE), jnp.float32),
                pltpu.VMEM((3, 3, 16, SIZE), jnp.float32),
                pltpu.VMEM((4, 3, 16, SIZE), jnp.float32),
                pltpu.SemaphoreType.DMA((4, 6)),
                pltpu.SemaphoreType.DMA((4, 6)),
                pltpu.SemaphoreType.DMA((3, 3)),
                pltpu.SemaphoreType.DMA((3, 3)),
                pltpu.SemaphoreType.DMA((3,)),
                pltpu.SemaphoreType.DMA((3,)),
            ],
            name="advect",
        )(wind_scale, tracer, wind_a, wind_b, gain)
        return out

    field_spec = P(('member', 'panel'), 'tx', 'ty')
    wind_spec = P('panel', 'tx', 'ty')
    return jax.shard_map(local_run, mesh=mesh, in_specs=(field_spec, wind_spec, wind_spec, P()),
                         out_specs=field_spec, check_vma=False)


def kernel(own, steps, axis_names, ws_ref, q_in, wa_in, wb_in, gain_ref, out_ref,
           qa, qb, sw, wf, coef, tiles, result, send, recv, csend, crecv,
           ssem, rsem, tsend, trecv, osend, orecv):
    tx, ty, core = lax.axis_index('tx'), lax.axis_index('ty'), lax.axis_index('panel')
    by, bz, bx = tx, ty, lax.rem(core + tx + 1, 2)

    def place(kx, ky, kc):
        return {name: {'tx': kx, 'ty': ky, 'panel': kc}.get(name, 0) for name in axis_names}

    def at(ox, oy, oz):
        return place(oy, oz, lax.rem(ox + oy + 1, 2))

    def pick(first, second):
        return jnp.where(core == 0, first, second)

    homes = (
        (pick(1, tx), pick(tx, 0), ty, pick(0, 1)),
        (pick(1 - tx, 1 - ty), pick(1, tx), pick(ty, 1), pick(1, 2)),
        (pick(0, ty), pick(1 - tx, tx), pick(ty, 0), pick(0, 2)),
    )
    leaves = [jnp.logical_not((ox == bx) & (oy == by) & (oz == bz)) for ox, oy, oz, _ in homes]
    flip_a = (1 - lax.rem(bx + by, 2), lax.rem(bx + by, 2), by)
    flip_b = (bz, bz, jnp.where(bz == 1, 1 - bx, bx))
    panel = (jnp.where(bx == 1, 0, 2), jnp.where(by == 1, 1, 3), jnp.where(bz == 1, 4, 5))
    holder = [place(flip_a[n], flip_b[n], panel[n] // 3) for n in range(3)]
    slot_of = [lax.rem(panel[n], 3) for n in range(3)]
    comes = [jnp.logical_not((flip_a[n] == tx) & (flip_b[n] == ty) & (panel[n] // 3 == core)) for n in range(3)]

    fields = (q_in, wa_in, wb_in)

    def tile_copy(f, slot, quad, device):
        return pltpu.make_async_remote_copy(
            fields[f].at[slot], tiles.at[f, quad], tsend.at[f, slot], trecv.at[f, quad],
            device_id=device, device_id_type=MESH)

    for f in (1, 2, 0):
        for slot in range(3):
            ox, oy, oz, quad = homes[slot]

            @pl.when(leaves[slot])
            def _():
                tile_copy(f, slot, quad, at(ox, oy, oz)).start()

            @pl.when(jnp.logical_not(leaves[slot]))
            def _():
                tiles[f, quad] = fields[f][slot]

    def placing(shape, spot_axis, to_idx, flip):
        dist = to_idx(lax.broadcasted_iota(jnp.int32, shape, spot_axis)) - LOW
        cell = lax.broadcasted_iota(jnp.int32, shape, 1 - spot_axis)
        inside = (dist >= 0) & (dist < own)
        source = jnp.where(inside, jnp.where(flip == 1, own - 1 - dist, dist), -1)
        return jnp.where(source == cell, 1.0, 0.0)

    def row_to_idx(row):
        return TILES * lax.rem(row, 8) + row // 8

    def lane_to_idx(spot):
        b = spot // 8
        half = (b + 1) // 2
        return TILES * lax.rem(spot, 8) + 8 - half + 2 * half * (1 - lax.rem(b, 2))

    def dot(lhs, rhs):
        return jnp.dot(lhs, rhs, precision=HIGHEST, preferred_element_type=jnp.float32)

    PLAIN = (0, 2, 5)

    sub = lax.broadcasted_iota(jnp.int32, (8, SIZE), 0)
    lane = lax.broadcasted_iota(jnp.int32, (8, SIZE), 1)
    lane_s, lane_i = lax.rem(lane, 8), lax.rem(lane_to_idx(lane), TILES)
    halo_lane = (lane_s >= 6) | ((lane_s == 5) & (lane_i >= 12))

    def mirror_lane(number):
        return jnp.where(lane_i < 8, 8 * (1 + 2 * lane_i) + 11 - number, 8 * (30 - 2 * lane_i) + 10 - number)

    pair_src = mirror_lane(6 + lax.rem(lane, 2))
    edge_src = jnp.where(lane_i >= 12, mirror_lane(5), 0)
    halo_src = jnp.where(halo_lane, mirror_lane(lane_s), 0)
    row_even, row_odd = 5 - lax.rem(sub, 2), 4 - lax.rem(sub, 2)
    row_pair, lane_pair = sub // 2, lane_s // 2

    def take(tile, idx, axis):
        return jnp.take_along_axis(tile, idx, axis=axis, mode="promise_in_bounds")

    def by_number(number, parts):
        res = parts[3]
        for m in (2, 1, 0):
            res = jnp.where(number == m, parts[m], res)
        return res

    def peer(mirrored):
        return at(*(1 - b if m else b for b, m in zip((bx, by, bz), mirrored)))

    def strip_copy(axis, out, slot):
        return pltpu.make_async_remote_copy(
            send.at[out, axis], recv.at[slot, axis], ssem.at[slot, axis], rsem.at[slot, axis],
            device_id=peer(tuple(int(n == axis) for n in range(3))), device_id_type=MESH)

    def corner_copy(k, out, slot):
        n = PRIMARY.index(k)
        return pltpu.make_async_remote_copy(
            csend.at[out, n], crecv.at[slot, n], ssem.at[slot, 3 + n], rsem.at[slot, 3 + n],
            device_id=peer(CORNERS[k][0]), device_id_type=MESH)

    def signed(sign, arr):
        return arr if sign == 1.0 else sign * arr

    def pack_strip(arrs, axis, out, sign):
        msgs, tails = [], []
        for k in STRIPS[axis]:
            a = tiles_of(arrs[k])
            for j in range(4):
                first, perm = (7, row_even) if j < 2 else (23, row_odd)
                msgs.append(signed(sign, by_number(row_pair, [take(a[first - 4 * j - m], perm, 0) for m in range(4)])))
            tails.append(by_number(lax.rem(sub, 4), [take(a[11 - m], 0 * sub + 5, 0) for m in range(4)]))
        tail = signed(sign, jnp.where(sub < 4, tails[0], tails[1]))
        send[out, axis] = jnp.concatenate(msgs + [tail], axis=0)
        return msgs, tail

    def pack_corner(k, packed, out, sign):
        n = CORNERS[k][2]
        msg, tail = packed[0][4 * n:4 * n + 4], packed[1]
        pairs = by_number(lane_pair, [take(m, pair_src, 1) for m in msg])
        edges = by_number(lane_s, [take(m, edge_src, 1) for m in msg])
        rest = jnp.where(halo_lane, take(tail, halo_src, 1), edges)
        csend[out, PRIMARY.index(k)] = signed(sign, jnp.concatenate([pairs, rest], axis=0))

    def start_all(arrs, out, slot, row_sign, corner_sign):
        pack_strip(arrs, 2, out, row_sign)
        strip_copy(2, out, slot).start()
        packed = [pack_strip(arrs, axis, out, row_sign) for axis in (0, 1)]
        for k in PRIMARY:
            pack_corner(k, packed[CORNERS[k][1]], out, corner_sign)
        corner_copy(0, out, slot).start()
        corner_copy(4, out, slot).start()
        strip_copy(1, out, slot).start()
        corner_copy(2, out, slot).start()
        strip_copy(0, out, slot).start()

    def halo_tiles(k, axis, n, slot, with_corner):
        msg = [recv[slot, axis, 32 * n + 8 * j:32 * n + 8 * j + 8] for j in range(4)]
        tail = recv[slot, axis, 64:72]
        if with_corner:
            pairs, rest = crecv[slot, PRIMARY.index(k), 0:8], crecv[slot, PRIMARY.index(k), 8:16]
            edge = (lane_s == 5) & (lane_i >= 12)
            for j in range(4):
                mixed = jnp.where(lane_s >= 6, pltpu.roll(pairs, (6 - 2 * j) % SIZE, 1), msg[j])
                msg[j] = jnp.where(edge, pltpu.roll(rest, (5 - j) % SIZE, 1), mixed)
            tail = jnp.where(halo_lane, rest, tail)
        res = []
        for i in range(TILES):
            tile = roll_rows(msg[i // 4], 6 - 2 * (i % 4))
            if i >= 12:
                tile = jnp.where(sub == 5, roll_rows(tail, 17 - i - 4 * n), tile)
            res.append(tile)
        return res

    def own_rows(i):
        return sub < (6 if i < 12 else 5)

    def wait_all(out, slot):
        for axis in (0, 1, 2):
            strip_copy(axis, out, slot).wait()
        for k in PRIMARY:
            corner_copy(k, out, slot).wait()

    def all_halos(slot):
        halos = [None] * 6
        for with_corner in (False, True):
            for axis in range(3):
                for n, k in enumerate(STRIPS[axis]):
                    if (k in PRIMARY) == with_corner:
                        halos[k] = halo_tiles(k, axis, n, slot, with_corner)
        return halos

    def merge(arrs, k, halos, lanes):
        a, side = tiles_of(arrs[k]), tiles_of(lanes)
        for i in range(TILES):
            if k in PRIMARY:
                new = jnp.where(own_rows(i), jnp.where(halo_lane, side[i], a[i]), halos[k][i])
            else:
                new = jnp.where(halo_lane, side[i], jnp.where(own_rows(i), a[i], halos[k][i]))
            arrs[k, 8 * i:8 * i + 8] = new

    def finish(slot):
        wait_all(0, slot)
        halos = all_halos(slot)
        lanes = [None] * 6
        for k in (1, 3, 5, 0, 2, 4):
            lanes[TWIN[k]] = turn(join(halos[k]))
        for k in (0, 2, 4, 1, 3, 5):
            merge(qa, k, halos, lanes[k])
        for k in range(6):
            near = ACROSS[k]
            qa[k, 0:1] = qa[near, 24:25]
            qa[k, 8:9] = qa[near, 16:17]

    def scale_faces(first_step):
        def one(step, carry):
            scale = ws_ref[lax.rem(first_step + step, steps)]
            sw[step] = scale * wf[...]
            return carry
        lax.fori_loop(0, BLOCK_STEPS, one, 0)

    for f in (1, 2, 0):
        for slot in range(3):
            ox, oy, oz, quad = homes[slot]

            @pl.when(leaves[slot])
            def _():
                tile_copy(f, slot, quad, at(ox, oy, oz)).wait_send()
        for quad in range(3):
            @pl.when(comes[quad])
            def _():
                tile_copy(f, 0, quad, holder[quad]).wait_recv()
        for quad in range(3):
            loc = dot(dot(placing((SIZE, own), 0, row_to_idx, flip_a[quad]), tiles[f, quad]),
                      placing((own, SIZE), 1, lane_to_idx, flip_b[quad]))
            plain, turned = PLAIN[quad], TWIN[PLAIN[quad]]
            if f == 0:
                qa[plain] = loc
                qa[turned] = turn(loc)
            elif f == 1:
                loc = jnp.where(flip_a[quad] == 1, -1.0, 1.0) * loc
                qb[plain] = loc
                sw[0, turned] = turn(loc)
            else:
                loc = jnp.where(flip_b[quad] == 1, -1.0, 1.0) * loc
                sw[0, plain] = loc
                qb[turned] = turn(loc)
        if f == 2:
            start_all(qb, 1, 2, -1.0, 1.0)
            start_all(sw.at[0], 2, 3, 1.0, -1.0)
    start_all(qa, 0, 0, 1.0, 1.0)

    coef[0] = gain_ref[...]
    coef[1] = 1.0 - 4.0 * gain_ref[...]
    coef[2] = 0.5 * gain_ref[...]
    coef[3] = 0.5 - 2.0 * gain_ref[...]

    wait_all(1, 2)
    wait_all(2, 3)
    wind_halos, side_halos = all_halos(2), all_halos(3)
    for k in range(6):
        merge(qb, k, wind_halos, turn(join(side_halos[TWIN[k]])))
    for k in range(6):
        qb[k, 8:9] = -qb[ACROSS[k], 16:17]
    for k in range(6):
        here = qb[k]
        after = jnp.concatenate([here[8:], roll_rows(here[:8], -1)], axis=0)
        wf[k] = (0.5 / (6.0 * C_SPEED)) * (here + after)
    scale_faces(0)

    def x_part(a_ref, k, faces):
        a = a_ref[k]
        before = jnp.concatenate([a_ref[k, 119:127], a[:120]], axis=0)
        after = jnp.concatenate([a[8:], a_ref[k, 1:9]], axis=0)
        m = before + after
        v = 8.0 * a - m
        v_after = jnp.concatenate([v[8:], roll_rows(v[:8], -1)], axis=0)
        flux = faces * (v + v_after)
        flux_before = jnp.concatenate([roll_rows(flux[120:], 1), flux[:120]], axis=0)
        return (m - flux) + flux_before

    def stage(src, dst, second, step):
        part, turned = [None] * 6, [None] * 6
        for group in GROUPS:
            for k in group:
                part[k] = coef[2 if second else 0] * x_part(src, k, sw[step, k])
                if k in PRIMARY:
                    own_part = coef[3 if second else 1] * src[k]
                    if second:
                        own_part = 0.5 * dst[k] + own_part
                    part[k] = own_part + part[k]
            for k in group:
                turned[k] = turn(part[k])
        new = [part[k] + turned[TWIN[k]] for k in range(6)]
        for k in range(6):
            dst[k] = new[k]
        for k in range(6):
            near = new[ACROSS[k]]
            dst[k, 0:1] = near[24:25]
            dst[k, 8:9] = near[16:17]

    def one_step(step, carry):
        stage(qa, qb, False, step)
        stage(qb, qa, True, step)
        return carry

    def run_steps(count):
        lax.fori_loop(0, count, one_step, 0, unroll=True)

    full_blocks = (steps - 1) // BLOCK_STEPS

    def block(blk, carry):
        finish(lax.rem(blk, 2))
        run_steps(BLOCK_STEPS)
        start_all(qa, 0, lax.rem(blk + 1, 2), 1.0, 1.0)
        scale_faces((blk + 1) * BLOCK_STEPS)
        return carry

    lax.fori_loop(0, full_blocks, block, 0)
    finish(full_blocks % 2)
    run_steps(steps - full_blocks * BLOCK_STEPS)

    def result_copy(quad, slot, device, number):
        return pltpu.make_async_remote_copy(
            result.at[quad], out_ref.at[slot], osend.at[number], orecv.at[slot],
            device_id=device, device_id_type=MESH)

    for quad in range(3):
        result[quad] = dot(dot(placing((own, SIZE), 1, row_to_idx, flip_a[quad]), qa[PLAIN[quad]]),
                           placing((SIZE, own), 0, lane_to_idx, flip_b[quad]))

        @pl.when(comes[quad])
        def _():
            result_copy(quad, slot_of[quad], holder[quad], quad).start()

        @pl.when(jnp.logical_not(comes[quad]))
        def _():
            out_ref[slot_of[quad]] = result[quad]

    for quad in range(3):
        @pl.when(comes[quad])
        def _():
            result_copy(quad, slot_of[quad], holder[quad], quad).wait_send()
    for slot in range(3):
        ox, oy, oz, _ = homes[slot]

        @pl.when(leaves[slot])
        def _():
            result_copy(0, slot, at(ox, oy, oz), 0).wait_recv()
```

```python
import functools
import math

import jax
import jax.numpy as jnp
import numpy as np
from jax import lax
from jax.experimental import pallas as pl
from jax.experimental.pallas import tpu as pltpu
from jax.sharding import PartitionSpec as P

C_SPEED = 2.5
CFL_STEP = 0.12
MESH = pl.DeviceIdType.MESH
HIGHEST = lax.Precision.HIGHEST

TWIN = (1, 0, 3, 2, 5, 4)
ACROSS = (2, 4, 0, 5, 1, 3)
PRIMARY = (0, 2, 4)
STRIPS = ((2, 4), (0, 5), (1, 3))
STRIP_PLACE = {k: (axis, n) for axis in range(3) for n, k in enumerate(STRIPS[axis])}
CORNERS = {0: (0, 1, 1), 2: (1, 0, 1), 4: (1, 1, 0)}

SIZE = 128
TILES = 16
LOW = 2
OWN = 90
BLOCK_STEPS = 9
LANE_ORDER = (8, 7, 9, 6, 10, 5, 11, 4, 12, 3, 13, 2, 14, 1, 15, 0)
GROUPS = ((0, 2), (1, 3), (4, 5))


def row_idx(row):
    return TILES * (row % 8) + row // 8


def lane_group(b):
    half = (b + 1) // 2
    return 8 - half + 2 * half * (1 - b % 2)


def turn(arr):
    turned = jnp.concatenate([arr[8 * i:8 * i + 8] for i in LANE_ORDER], axis=0).T
    return jnp.concatenate([turned[8 * b:8 * b + 8] for b in map(LANE_ORDER.index, range(TILES))], axis=0)


def tiles_of(arr):
    return [arr[8 * i:8 * i + 8] for i in range(arr.shape[0] // 8)]


def join(tiles):
    return jnp.concatenate(tiles, axis=0)


def roll_rows(tile, shift):
    return pltpu.roll(tile, shift % 8, 0)


def solution(mesh):
    axis_names = mesh.axis_names

    def local_run(tracer, wind_a, wind_b, wind_scale):
        own = tracer.shape[1]
        cells = 2 * own
        steps = wind_scale.shape[0]
        dalpha = 0.5 * math.pi / cells
        place = np.arange(SIZE)
        lane_idx = TILES * (place % 8) + lane_group(place // 8)
        tan_a = np.tan((row_idx(place) - LOW + 0.5) * dalpha - 0.25 * math.pi)[:, None]
        tan_b = np.tan((lane_idx - LOW + 0.5) * dalpha - 0.25 * math.pi)[None, :]
        r_sq = 1.0 + tan_a * tan_a + tan_b * tan_b
        inv_sqrt_g = r_sq * np.sqrt(r_sq) / ((1.0 + tan_a * tan_a) * (1.0 + tan_b * tan_b))
        gain = (0.5 * C_SPEED * CFL_STEP * inv_sqrt_g).astype(np.float32)
        out = pl.pallas_call(
            functools.partial(kernel, own, steps, axis_names),
            out_shape=jax.ShapeDtypeStruct(tracer.shape, jnp.float32),
            in_specs=[pl.BlockSpec(memory_space=pl.ANY)] * 5,
            out_specs=pl.BlockSpec(memory_space=pl.ANY),
            scratch_shapes=[
                pltpu.SMEM((steps,), jnp.float32),
                pltpu.VMEM((3, 3, own, own), jnp.float32),
                pltpu.VMEM((6, SIZE, SIZE), jnp.float32),
                pltpu.VMEM((6, SIZE, SIZE), jnp.float32),
                pltpu.VMEM((BLOCK_STEPS, 6, SIZE, SIZE), jnp.float32),
                pltpu.VMEM((6, SIZE, SIZE), jnp.float32),
                pltpu.VMEM((4, SIZE, SIZE), jnp.float32),
                pltpu.VMEM((3, 3, own, own), jnp.float32),
                pltpu.VMEM((3, own, own), jnp.float32),
                pltpu.VMEM((3, 3, 72, SIZE), jnp.float32),
                pltpu.VMEM((4, 3, 72, SIZE), jnp.float32),
                pltpu.VMEM((3, 3, 16, SIZE), jnp.float32),
                pltpu.VMEM((4, 3, 16, SIZE), jnp.float32),
                pltpu.SemaphoreType.DMA((4, 6)),
                pltpu.SemaphoreType.DMA((4, 6)),
                pltpu.SemaphoreType.DMA((3, 3)),
                pltpu.SemaphoreType.DMA((3, 3)),
                pltpu.SemaphoreType.DMA((3,)),
                pltpu.SemaphoreType.DMA((3,)),
                pltpu.SemaphoreType.DMA((5,)),
            ],
            compiler_params=pltpu.CompilerParams(collective_id=0, has_side_effects=True),
            name="advect",
        )(wind_scale, tracer, wind_a, wind_b, gain)
        return out

    field_spec = P(('member', 'panel'), 'tx', 'ty')
    wind_spec = P('panel', 'tx', 'ty')
    return jax.shard_map(local_run, mesh=mesh, in_specs=(field_spec, wind_spec, wind_spec, P()),
                         out_specs=field_spec, check_vma=False)


def kernel(own, steps, axis_names, ws_in, q_in, wa_in, wb_in, gain_in, out_ref,
           ws_ref, fields, qa, qb, sw, wf, coef, tiles, result, send, recv, csend, crecv,
           ssem, rsem, tsend, trecv, osend, orecv, isem):
    tx, ty, core = lax.axis_index('tx'), lax.axis_index('ty'), lax.axis_index('panel')
    by, bz, bx = tx, ty, lax.rem(core + tx + 1, 2)

    def place(kx, ky, kc):
        return {name: {'tx': kx, 'ty': ky, 'panel': kc}.get(name, 0) for name in axis_names}

    barrier = pltpu.get_barrier_semaphore()
    for other in range(1, 8):
        near = [1 - at if other & bit else at for at, bit in ((tx, 1), (ty, 2), (core, 4))]
        pl.semaphore_signal(barrier, inc=1, device_id=place(*near), device_id_type=MESH)
    loads = [pltpu.make_async_copy(src, dst, isem.at[n]) for n, (src, dst) in enumerate((
        (wa_in, fields.at[1]), (wb_in, fields.at[2]), (q_in, fields.at[0]), (gain_in, coef.at[0]), (ws_in, ws_ref)))]
    for load in loads:
        load.start()

    def at(ox, oy, oz):
        return place(oy, oz, lax.rem(ox + oy + 1, 2))

    def pick(first, second):
        return jnp.where(core == 0, first, second)

    homes = (
        (pick(1, tx), pick(tx, 0), ty, pick(0, 1)),
        (pick(1 - tx, 1 - ty), pick(1, tx), pick(ty, 1), pick(1, 2)),
        (pick(0, ty), pick(1 - tx, tx), pick(ty, 0), pick(0, 2)),
    )
    leaves = [jnp.logical_not((ox == bx) & (oy == by) & (oz == bz)) for ox, oy, oz, _ in homes]
    flip_a = (1 - lax.rem(bx + by, 2), lax.rem(bx + by, 2), by)
    flip_b = (bz, bz, jnp.where(bz == 1, 1 - bx, bx))
    panel = (jnp.where(bx == 1, 0, 2), jnp.where(by == 1, 1, 3), jnp.where(bz == 1, 4, 5))
    holder = [place(flip_a[n], flip_b[n], panel[n] // 3) for n in range(3)]
    slot_of = [lax.rem(panel[n], 3) for n in range(3)]
    comes = [jnp.logical_not((flip_a[n] == tx) & (flip_b[n] == ty) & (panel[n] // 3 == core)) for n in range(3)]

    def tile_copy(f, slot, quad, device):
        return pltpu.make_async_remote_copy(
            fields.at[f, slot], tiles.at[f, quad], tsend.at[f, slot], trecv.at[f, quad],
            device_id=device, device_id_type=MESH)

    for load in loads:
        load.wait()
    pl.semaphore_wait(barrier, 7)
    for f in (1, 2, 0):
        for slot in range(3):
            ox, oy, oz, quad = homes[slot]

            @pl.when(leaves[slot])
            def _():
                tile_copy(f, slot, quad, at(ox, oy, oz)).start()

            @pl.when(jnp.logical_not(leaves[slot]))
            def _():
                tiles[f, quad] = fields[f, slot]

    def placing(shape, spot_axis, to_idx, flip):
        dist = to_idx(lax.broadcasted_iota(jnp.int32, shape, spot_axis)) - LOW
        cell = lax.broadcasted_iota(jnp.int32, shape, 1 - spot_axis)
        inside = (dist >= 0) & (dist < own)
        source = jnp.where(inside, jnp.where(flip == 1, own - 1 - dist, dist), -1)
        return jnp.where(source == cell, 1.0, 0.0)

    def row_to_idx(row):
        return TILES * lax.rem(row, 8) + row // 8

    def lane_to_idx(spot):
        b = spot // 8
        half = (b + 1) // 2
        return TILES * lax.rem(spot, 8) + 8 - half + 2 * half * (1 - lax.rem(b, 2))

    def dot(lhs, rhs):
        return jnp.dot(lhs, rhs, precision=HIGHEST, preferred_element_type=jnp.float32)

    PLAIN = (0, 2, 5)

    sub = lax.broadcasted_iota(jnp.int32, (8, SIZE), 0)
    lane = lax.broadcasted_iota(jnp.int32, (8, SIZE), 1)
    lane_s, lane_i = lax.rem(lane, 8), lax.rem(lane_to_idx(lane), TILES)
    halo_lane = (lane_s >= 6) | ((lane_s == 5) & (lane_i >= 12))

    def mirror_lane(number):
        return jnp.where(lane_i < 8, 8 * (1 + 2 * lane_i) + 11 - number, 8 * (30 - 2 * lane_i) + 10 - number)

    pair_src = mirror_lane(6 + lax.rem(lane, 2))
    edge_src = jnp.where(lane_i >= 12, mirror_lane(5), 0)
    halo_src = jnp.where(halo_lane, mirror_lane(lane_s), 0)
    row_even, row_odd = 5 - lax.rem(sub, 2), 4 - lax.rem(sub, 2)
    row_pair, lane_pair = sub // 2, lane_s // 2

    def take(tile, idx, axis):
        return jnp.take_along_axis(tile, idx, axis=axis, mode="promise_in_bounds")

    def by_number(number, parts):
        res = parts[3]
        for m in (2, 1, 0):
            res = jnp.where(number == m, parts[m], res)
        return res

    def peer(mirrored):
        return at(*(1 - b if m else b for b, m in zip((bx, by, bz), mirrored)))

    def strip_copy(axis, out, slot):
        return pltpu.make_async_remote_copy(
            send.at[out, axis], recv.at[slot, axis], ssem.at[slot, axis], rsem.at[slot, axis],
            device_id=peer(tuple(int(n == axis) for n in range(3))), device_id_type=MESH)

    def corner_copy(k, out, slot):
        n = PRIMARY.index(k)
        return pltpu.make_async_remote_copy(
            csend.at[out, n], crecv.at[slot, n], ssem.at[slot, 3 + n], rsem.at[slot, 3 + n],
            device_id=peer(CORNERS[k]), device_id_type=MESH)

    def signed(sign, arr):
        return arr if sign == 1.0 else sign * arr

    def pack(arrs, k, out, sign, corner_sign):
        axis, n = STRIP_PLACE[k]
        a = tiles_of(arrs[k])
        msg = []
        for j in range(4):
            first, perm = (7, row_even) if j < 2 else (23, row_odd)
            msg.append(signed(sign, by_number(row_pair, [take(a[first - 4 * j - m], perm, 0) for m in range(4)])))
        tail = signed(sign, by_number(lax.rem(sub, 4), [take(a[11 - m], 0 * sub + 5, 0) for m in range(4)]))
        send[out, axis, 32 * n:32 * n + 32] = jnp.concatenate(msg, axis=0)
        send[out, axis, 64 + 4 * n:68 + 4 * n] = tail[4 * n:4 * n + 4]
        if k in PRIMARY:
            pairs = by_number(lane_pair, [take(m, pair_src, 1) for m in msg])
            edges = by_number(lane_s, [take(m, edge_src, 1) for m in msg])
            rest = jnp.where(halo_lane, take(tail, halo_src, 1), edges)
            csend[out, PRIMARY.index(k)] = signed(corner_sign, jnp.concatenate([pairs, rest], axis=0))

    def start_first(arrs, out, slot, sign, corner_sign):
        for k in (1, 3):
            pack(arrs, k, out, sign, corner_sign)
        strip_copy(2, out, slot).start()
        for k in (0, 2):
            pack(arrs, k, out, sign, corner_sign)
        for k in (0, 2):
            corner_copy(k, out, slot).start()

    def start_rest(arrs, out, slot, sign, corner_sign):
        for k in (4, 5):
            pack(arrs, k, out, sign, corner_sign)
        corner_copy(4, out, slot).start()
        strip_copy(1, out, slot).start()
        strip_copy(0, out, slot).start()

    def halo_tiles(k, axis, n, slot, with_corner):
        msg = [recv[slot, axis, 32 * n + 8 * j:32 * n + 8 * j + 8] for j in range(4)]
        tail = recv[slot, axis, 64:72]
        if with_corner:
            pairs, rest = crecv[slot, PRIMARY.index(k), 0:8], crecv[slot, PRIMARY.index(k), 8:16]
            edge = (lane_s == 5) & (lane_i >= 12)
            for j in range(4):
                mixed = jnp.where(lane_s >= 6, pltpu.roll(pairs, (6 - 2 * j) % SIZE, 1), msg[j])
                msg[j] = jnp.where(edge, pltpu.roll(rest, (5 - j) % SIZE, 1), mixed)
            tail = jnp.where(halo_lane, rest, tail)
        res = []
        for i in range(TILES):
            tile = roll_rows(msg[i // 4], 6 - 2 * (i % 4))
            if i >= 12:
                tile = jnp.where(sub == 5, roll_rows(tail, 17 - i - 4 * n), tile)
            res.append(tile)
        return res

    def own_rows(i):
        return sub < (6 if i < 12 else 5)

    def wait_all(out, slot):
        for axis in (0, 1):
            strip_copy(axis, out, slot).wait()
        for k in (2, 4, 0):
            corner_copy(k, out, slot).wait()
        strip_copy(2, out, slot).wait()

    def halos_of(slot):
        halos = {}
        for k in (1, 3, 5, 0, 2, 4):
            halos[k] = halo_tiles(k, *STRIP_PLACE[k], slot, k in PRIMARY)
        return halos

    def merge(arrs, k, rows, lanes):
        side = tiles_of(lanes)
        for i in range(TILES):
            new = arrs[k, 8 * i:8 * i + 8]
            if k in PRIMARY:
                new = jnp.where(own_rows(i), jnp.where(halo_lane, side[i], new), rows[i])
            else:
                new = jnp.where(halo_lane, side[i], jnp.where(own_rows(i), new, rows[i]))
            arrs[k, 8 * i:8 * i + 8] = new

    def finish(slot):
        wait_all(0, slot)
        halos = halos_of(slot)
        lanes = {TWIN[k]: turn(join(halos[k])) for k in (1, 3, 5, 0, 2, 4)}
        for k in (0, 2, 4, 1, 3, 5):
            merge(qa, k, halos[k], lanes[k])
        for k in range(6):
            near = ACROSS[k]
            qa[k, 0:1] = qa[near, 24:25]
            qa[k, 8:9] = qa[near, 16:17]

    def scale_faces(first_step):
        def one(step, carry):
            scale = ws_ref[lax.rem(first_step + step, steps)]
            sw[step] = scale * wf[...]
            return carry
        lax.fori_loop(0, BLOCK_STEPS, one, 0)

    for f in (1, 2, 0):
        for slot in range(3):
            ox, oy, oz, quad = homes[slot]

            @pl.when(leaves[slot])
            def _():
                tile_copy(f, slot, quad, at(ox, oy, oz)).wait_send()
        for quad in range(3):
            @pl.when(comes[quad])
            def _():
                tile_copy(f, 0, quad, holder[quad]).wait_recv()
        for quad in range(3):
            loc = dot(dot(placing((SIZE, own), 0, row_to_idx, flip_a[quad]), tiles[f, quad]),
                      placing((own, SIZE), 1, lane_to_idx, flip_b[quad]))
            plain, turned = PLAIN[quad], TWIN[PLAIN[quad]]
            if f == 0:
                qa[plain] = loc
                qa[turned] = turn(loc)
            elif f == 1:
                loc = jnp.where(flip_a[quad] == 1, -1.0, 1.0) * loc
                qb[plain] = loc
                sw[0, turned] = turn(loc)
            else:
                loc = jnp.where(flip_b[quad] == 1, -1.0, 1.0) * loc
                sw[0, plain] = loc
                qb[turned] = turn(loc)
        if f == 2:
            start_first(qb, 1, 2, -1.0, 1.0)
            start_rest(qb, 1, 2, -1.0, 1.0)
            start_first(sw.at[0], 2, 3, 1.0, -1.0)
            start_rest(sw.at[0], 2, 3, 1.0, -1.0)
    start_first(qa, 0, 0, 1.0, 1.0)
    start_rest(qa, 0, 0, 1.0, 1.0)

    coef[1] = 1.0 - 4.0 * coef[0]
    coef[2] = 0.5 * coef[0]
    coef[3] = 0.5 - 2.0 * coef[0]

    wait_all(1, 2)
    wait_all(2, 3)
    wind_halos, side_halos = halos_of(2), halos_of(3)
    for k in range(6):
        merge(qb, k, wind_halos[k], turn(join(side_halos[TWIN[k]])))
    for k in range(6):
        qb[k, 8:9] = -qb[ACROSS[k], 16:17]
    for k in range(6):
        here = qb[k]
        after = jnp.concatenate([here[8:], roll_rows(here[:8], -1)], axis=0)
        wf[k] = (0.5 / (6.0 * C_SPEED)) * (here + after)
    scale_faces(0)

    def x_part(a_ref, k, faces):
        a = a_ref[k]
        before = jnp.concatenate([a_ref[k, 119:127], a[:120]], axis=0)
        after = jnp.concatenate([a[8:], a_ref[k, 1:9]], axis=0)
        m = before + after
        v = 8.0 * a - m
        v_after = jnp.concatenate([v[8:], roll_rows(v[:8], -1)], axis=0)
        flux = faces * (v + v_after)
        flux_before = jnp.concatenate([roll_rows(flux[120:], 1), flux[:120]], axis=0)
        return (m - flux) + flux_before

    def parts_of(src, dst, second, step, group):
        part = {}
        for k in group:
            part[k] = coef[2 if second else 0] * x_part(src, k, sw[step, k])
            if k in PRIMARY:
                own_part = coef[3 if second else 1] * src[k]
                if second:
                    own_part = 0.5 * dst[k] + own_part
                part[k] = own_part + part[k]
        return part, {k: turn(part[k]) for k in group}

    def stage(src, dst, second, step, before_end=None):
        part, turned = {}, {}
        for group in GROUPS:
            more = parts_of(src, dst, second, step, group)
            part.update(more[0])
            turned.update(more[1])
        new = {}
        for pair in ((0, 1, 2, 3), (4, 5)):
            for k in pair:
                new[k] = part[k] + turned[TWIN[k]]
            for k in pair:
                dst[k] = new[k]
            if before_end is not None and pair == (0, 1, 2, 3):
                before_end()
        if before_end is None:
            for k in range(6):
                near = new[ACROSS[k]]
                dst[k, 0:1] = near[24:25]
                dst[k, 8:9] = near[16:17]

    def run_block(count, slot, before_end):
        finish(slot)

        def one_step(step, carry):
            stage(qa, qb, False, step)
            stage(qb, qa, True, step)
            return carry

        lax.fori_loop(0, count - 1, one_step, 0, unroll=True)
        stage(qa, qb, False, count - 1)
        stage(qb, qa, True, count - 1, before_end=before_end)

    full_blocks = (steps - 1) // BLOCK_STEPS

    def block(blk, carry):
        out_slot = lax.rem(blk + 1, 2)
        run_block(BLOCK_STEPS, lax.rem(blk, 2), functools.partial(start_first, qa, 0, out_slot, 1.0, 1.0))
        start_rest(qa, 0, out_slot, 1.0, 1.0)
        scale_faces((blk + 1) * BLOCK_STEPS)
        return carry

    lax.fori_loop(0, full_blocks, block, 0)
    run_block(steps - full_blocks * BLOCK_STEPS, full_blocks % 2, lambda: None)

    def result_copy(quad, slot, device, number):
        return pltpu.make_async_remote_copy(
            result.at[quad], out_ref.at[slot], osend.at[number], orecv.at[slot],
            device_id=device, device_id_type=MESH)

    for quad in range(3):
        result[quad] = dot(dot(placing((own, SIZE), 1, row_to_idx, flip_a[quad]), qa[PLAIN[quad]]),
                           placing((SIZE, own), 0, lane_to_idx, flip_b[quad]))

        @pl.when(comes[quad])
        def _():
            result_copy(quad, slot_of[quad], holder[quad], quad).start()

        @pl.when(jnp.logical_not(comes[quad]))
        def _():
            pltpu.make_async_copy(result.at[quad], out_ref.at[slot_of[quad]], osend.at[quad]).start()

    for quad in range(3):
        @pl.when(comes[quad])
        def _():
            result_copy(quad, slot_of[quad], holder[quad], quad).wait_send()

        @pl.when(jnp.logical_not(comes[quad]))
        def _():
            pltpu.make_async_copy(result.at[quad], out_ref.at[slot_of[quad]], osend.at[quad]).wait()
    for slot in range(3):
        ox, oy, oz, _ = homes[slot]

        @pl.when(leaves[slot])
        def _():
            result_copy(0, slot, at(ox, oy, oz), 0).wait_recv()
```

```python
import functools
import math

import jax
import jax.numpy as jnp
import numpy as np
from jax import lax
from jax.experimental import pallas as pl
from jax.experimental.pallas import tpu as pltpu
from jax.sharding import PartitionSpec as P

C_SPEED = 2.5
CFL_STEP = 0.12
MESH = pl.DeviceIdType.MESH
HIGHEST = lax.Precision.HIGHEST

TWIN = (1, 0, 3, 2, 5, 4)
ACROSS = (2, 4, 0, 5, 1, 3)
PRIMARY = (0, 2, 4)
STRIPS = ((2, 4), (0, 5), (1, 3))
STRIP_PLACE = {k: (axis, n) for axis in range(3) for n, k in enumerate(STRIPS[axis])}
CORNERS = {0: (0, 1, 1), 2: (1, 0, 1), 4: (1, 1, 0)}

SIZE = 128
TILES = 16
LOW = 2
OWN = 90
BLOCK_STEPS = 9
LANE_ORDER = (8, 7, 9, 6, 10, 5, 11, 4, 12, 3, 13, 2, 14, 1, 15, 0)
GROUPS = ((0, 2), (1, 3), (4, 5))


def row_idx(row):
    return TILES * (row % 8) + row // 8


def lane_group(b):
    half = (b + 1) // 2
    return 8 - half + 2 * half * (1 - b % 2)


def tile(i, offset=0):
    return pl.ds(8 * i + offset, 8)


def row(i, offset=0):
    return pl.ds(8 * i + offset, 1)


def tiles_of(arr):
    return jnp.split(arr, arr.shape[0] // 8)


def join(tiles):
    return jnp.concatenate(tiles)


def roll_rows(tile, shift):
    return pltpu.roll(tile, shift % 8, 0)


def turn(arr):
    tiles = tiles_of(arr)
    turned = tiles_of(join([tiles[i] for i in LANE_ORDER]).T)
    return join([turned[LANE_ORDER.index(i)] for i in range(TILES)])


def solution(mesh):
    axis_names = mesh.axis_names

    def local_run(tracer, wind_a, wind_b, wind_scale):
        own = tracer.shape[1]
        cells = 2 * own
        steps = wind_scale.shape[0]
        dalpha = 0.5 * math.pi / cells
        place = np.arange(SIZE)
        lane_idx = TILES * (place % 8) + lane_group(place // 8)
        tan_a = np.tan((row_idx(place) - LOW + 0.5) * dalpha - 0.25 * math.pi)[:, None]
        tan_b = np.tan((lane_idx - LOW + 0.5) * dalpha - 0.25 * math.pi)[None, :]
        r_sq = 1.0 + tan_a * tan_a + tan_b * tan_b
        inv_sqrt_g = r_sq * np.sqrt(r_sq) / ((1.0 + tan_a * tan_a) * (1.0 + tan_b * tan_b))
        gain = (0.5 * C_SPEED * CFL_STEP * inv_sqrt_g).astype(np.float32)
        out = pl.pallas_call(
            functools.partial(kernel, own, steps, axis_names),
            out_shape=jax.ShapeDtypeStruct(tracer.shape, jnp.float32),
            in_specs=[pl.BlockSpec(memory_space=pl.ANY)] * 5,
            out_specs=pl.BlockSpec(memory_space=pl.ANY),
            scratch_shapes=[
                pltpu.SMEM((steps,), jnp.float32),
                pltpu.VMEM((3, 3, own, own), jnp.float32),
                pltpu.VMEM((6, SIZE, SIZE), jnp.float32),
                pltpu.VMEM((6, SIZE, SIZE), jnp.float32),
                pltpu.VMEM((BLOCK_STEPS, 6, SIZE, SIZE), jnp.float32),
                pltpu.VMEM((6, SIZE, SIZE), jnp.float32),
                pltpu.VMEM((4, SIZE, SIZE), jnp.float32),
                pltpu.VMEM((3, 3, own, own), jnp.float32),
                pltpu.VMEM((3, own, own), jnp.float32),
                pltpu.VMEM((3, 3, 72, SIZE), jnp.float32),
                pltpu.VMEM((4, 3, 72, SIZE), jnp.float32),
                pltpu.VMEM((3, 3, 8, SIZE), jnp.float32),
                pltpu.VMEM((4, 3, 8, SIZE), jnp.float32),
                pltpu.SemaphoreType.DMA((4, 6)),
                pltpu.SemaphoreType.DMA((4, 6)),
                pltpu.SemaphoreType.DMA((3, 3)),
                pltpu.SemaphoreType.DMA((3, 3)),
                pltpu.SemaphoreType.DMA((3,)),
                pltpu.SemaphoreType.DMA((3,)),
                pltpu.SemaphoreType.DMA((5,)),
            ],
            compiler_params=pltpu.CompilerParams(collective_id=0, has_side_effects=True),
            name="advect",
        )(wind_scale, tracer, wind_a, wind_b, gain)
        return out

    field_spec = P(('member', 'panel'), 'tx', 'ty')
    wind_spec = P('panel', 'tx', 'ty')
    return jax.shard_map(local_run, mesh=mesh, in_specs=(field_spec, wind_spec, wind_spec, P()),
                         out_specs=field_spec, check_vma=False)


def kernel(own, steps, axis_names, ws_in, q_in, wa_in, wb_in, gain_in, out_ref,
           ws_ref, fields, qa, qb, sw, wf, coef, tiles, result, send, recv, csend, crecv,
           ssem, rsem, tsend, trecv, osend, orecv, isem):
    tx, ty, core = lax.axis_index('tx'), lax.axis_index('ty'), lax.axis_index('panel')
    by, bz, bx = tx, ty, lax.rem(core + tx + 1, 2)

    def place(kx, ky, kc):
        return {name: {'tx': kx, 'ty': ky, 'panel': kc}.get(name, 0) for name in axis_names}

    barrier = pltpu.get_barrier_semaphore()
    for other in range(1, 8):
        near = [1 - at if other & bit else at for at, bit in ((tx, 1), (ty, 2), (core, 4))]
        pl.semaphore_signal(barrier, inc=1, device_id=place(*near), device_id_type=MESH)
    loads = [pltpu.make_async_copy(src, dst, isem.at[n]) for n, (src, dst) in enumerate((
        (wa_in, fields.at[1]), (wb_in, fields.at[2]), (q_in, fields.at[0]), (gain_in, coef.at[0]), (ws_in, ws_ref)))]
    for load in loads:
        load.start()

    def at(ox, oy, oz):
        return place(oy, oz, lax.rem(ox + oy + 1, 2))

    def pick(first, second):
        return jnp.where(core == 0, first, second)

    homes = (
        (pick(1, tx), pick(tx, 0), ty, pick(0, 1)),
        (pick(1 - tx, 1 - ty), pick(1, tx), pick(ty, 1), pick(1, 2)),
        (pick(0, ty), pick(1 - tx, tx), pick(ty, 0), pick(0, 2)),
    )
    leaves = [jnp.logical_not((ox == bx) & (oy == by) & (oz == bz)) for ox, oy, oz, _ in homes]
    flip_a = (1 - lax.rem(bx + by, 2), lax.rem(bx + by, 2), by)
    flip_b = (bz, bz, jnp.where(bz == 1, 1 - bx, bx))
    panel = (jnp.where(bx == 1, 0, 2), jnp.where(by == 1, 1, 3), jnp.where(bz == 1, 4, 5))
    holder = [place(flip_a[n], flip_b[n], panel[n] // 3) for n in range(3)]
    slot_of = [lax.rem(panel[n], 3) for n in range(3)]
    comes = [jnp.logical_not((flip_a[n] == tx) & (flip_b[n] == ty) & (panel[n] // 3 == core)) for n in range(3)]

    def tile_copy(f, slot, quad, device):
        return pltpu.make_async_remote_copy(
            fields.at[f, slot], tiles.at[f, quad], tsend.at[f, slot], trecv.at[f, quad],
            device_id=device, device_id_type=MESH)

    for load in loads:
        load.wait()
    pl.semaphore_wait(barrier, 7)
    for f in (1, 2, 0):
        for slot in range(3):
            ox, oy, oz, quad = homes[slot]

            @pl.when(leaves[slot])
            def _():
                tile_copy(f, slot, quad, at(ox, oy, oz)).start()

            @pl.when(jnp.logical_not(leaves[slot]))
            def _():
                tiles[f, quad] = fields[f, slot]

    def placing(shape, spot_axis, to_idx, flip):
        dist = to_idx(lax.broadcasted_iota(jnp.int32, shape, spot_axis)) - LOW
        cell = lax.broadcasted_iota(jnp.int32, shape, 1 - spot_axis)
        inside = (dist >= 0) & (dist < own)
        source = jnp.where(inside, jnp.where(flip == 1, own - 1 - dist, dist), -1)
        return jnp.where(source == cell, 1.0, 0.0)

    def row_to_idx(row):
        return TILES * lax.rem(row, 8) + row // 8

    def lane_to_idx(spot):
        b = spot // 8
        half = (b + 1) // 2
        return TILES * lax.rem(spot, 8) + 8 - half + 2 * half * (1 - lax.rem(b, 2))

    def dot(lhs, rhs):
        return jnp.dot(lhs, rhs, precision=HIGHEST, preferred_element_type=jnp.float32)

    PLAIN = (0, 2, 5)

    sub = lax.broadcasted_iota(jnp.int32, (8, SIZE), 0)
    lane = lax.broadcasted_iota(jnp.int32, (8, SIZE), 1)
    lane_s, lane_i = lax.rem(lane, 8), lax.rem(lane_to_idx(lane), TILES)
    halo_lane = (lane_s >= 6) | ((lane_s == 5) & (lane_i >= 12))

    def mirror_lane(number):
        return jnp.where(lane_i < 8, 8 * (1 + 2 * lane_i) + 11 - number, 8 * (30 - 2 * lane_i) + 10 - number)

    odd_row, odd_lane = lax.rem(sub, 2), lax.rem(lane, 2)
    pair_src = mirror_lane(6 + odd_lane)
    row_pair, lane_pair = sub // 2, lane_s // 2
    late_group = lane_i >= 14
    from_twin = (lane_pair == 2) | ((lane_pair == 3) & jnp.logical_not(late_group))
    twin_src = jnp.where(from_twin, mirror_lane(4 + lane_pair), 0)
    inner_src = jnp.where(lane_pair == 3, mirror_lane(5), 8 * (34 - 2 * lane_i) + 5)
    primary_src = jnp.where(from_twin, 0, jnp.where((lane_pair > 0) & late_group, inner_src, mirror_lane(6 + lane_pair)))
    inner_lane = jnp.where(late_group, 16 * lane_i - 121, 16 * lane_i - 93)
    primary_back = jnp.where(lane_s == 6, lane - 5, jnp.where(lane_s == 7, lane - 4, jnp.where(halo_lane, inner_lane, 0)))
    twin_back = jnp.where(lane_s == 6, lane - 1, lane)

    def rows_by(arr, idx):
        return jnp.take_along_axis(arr, idx, axis=0, mode="promise_in_bounds")

    def lanes_by(arr, idx):
        return jnp.take_along_axis(arr, idx, axis=1, mode="promise_in_bounds")

    def by_number(number, parts):
        res = parts[3]
        for m in (2, 1, 0):
            res = jnp.where(number == m, parts[m], res)
        return res

    def peer(mirrored):
        return at(*(1 - b if m else b for b, m in zip((bx, by, bz), mirrored)))

    def strip_copy(axis, out, slot):
        return pltpu.make_async_remote_copy(
            send.at[out, axis], recv.at[slot, axis], ssem.at[slot, axis], rsem.at[slot, axis],
            device_id=peer(tuple(int(n == axis) for n in range(3))), device_id_type=MESH)

    def corner_copy(k, out, slot):
        n = PRIMARY.index(k)
        return pltpu.make_async_remote_copy(
            csend.at[out, n], crecv.at[slot, n], ssem.at[slot, 3 + n], rsem.at[slot, 3 + n],
            device_id=peer(CORNERS[k]), device_id_type=MESH)

    def signed(sign, arr):
        return arr if sign == 1.0 else sign * arr

    def pack(arrs, k, out, sign):
        axis, n = STRIP_PLACE[k]
        a = tiles_of(arrs[k])
        msg = []
        for j in range(4):
            first, sublane = (7, 5 - odd_row) if j < 2 else (23, 4 - odd_row)
            msg.append(signed(sign, by_number(row_pair, [rows_by(a[first - 4 * j - m], sublane) for m in range(4)])))
        tail = signed(sign, by_number(lax.rem(sub, 4), [rows_by(a[11 - m], 5 + 0 * sub) for m in range(4)]))
        send[out, axis, pl.ds(32 * n, 32)] = join(msg)
        send[out, axis, pl.ds(64 + 4 * n, 4)] = tail[4 * n:4 * n + 4]
        return msg, tail

    def pack_pair(arrs, k, out, sign, corner_sign, twin_tail):
        msg, tail = pack(arrs, k, out, sign)
        pairs = by_number(lane_pair, [lanes_by(m, pair_src) for m in msg])
        inner = jnp.where(from_twin, lanes_by(rows_by(twin_tail, row_pair), twin_src), lanes_by(rows_by(tail, row_pair), primary_src))
        csend[out, PRIMARY.index(k)] = signed(corner_sign, jnp.where(odd_row * odd_lane == 1, inner, pairs))

    def start_first(arrs, out, slot, sign, corner_sign):
        tails = [pack(arrs, k, out, sign)[1] for k in (1, 3)]
        strip_copy(2, out, slot).start()
        for k, tail in zip((0, 2), tails):
            pack_pair(arrs, k, out, sign, corner_sign, tail)
        for k in (0, 2):
            corner_copy(k, out, slot).start()

    def start_rest(arrs, out, slot, sign, corner_sign):
        pack_pair(arrs, 4, out, sign, corner_sign, pack(arrs, 5, out, sign)[1])
        corner_copy(4, out, slot).start()
        strip_copy(1, out, slot).start()
        strip_copy(0, out, slot).start()

    def halo_tiles(k, slot):
        axis, n = STRIP_PLACE[k]
        msg = [recv[slot, axis, tile(j, 32 * n)] for j in range(4)]
        tail = recv[slot, axis, pl.ds(64, 8)]
        corner = crecv[slot, k // 2]
        inner = rows_by(corner, 2 * lax.rem(sub, 4) + 1)
        if k in PRIMARY:
            tail = jnp.where(halo_lane, lanes_by(inner, primary_back), tail)
            msg = [jnp.where(lane_s >= 6, pltpu.roll(corner, (6 - 2 * j) % SIZE, 1), msg[j]) for j in range(4)]
        else:
            tail = jnp.where(lane_s >= 6, lanes_by(inner, twin_back), tail)
        res = [roll_rows(msg[i // 4], 6 - 2 * (i % 4)) for i in range(TILES)]
        for i in range(12, TILES):
            res[i] = jnp.where(sub == 5, roll_rows(tail, 17 - i - 4 * n), res[i])
        return res

    def wait_all(out, slot):
        for axis in (0, 1):
            strip_copy(axis, out, slot).wait()
        for k in (2, 4, 0):
            corner_copy(k, out, slot).wait()
        strip_copy(2, out, slot).wait()

    inner_edge = halo_lane & (lane_s == 5)

    def merge(arrs, k, rows, lanes):
        side = tiles_of(lanes)
        for i in range(TILES):
            own_rows = sub < (6 if i < 12 else 5)
            if k in PRIMARY:
                sideways = (halo_lane & own_rows) | (inner_edge & (sub >= 6))
            else:
                sideways = halo_lane if i < 12 else halo_lane & ((sub != 5) | inner_edge)
            arrs[k, tile(i)] = jnp.where(sideways, side[i], jnp.where(own_rows, arrs[k, tile(i)], rows[i]))

    def ghosts_from(dst, src):
        for k in range(6):
            near = src[ACROSS[k]]
            dst[k, row(0)] = near[24:25]
            dst[k, row(1)] = near[16:17]

    def finish(slot):
        wait_all(0, slot)
        halos = {k: halo_tiles(k, slot) for k in (1, 3, 5, 0, 2, 4)}
        lanes = {TWIN[k]: turn(join(halos[k])) for k in (1, 3, 5, 0, 2, 4)}
        for k in (0, 2, 4, 1, 3, 5):
            merge(qa, k, halos[k], lanes[k])
        ghosts_from(qa, [qa[k, pl.ds(0, 32)] for k in range(6)])

    def scale_faces(first_step):
        def one(step, carry):
            scale = ws_ref[lax.rem(first_step + step, steps)]
            sw[step] = scale * wf[...]
            return carry
        lax.fori_loop(0, BLOCK_STEPS, one, 0)

    for f in (1, 2, 0):
        for slot in range(3):
            ox, oy, oz, quad = homes[slot]

            @pl.when(leaves[slot])
            def _():
                tile_copy(f, slot, quad, at(ox, oy, oz)).wait_send()
        for quad in range(3):
            @pl.when(comes[quad])
            def _():
                tile_copy(f, 0, quad, holder[quad]).wait_recv()
        for quad in range(3):
            loc = dot(dot(placing((SIZE, own), 0, row_to_idx, flip_a[quad]), tiles[f, quad]),
                      placing((own, SIZE), 1, lane_to_idx, flip_b[quad]))
            plain, turned = PLAIN[quad], TWIN[PLAIN[quad]]
            if f == 0:
                qa[plain] = loc
                qa[turned] = turn(loc)
            elif f == 1:
                loc = jnp.where(flip_a[quad] == 1, -1.0, 1.0) * loc
                qb[plain] = loc
                sw[0, turned] = turn(loc)
            else:
                loc = jnp.where(flip_b[quad] == 1, -1.0, 1.0) * loc
                sw[0, plain] = loc
                qb[turned] = turn(loc)
        if f == 2:
            start_first(qb, 1, 2, -1.0, 1.0)
            start_rest(qb, 1, 2, -1.0, 1.0)
            start_first(sw.at[0], 2, 3, 1.0, -1.0)
            start_rest(sw.at[0], 2, 3, 1.0, -1.0)
    start_first(qa, 0, 0, 1.0, 1.0)
    start_rest(qa, 0, 0, 1.0, 1.0)

    coef[1] = 1.0 - 4.0 * coef[0]
    coef[2] = 0.5 * coef[0]
    coef[3] = 0.5 - 2.0 * coef[0]

    wait_all(1, 2)
    wait_all(2, 3)
    for k in range(6):
        merge(qb, k, halo_tiles(k, 2), turn(join(halo_tiles(TWIN[k], 3))))
    for k in range(6):
        qb[k, row(1)] = -qb[ACROSS[k], row(2)]
    for k in range(6):
        here = qb[k]
        after = join([here[8:], roll_rows(here[:8], -1)])
        wf[k] = (0.5 / (6.0 * C_SPEED)) * (here + after)
    scale_faces(0)

    def x_part(a_ref, k, faces):
        a = a_ref[k]
        before = join([a_ref[k, tile(15, -1)], a[:-8]])
        after = join([a[8:], a_ref[k, tile(0, 1)]])
        m = before + after
        v = 8.0 * a - m
        flux = faces * (v + join([v[8:], roll_rows(v[:8], -1)]))
        return (m - flux) + join([roll_rows(flux[-8:], 1), flux[:-8]])

    def parts_of(src, dst, second, step, group):
        part = {}
        for k in group:
            part[k] = coef[2 if second else 0] * x_part(src, k, sw[step, k])
            if k in PRIMARY:
                own_part = coef[3 if second else 1] * src[k]
                if second:
                    own_part = 0.5 * dst[k] + own_part
                part[k] = own_part + part[k]
        return part, {k: turn(part[k]) for k in group}

    def stage(src, dst, second, step, before_end=None):
        part, turned = {}, {}
        for group in GROUPS:
            more = parts_of(src, dst, second, step, group)
            part.update(more[0])
            turned.update(more[1])
        new = {}
        for pair in ((0, 1, 2, 3), (4, 5)):
            for k in pair:
                new[k] = part[k] + turned[TWIN[k]]
            for k in pair:
                dst[k] = new[k]
            if before_end is not None and pair == (0, 1, 2, 3):
                before_end()
        if before_end is None:
            ghosts_from(dst, new)

    def run_block(count, slot, before_end):
        finish(slot)

        def one_step(step, carry):
            stage(qa, qb, False, step)
            stage(qb, qa, True, step)
            return carry

        lax.fori_loop(0, count - 1, one_step, 0, unroll=True)
        stage(qa, qb, False, count - 1)
        stage(qb, qa, True, count - 1, before_end=before_end)

    full_blocks = (steps - 1) // BLOCK_STEPS

    def block(blk, carry):
        out_slot = lax.rem(blk + 1, 2)
        run_block(BLOCK_STEPS, lax.rem(blk, 2), functools.partial(start_first, qa, 0, out_slot, 1.0, 1.0))
        start_rest(qa, 0, out_slot, 1.0, 1.0)
        scale_faces((blk + 1) * BLOCK_STEPS)
        return carry

    lax.fori_loop(0, full_blocks, block, 0)
    run_block(steps - full_blocks * BLOCK_STEPS, full_blocks % 2, lambda: None)

    def result_copy(quad, slot, device, number):
        return pltpu.make_async_remote_copy(
            result.at[quad], out_ref.at[slot], osend.at[number], orecv.at[slot],
            device_id=device, device_id_type=MESH)

    for quad in range(3):
        result[quad] = dot(dot(placing((own, SIZE), 1, row_to_idx, flip_a[quad]), qa[PLAIN[quad]]),
                           placing((SIZE, own), 0, lane_to_idx, flip_b[quad]))

        @pl.when(comes[quad])
        def _():
            result_copy(quad, slot_of[quad], holder[quad], quad).start()

        @pl.when(jnp.logical_not(comes[quad]))
        def _():
            pltpu.make_async_copy(result.at[quad], out_ref.at[slot_of[quad]], osend.at[quad]).start()

    for quad in range(3):
        @pl.when(comes[quad])
        def _():
            result_copy(quad, slot_of[quad], holder[quad], quad).wait_send()

        @pl.when(jnp.logical_not(comes[quad]))
        def _():
            pltpu.make_async_copy(result.at[quad], out_ref.at[slot_of[quad]], osend.at[quad]).wait()
    for slot in range(3):
        ox, oy, oz, _ = homes[slot]

        @pl.when(leaves[slot])
        def _():
            result_copy(0, slot, at(ox, oy, oz), 0).wait_recv()
```

```python
import functools
import math

import jax
import jax.numpy as jnp
import numpy as np
from jax import lax
from jax.experimental import pallas as pl
from jax.experimental.pallas import tpu as pltpu
from jax.sharding import PartitionSpec as P

C_SPEED = 2.5
CFL_STEP = 0.12
MESH = pl.DeviceIdType.MESH
HIGHEST = lax.Precision.HIGHEST

TWIN = tuple(k ^ 1 for k in range(6))
ACROSS = (2, 4, 0, 5, 1, 3)
PRIMARY = (0, 2, 4)
STRIPS = ((2, 4), (0, 5), (1, 3))
STRIP_PLACE = {k: (axis, n) for axis, pair in enumerate(STRIPS) for n, k in enumerate(pair)}
CORNERS = {0: (0, 1, 1), 2: (1, 0, 1), 4: (1, 1, 0)}

SIZE = 128
TILES = 16
EDGE = 10
BLOCK_STEPS = 10
GROUPS = ((0, 2), (1, 3), (4, 5))


def row_idx(row):
    return TILES * (row % 8) + row // 8


def lane_group(b):
    half = (b + 1) // 2
    return 8 - half + 2 * half * (1 - b % 2)


LANE_ORDER = tuple(lane_group(b) for b in range(TILES))


def tile(i):
    return pl.ds(8 * i, 8)


def row(i, sublane=0):
    return pl.ds(8 * i + sublane, 1)


def tiles_of(arr):
    return jnp.split(arr, arr.shape[0] // 8)


def join(tiles):
    return jnp.concatenate(tiles)


def roll_rows(tile, shift):
    return pltpu.roll(tile, shift % 8, 0)


def turn(arr):
    tiles = tiles_of(arr)
    turned = tiles_of(join([tiles[i] for i in LANE_ORDER]).T)
    return join([turned[LANE_ORDER.index(i)] for i in range(TILES)])


def solution(mesh):
    axis_names = mesh.axis_names

    def local_run(tracer, wind_a, wind_b, wind_scale):
        own = tracer.shape[1]
        cells = 2 * own
        steps = wind_scale.shape[0]
        dalpha = 0.5 * math.pi / cells
        place = np.arange(SIZE)
        lane_idx = TILES * (place % 8) + lane_group(place // 8)
        tan_a = np.tan((row_idx(place) + 0.5) * dalpha - 0.25 * math.pi)[:, None]
        tan_b = np.tan((lane_idx + 0.5) * dalpha - 0.25 * math.pi)[None, :]
        r_sq = 1.0 + tan_a * tan_a + tan_b * tan_b
        inv_sqrt_g = r_sq * np.sqrt(r_sq) / ((1.0 + tan_a * tan_a) * (1.0 + tan_b * tan_b))
        gain = (0.5 * C_SPEED * CFL_STEP * inv_sqrt_g).astype(np.float32)
        out = pl.pallas_call(
            functools.partial(kernel, own, steps, axis_names),
            out_shape=jax.ShapeDtypeStruct(tracer.shape, jnp.float32),
            in_specs=[pl.BlockSpec(memory_space=pl.ANY)] * 5,
            out_specs=pl.BlockSpec(memory_space=pl.ANY),
            scratch_shapes=[
                pltpu.SMEM((steps,), jnp.float32),
                pltpu.VMEM((3, 3, own, own), jnp.float32),
                pltpu.VMEM((6, SIZE, SIZE), jnp.float32),
                pltpu.VMEM((6, SIZE, SIZE), jnp.float32),
                pltpu.VMEM((BLOCK_STEPS, 6, SIZE, SIZE), jnp.float32),
                pltpu.VMEM((6, SIZE, SIZE), jnp.float32),
                pltpu.VMEM((6, 8, SIZE), jnp.float32),
                pltpu.VMEM((4, SIZE, SIZE), jnp.float32),
                pltpu.VMEM((3, 3, own, own), jnp.float32),
                pltpu.VMEM((3, own, own), jnp.float32),
                pltpu.VMEM((3, 6, 40, SIZE), jnp.float32),
                pltpu.VMEM((4, 6, 40, SIZE), jnp.float32),
                pltpu.VMEM((3, 3, 16, SIZE), jnp.float32),
                pltpu.VMEM((4, 3, 16, SIZE), jnp.float32),
            ] + [pltpu.SemaphoreType.DMA(shape) for shape in ((4, 6), (3, 3), (3,)) for _ in range(2)] + [
                pltpu.SemaphoreType.DMA((5,)),
            ],
            compiler_params=pltpu.CompilerParams(collective_id=0, has_side_effects=True),
            name="advect",
        )(wind_scale, tracer, wind_a, wind_b, gain)
        return out

    field_spec = P(('member', 'panel'), 'tx', 'ty')
    wind_spec = P('panel', 'tx', 'ty')
    return jax.shard_map(local_run, mesh=mesh, in_specs=(field_spec, wind_spec, wind_spec, P()),
                         out_specs=field_spec, check_vma=False)


def kernel(own, steps, axis_names, ws_in, q_in, wa_in, wb_in, gain_in, out_ref,
           ws_ref, fields, qa, qb, sw, wf, wlast, coef, tiles, result, send, recv, csend, crecv,
           ssem, rsem, tsend, trecv, osend, orecv, isem):
    tx, ty, core = lax.axis_index('tx'), lax.axis_index('ty'), lax.axis_index('panel')
    by, bz, bx = tx, ty, lax.rem(core + tx + 1, 2)

    def place(kx, ky, kc):
        return {name: {'tx': kx, 'ty': ky, 'panel': kc}.get(name, 0) for name in axis_names}

    barrier = pltpu.get_barrier_semaphore()
    for other in range(1, 8):
        near = [1 - at if other & bit else at for at, bit in ((tx, 1), (ty, 2), (core, 4))]
        pl.semaphore_signal(barrier, inc=1, device_id=place(*near), device_id_type=MESH)
    loads = [pltpu.make_async_copy(src, dst, isem.at[n]) for n, (src, dst) in enumerate((
        (wa_in, fields.at[1]), (wb_in, fields.at[2]), (q_in, fields.at[0]), (gain_in, coef.at[0]), (ws_in, ws_ref)))]
    for load in loads:
        load.start()

    def at(ox, oy, oz):
        return place(oy, oz, lax.rem(ox + oy + 1, 2))

    def pick(first, second):
        return jnp.where(core == 0, first, second)

    homes = (
        (pick(1, tx), pick(tx, 0), ty, pick(0, 1)),
        (pick(1 - tx, 1 - ty), pick(1, tx), pick(ty, 1), pick(1, 2)),
        (pick(0, ty), pick(1 - tx, tx), pick(ty, 0), pick(0, 2)),
    )
    leaves = [jnp.logical_not((ox == bx) & (oy == by) & (oz == bz)) for ox, oy, oz, _ in homes]
    flip_a = (1 - lax.rem(bx + by, 2), lax.rem(bx + by, 2), by)
    flip_b = (bz, bz, jnp.where(bz == 1, 1 - bx, bx))
    panel = (jnp.where(bx == 1, 0, 2), jnp.where(by == 1, 1, 3), jnp.where(bz == 1, 4, 5))
    holder = [place(flip_a[n], flip_b[n], panel[n] // 3) for n in range(3)]
    slot_of = [lax.rem(panel[n], 3) for n in range(3)]
    comes = [jnp.logical_not((flip_a[n] == tx) & (flip_b[n] == ty) & (panel[n] // 3 == core)) for n in range(3)]

    def tile_copy(f, slot, quad, device):
        return pltpu.make_async_remote_copy(
            fields.at[f, slot], tiles.at[f, quad], tsend.at[f, slot], trecv.at[f, quad],
            device_id=device, device_id_type=MESH)

    for load in loads:
        load.wait()
    pl.semaphore_wait(barrier, 7)
    for f in (1, 2, 0):
        for slot in range(3):
            ox, oy, oz, quad = homes[slot]

            @pl.when(leaves[slot])
            def _():
                tile_copy(f, slot, quad, at(ox, oy, oz)).start()

            @pl.when(jnp.logical_not(leaves[slot]))
            def _():
                tiles[f, quad] = fields[f, slot]

    def placing(shape, spot_axis, to_idx, flip):
        dist = to_idx(lax.broadcasted_iota(jnp.int32, shape, spot_axis))
        cell = lax.broadcasted_iota(jnp.int32, shape, 1 - spot_axis)
        source = jnp.where(dist < own, jnp.where(flip == 1, own - 1 - dist, dist), -1)
        return jnp.where(source == cell, 1.0, 0.0)

    def row_to_idx(row):
        return TILES * lax.rem(row, 8) + row // 8

    def lane_to_idx(spot):
        b = spot // 8
        half = (b + 1) // 2
        return TILES * lax.rem(spot, 8) + 8 - half + 2 * half * (1 - lax.rem(b, 2))

    def dot(lhs, rhs):
        return jnp.dot(lhs, rhs, precision=HIGHEST, preferred_element_type=jnp.float32)

    PLAIN = (0, 2, 5)

    sub = lax.broadcasted_iota(jnp.int32, (8, SIZE), 0)
    lane = lax.broadcasted_iota(jnp.int32, (8, SIZE), 1)
    lane_s, lane_i = lax.rem(lane, 8), lax.rem(lane_to_idx(lane), TILES)
    edge_lane = (lane_s == 5) & (lane_i >= EDGE)
    halo_lane = (lane_s >= 6) | edge_lane

    def mirror_lane(number):
        there = lax.rem(19 - lane_i, TILES)
        group = jnp.where(there < 8, 15 - 2 * there, 2 * there - TILES)
        return 8 * group + jnp.where(lane_i < 4, 11, EDGE) - number

    odd_row = lax.rem(sub, 2)
    pair_src = mirror_lane(6 + lax.rem(lane, 2))
    twin_src = jnp.where(lane_s < 2, mirror_lane(6 + lane_s), 0)
    tail_src = jnp.where(halo_lane, mirror_lane(lane_s), 0)
    row_pair, lane_pair = sub // 2, lane_s // 2

    def rows_by(arr, idx):
        return jnp.take_along_axis(arr, idx, axis=0, mode="promise_in_bounds")

    def lanes_by(arr, idx):
        return jnp.take_along_axis(arr, idx, axis=1, mode="promise_in_bounds")

    def by_number(number, parts):
        res = parts[0]
        for m, part in enumerate(parts):
            res = jnp.where(number == m, part, res) if m else res
        return res

    def peer(mirrored):
        return at(*(1 - b if m else b for b, m in zip((bx, by, bz), mirrored)))

    def strip_copy(axis, out, slot):
        return pltpu.make_async_remote_copy(
            send.at[out, pl.ds(2 * axis, 2)], recv.at[slot, pl.ds(2 * axis, 2)], ssem.at[slot, axis], rsem.at[slot, axis],
            device_id=peer(tuple(int(n == axis) for n in range(3))), device_id_type=MESH)

    def corner_copy(k, out, slot):
        n = PRIMARY.index(k)
        return pltpu.make_async_remote_copy(
            csend.at[out, n], crecv.at[slot, n], ssem.at[slot, 3 + n], rsem.at[slot, 3 + n],
            device_id=peer(CORNERS[k]), device_id_type=MESH)

    def signed(sign, arr):
        return arr if sign == 1.0 else sign * arr

    def pack(arrs, k, out, sign):
        axis, n = STRIP_PLACE[k]
        a = tiles_of(arrs[k])

        def mirrored(i, sublane):
            return rows_by(a[(19 - i) % TILES], sublane)

        msg = [by_number(row_pair, [mirrored(i, (5 if i < 4 else 4) - odd_row) for i in range(4 * j, 4 * j + 4)])
               for j in range(4)]
        tail = [mirrored(i, 5 + 0 * sub) for i in range(EDGE, TILES)] + [mirrored(i, 3 + 0 * sub) for i in range(2)]
        msg = [signed(sign, part) for part in msg + [by_number(sub, tail)]]
        send[out, 2 * axis + n] = join(msg)
        return msg

    def pack_pair(arrs, k, out, sign, corner_sign, twin_tail):
        *msg, tail = pack(arrs, k, out, sign)
        pairs = by_number(lane_pair, [lanes_by(m, pair_src) for m in msg])
        near = jnp.where(lane_s < 2, lanes_by(twin_tail, twin_src), lanes_by(tail, tail_src))
        csend[out, k // 2] = signed(corner_sign, join([pairs, near]))

    def start_first(arrs, out, slot, sign, corner_sign):
        tails = [pack(arrs, k, out, sign)[-1] for k in (1, 3)]
        strip_copy(2, out, slot).start()
        for k, tail in zip((0, 2), tails):
            pack_pair(arrs, k, out, sign, corner_sign, tail)
        for k in (0, 2):
            corner_copy(k, out, slot).start()

    def start_rest(arrs, out, slot, sign, corner_sign):
        pack_pair(arrs, 4, out, sign, corner_sign, pack(arrs, 5, out, sign)[-1])
        corner_copy(4, out, slot).start()
        strip_copy(1, out, slot).start()
        strip_copy(0, out, slot).start()

    def strip(k, slot):
        axis, n = STRIP_PLACE[k]
        return tiles_of(recv[slot, 2 * axis + n])

    def halo_tiles(k, slot):
        *msg, tail = strip(k, slot)
        pairs, near = tiles_of(crecv[slot, k // 2])
        if k in PRIMARY:
            tail = jnp.where(halo_lane, near, tail)
            msg = [jnp.where(lane_s >= 6, pltpu.roll(pairs, (6 - 2 * j) % SIZE, 1), msg[j]) for j in range(4)]
        else:
            tail = jnp.where(lane_s >= 6, pltpu.roll(near, 6, 1), tail)
        res = [roll_rows(msg[i // 4], 6 - 2 * (i % 4)) for i in range(TILES)]
        for i in range(EDGE, TILES):
            res[i] = jnp.where(sub == 5, roll_rows(tail, 15 - i), res[i])
        return res

    def wait_all(out, slot):
        for axis in (0, 1):
            strip_copy(axis, out, slot).wait()
        for k in (2, 4, 0):
            corner_copy(k, out, slot).wait()
        strip_copy(2, out, slot).wait()

    def merge(arrs, k, rows, lanes):
        side = tiles_of(lanes)
        for i in range(TILES):
            own_rows = sub < (6 if i < EDGE else 5)
            if k in PRIMARY:
                sideways = (halo_lane & own_rows) | (edge_lane & (sub >= 6))
            else:
                sideways = halo_lane if i < EDGE else halo_lane & ((sub != 5) | edge_lane)
            arrs[k, tile(i)] = jnp.where(sideways, side[i], jnp.where(own_rows, arrs[k, tile(i)], rows[i]))

    def finish(slot):
        wait_all(0, slot)
        halos = {k: halo_tiles(k, slot) for k in (1, 3, 5, 0, 2, 4)}
        lanes = {TWIN[k]: turn(join(halos[k])) for k in (1, 3, 5, 0, 2, 4)}
        for k in (0, 2, 4, 1, 3, 5):
            merge(qa, k, halos[k], lanes[k])

    def scale_faces(first_step):
        def one(step, carry):
            scale = ws_ref[lax.rem(first_step + step, steps)]
            sw[step] = scale * wf[...]
            return carry
        lax.fori_loop(0, BLOCK_STEPS, one, 0)

    for f in (1, 2, 0):
        for slot in range(3):
            ox, oy, oz, quad = homes[slot]

            @pl.when(leaves[slot])
            def _():
                tile_copy(f, slot, quad, at(ox, oy, oz)).wait_send()
        for quad in range(3):
            @pl.when(comes[quad])
            def _():
                tile_copy(f, 0, quad, holder[quad]).wait_recv()
        for quad in range(3):
            loc = dot(dot(placing((SIZE, own), 0, row_to_idx, flip_a[quad]), tiles[f, quad]),
                      placing((own, SIZE), 1, lane_to_idx, flip_b[quad]))
            plain, turned = PLAIN[quad], TWIN[PLAIN[quad]]
            if f == 0:
                qa[plain] = loc
                qa[turned] = turn(loc)
            elif f == 1:
                loc = jnp.where(flip_a[quad] == 1, -1.0, 1.0) * loc
                qb[plain] = loc
                sw[0, turned] = turn(loc)
            else:
                loc = jnp.where(flip_b[quad] == 1, -1.0, 1.0) * loc
                sw[0, plain] = loc
                qb[turned] = turn(loc)
        if f == 2:
            start_first(qb, 1, 2, -1.0, 1.0)
            start_rest(qb, 1, 2, -1.0, 1.0)
            start_first(sw.at[0], 2, 3, 1.0, -1.0)
            start_rest(sw.at[0], 2, 3, 1.0, -1.0)
    start_first(qa, 0, 0, 1.0, 1.0)
    start_rest(qa, 0, 0, 1.0, 1.0)

    coef[1] = 1.0 - 4.0 * coef[0]
    coef[2] = 0.5 * coef[0]
    coef[3] = 0.5 - 2.0 * coef[0]

    wait_all(1, 2)
    wait_all(2, 3)
    for k in range(6):
        merge(qb, k, halo_tiles(k, 2), turn(join(halo_tiles(TWIN[k], 3))))
    for k in range(6):
        here = qb[k]
        scaled = 0.5 / (6.0 * C_SPEED)
        after = join([here[8:], roll_rows(here[:8], -1)])
        beyond = jnp.where(sub == 7, roll_rows(strip(k, 2)[-1], 1), after[-8:])
        wf[k] = scaled * (here + after)
        wf[k, row(15, 7)] = scaled * (here[:1] - qb[ACROSS[k], row(0)])
        wlast[k] = scaled * (here[-8:] + beyond)
    scale_faces(0)

    def x_part(a_ref, k, faces, ghosts=False, beyond=None):
        a = a_ref[k]
        first, last = a[:8], a[-8:]
        below, above = roll_rows(last, 1), roll_rows(first, -1)
        if ghosts:
            below = jnp.where(sub == 0, a_ref[ACROSS[k], tile(0)], below)
        if beyond is not None:
            above = jnp.where(sub == 7, roll_rows(beyond[0], 1), above)
        m = join([below, a[:-8]]) + join([a[8:], above])
        v = 8.0 * a - m
        v_above, here = roll_rows(v[:8], -1), faces
        if beyond is not None:
            v_above = 8.0 * above - (last + jnp.where(sub == 7, beyond[0], roll_rows(a[8:16], -1)))
            here = join([faces[:-8], beyond[1]])
        flux = here * (v + join([v[8:], v_above]))
        flux_below = roll_rows(flux[-8:], 1)
        if ghosts:
            v_below = 8.0 * below - (jnp.where(sub == 0, a_ref[ACROSS[k], tile(1)], roll_rows(a[-16:-8], 1)) + first)
            flux_below = roll_rows(faces[-8:], 1) * (v_below + v[:8])
        return (m - flux) + join([flux_below, flux[:-8]])

    def parts_of(src, dst, second, step, group, ghosts, scale, slot):
        part = {}
        for k in group:
            beyond = None if scale is None else (strip(k, slot)[-1], scale * wlast[k])
            part[k] = coef[2 if second else 0] * x_part(src, k, sw[step, k], ghosts, beyond)
            if k in PRIMARY:
                own_part = coef[3 if second else 1] * src[k]
                if second:
                    own_part = 0.5 * dst[k] + own_part
                part[k] = own_part + part[k]
        return part, {k: turn(part[k]) for k in group}

    def stage(src, dst, second, step, ghosts=False, scale=None, slot=None, before_end=None):
        part, turned = {}, {}
        for group in GROUPS:
            more = parts_of(src, dst, second, step, group, ghosts, scale, slot)
            part.update(more[0])
            turned.update(more[1])
        new = {}
        for pair in ((0, 1, 2, 3), (4, 5)):
            for k in pair:
                new[k] = part[k] + turned[TWIN[k]]
            for k in pair:
                dst[k] = new[k]
            if before_end is not None and pair == (0, 1, 2, 3):
                before_end()
        if before_end is None and scale is None:
            for k in range(6):
                near = new[ACROSS[k]]
                dst[k, row(14, 7)] = near[8:9]
                dst[k, row(15, 7)] = near[:1]

    def run_block(first_step, count, slot, before_end):
        finish(slot)
        stage(qa, qb, False, 0, ghosts=True, scale=ws_ref[first_step], slot=slot)
        stage(qb, qa, True, 0, ghosts=True)

        def one_step(step, carry):
            stage(qa, qb, False, step)
            stage(qb, qa, True, step)
            return carry

        lax.fori_loop(1, count - 1, one_step, 0, unroll=True)
        stage(qa, qb, False, count - 1)
        stage(qb, qa, True, count - 1, before_end=before_end)

    full_blocks = (steps - 1) // BLOCK_STEPS

    def block(blk, carry):
        out_slot = lax.rem(blk + 1, 2)
        run_block(blk * BLOCK_STEPS, BLOCK_STEPS, lax.rem(blk, 2), functools.partial(start_first, qa, 0, out_slot, 1.0, 1.0))
        start_rest(qa, 0, out_slot, 1.0, 1.0)
        scale_faces((blk + 1) * BLOCK_STEPS)
        return carry

    lax.fori_loop(0, full_blocks, block, 0)
    run_block(full_blocks * BLOCK_STEPS, steps - full_blocks * BLOCK_STEPS, full_blocks % 2, lambda: None)

    def result_copy(quad, slot, device, number):
        return pltpu.make_async_remote_copy(
            result.at[quad], out_ref.at[slot], osend.at[number], orecv.at[slot],
            device_id=device, device_id_type=MESH)

    for quad in range(3):
        result[quad] = dot(dot(placing((own, SIZE), 1, row_to_idx, flip_a[quad]), qa[PLAIN[quad]]),
                           placing((SIZE, own), 0, lane_to_idx, flip_b[quad]))

        @pl.when(comes[quad])
        def _():
            result_copy(quad, slot_of[quad], holder[quad], quad).start()

        @pl.when(jnp.logical_not(comes[quad]))
        def _():
            pltpu.make_async_copy(result.at[quad], out_ref.at[slot_of[quad]], osend.at[quad]).start()

    for quad in range(3):
        @pl.when(comes[quad])
        def _():
            result_copy(quad, slot_of[quad], holder[quad], quad).wait_send()

        @pl.when(jnp.logical_not(comes[quad]))
        def _():
            pltpu.make_async_copy(result.at[quad], out_ref.at[slot_of[quad]], osend.at[quad]).wait()
    for slot in range(3):
        ox, oy, oz, _ = homes[slot]

        @pl.when(leaves[slot])
        def _():
            result_copy(0, slot, at(ox, oy, oz), 0).wait_recv()
```

```python
import functools
import math

import jax
import jax.numpy as jnp
import numpy as np
from jax import lax
from jax.experimental import pallas as pl
from jax.experimental.pallas import tpu as pltpu
from jax.sharding import PartitionSpec as P

C_SPEED = 2.5
CFL_STEP = 0.12
MESH = pl.DeviceIdType.MESH
HIGHEST = lax.Precision.HIGHEST

TWIN = tuple(k ^ 1 for k in range(6))
ACROSS = (2, 4, 0, 5, 1, 3)
PRIMARY = (0, 2, 4)
STRIPS = ((2, 4), (0, 5), (1, 3))
STRIP_PLACE = {k: (axis, n) for axis, pair in enumerate(STRIPS) for n, k in enumerate(pair)}
CORNERS = {1: (0, 1, 1), 3: (1, 0, 1), 4: (1, 1, 0)}

SIZE = 128
TILES = 16
EDGE = 10
BLOCK_STEPS = 10
GROUPS = ((0, 2), (1, 3), (4, 5))


def row_idx(row):
    return TILES * (row % 8) + row // 8


def lane_group(b):
    half = (b + 1) // 2
    return 8 - half + 2 * half * (1 - b % 2)


LANE_ORDER = tuple(lane_group(b) for b in range(TILES))


def tile(i):
    return pl.ds(8 * i, 8)


def row(i, sublane=0):
    return pl.ds(8 * i + sublane, 1)


def tiles_of(arr):
    return jnp.split(arr, arr.shape[0] // 8)


def join(tiles):
    return jnp.concatenate(tiles)


def roll_rows(tile, shift):
    return pltpu.roll(tile, shift % 8, 0)


def turn(arr):
    tiles = tiles_of(arr)
    turned = tiles_of(join([tiles[i] for i in LANE_ORDER]).T)
    return join([turned[LANE_ORDER.index(i)] for i in range(TILES)])


def solution(mesh):
    axis_names = mesh.axis_names

    def local_run(tracer, wind_a, wind_b, wind_scale):
        own = tracer.shape[1]
        cells = 2 * own
        steps = wind_scale.shape[0]
        dalpha = 0.5 * math.pi / cells
        place = np.arange(SIZE)
        lane_idx = TILES * (place % 8) + lane_group(place // 8)
        tan_a = np.tan((row_idx(place) + 0.5) * dalpha - 0.25 * math.pi)[:, None]
        tan_b = np.tan((lane_idx + 0.5) * dalpha - 0.25 * math.pi)[None, :]
        r_sq = 1.0 + tan_a * tan_a + tan_b * tan_b
        inv_sqrt_g = r_sq * np.sqrt(r_sq) / ((1.0 + tan_a * tan_a) * (1.0 + tan_b * tan_b))
        gain = (0.5 * C_SPEED * CFL_STEP * inv_sqrt_g).astype(np.float32)
        out = pl.pallas_call(
            functools.partial(kernel, own, steps, axis_names),
            out_shape=jax.ShapeDtypeStruct(tracer.shape, jnp.float32),
            in_specs=[pl.BlockSpec(memory_space=pl.ANY)] * 5,
            out_specs=pl.BlockSpec(memory_space=pl.ANY),
            scratch_shapes=[
                pltpu.SMEM((steps,), jnp.float32),
                pltpu.VMEM((3, 3, own, own), jnp.float32),
                pltpu.VMEM((6, SIZE, SIZE), jnp.float32),
                pltpu.VMEM((6, SIZE, SIZE), jnp.float32),
                pltpu.VMEM((BLOCK_STEPS, 6, SIZE, SIZE), jnp.float32),
                pltpu.VMEM((6, SIZE, SIZE), jnp.float32),
                pltpu.VMEM((6, 8, SIZE), jnp.float32),
                pltpu.VMEM((4, SIZE, SIZE), jnp.float32),
                pltpu.VMEM((3, 3, own, own), jnp.float32),
                pltpu.VMEM((3, own, own), jnp.float32),
                pltpu.VMEM((3, 6, 40, SIZE), jnp.float32),
                pltpu.VMEM((4, 6, 40, SIZE), jnp.float32),
                pltpu.VMEM((3, 3, 8, SIZE), jnp.float32),
                pltpu.VMEM((4, 3, 8, SIZE), jnp.float32),
            ] + [pltpu.SemaphoreType.DMA(shape) for shape in ((4, 6), (3, 3), (3,)) for _ in range(2)] + [
                pltpu.SemaphoreType.DMA((5,)),
            ],
            compiler_params=pltpu.CompilerParams(collective_id=0, has_side_effects=True),
            name="advect",
        )(wind_scale, tracer, wind_a, wind_b, gain)
        return out

    field_spec = P(('member', 'panel'), 'tx', 'ty')
    wind_spec = P('panel', 'tx', 'ty')
    return jax.shard_map(local_run, mesh=mesh, in_specs=(field_spec, wind_spec, wind_spec, P()),
                         out_specs=field_spec, check_vma=False)


def kernel(own, steps, axis_names, ws_in, q_in, wa_in, wb_in, gain_in, out_ref,
           ws_ref, fields, qa, qb, sw, wf, wlast, coef, tiles, result, send, recv, csend, crecv,
           ssem, rsem, tsend, trecv, osend, orecv, isem):
    tx, ty, core = lax.axis_index('tx'), lax.axis_index('ty'), lax.axis_index('panel')
    by, bz, bx = tx, ty, lax.rem(core + tx + 1, 2)

    def place(kx, ky, kc):
        return {name: {'tx': kx, 'ty': ky, 'panel': kc}.get(name, 0) for name in axis_names}

    barrier = pltpu.get_barrier_semaphore()
    for other in range(1, 8):
        near = [1 - at if other & bit else at for at, bit in ((tx, 1), (ty, 2), (core, 4))]
        pl.semaphore_signal(barrier, inc=1, device_id=place(*near), device_id_type=MESH)
    loads = [pltpu.make_async_copy(src, dst, isem.at[n]) for n, (src, dst) in enumerate((
        (wa_in, fields.at[1]), (wb_in, fields.at[2]), (q_in, fields.at[0]), (gain_in, coef.at[0]), (ws_in, ws_ref)))]
    for load in loads:
        load.start()

    def at(ox, oy, oz):
        return place(oy, oz, lax.rem(ox + oy + 1, 2))

    def pick(first, second):
        return jnp.where(core == 0, first, second)

    homes = (
        (pick(1, tx), pick(tx, 0), ty, pick(0, 1)),
        (pick(1 - tx, 1 - ty), pick(1, tx), pick(ty, 1), pick(1, 2)),
        (pick(0, ty), pick(1 - tx, tx), pick(ty, 0), pick(0, 2)),
    )
    leaves = [jnp.logical_not((ox == bx) & (oy == by) & (oz == bz)) for ox, oy, oz, _ in homes]
    flip_a = (1 - lax.rem(bx + by, 2), lax.rem(bx + by, 2), by)
    flip_b = (bz, bz, jnp.where(bz == 1, 1 - bx, bx))
    panel = (jnp.where(bx == 1, 0, 2), jnp.where(by == 1, 1, 3), jnp.where(bz == 1, 4, 5))
    holder = [place(flip_a[n], flip_b[n], panel[n] // 3) for n in range(3)]
    slot_of = [lax.rem(panel[n], 3) for n in range(3)]
    comes = [jnp.logical_not((flip_a[n] == tx) & (flip_b[n] == ty) & (panel[n] // 3 == core)) for n in range(3)]

    def tile_copy(f, slot, quad, device):
        return pltpu.make_async_remote_copy(
            fields.at[f, slot], tiles.at[f, quad], tsend.at[f, slot], trecv.at[f, quad],
            device_id=device, device_id_type=MESH)

    for load in loads:
        load.wait()
    pl.semaphore_wait(barrier, 7)
    for f in (1, 2, 0):
        for slot in range(3):
            ox, oy, oz, quad = homes[slot]

            @pl.when(leaves[slot])
            def _():
                tile_copy(f, slot, quad, at(ox, oy, oz)).start()

            @pl.when(jnp.logical_not(leaves[slot]))
            def _():
                tiles[f, quad] = fields[f, slot]

    def placing(shape, spot_axis, to_idx, flip):
        dist = to_idx(lax.broadcasted_iota(jnp.int32, shape, spot_axis))
        cell = lax.broadcasted_iota(jnp.int32, shape, 1 - spot_axis)
        source = jnp.where(dist < own, jnp.where(flip == 1, own - 1 - dist, dist), -1)
        return jnp.where(source == cell, 1.0, 0.0)

    def row_to_idx(row):
        return TILES * lax.rem(row, 8) + row // 8

    def lane_to_idx(spot):
        b = spot // 8
        half = (b + 1) // 2
        return TILES * lax.rem(spot, 8) + 8 - half + 2 * half * (1 - lax.rem(b, 2))

    def dot(lhs, rhs):
        return jnp.dot(lhs, rhs, precision=HIGHEST, preferred_element_type=jnp.float32)

    PLAIN = (0, 2, 5)

    sub = lax.broadcasted_iota(jnp.int32, (8, SIZE), 0)
    lane = lax.broadcasted_iota(jnp.int32, (8, SIZE), 1)
    lane_s, lane_i = lax.rem(lane, 8), lax.rem(lane_to_idx(lane), TILES)
    edge_lane = (lane_s == 5) & (lane_i >= EDGE)
    halo_lane = (lane_s >= 6) | edge_lane

    def group_lane(group, number):
        return 8 * jnp.where(group < 8, 15 - 2 * group, 2 * group - TILES) + number

    def mirror_lane(group, number):
        return group_lane(lax.rem(19 - group, TILES), jnp.where(group < 4, 11, EDGE) - number)

    odd_row = lax.rem(sub, 2)
    row_pair, lane_pair = sub // 2, lane_s // 2
    high, mid = lane_i >= EDGE, (lane_i >= 4) & (lane_i < EDGE)
    edge_group = jnp.where(mid, lane_i + 6, lane_i)
    at_edge = ((lane_s == 5) | (lane_s == 7)) & (high | mid)
    source_vreg = jnp.where(at_edge, jnp.where(lane_s == 7, 0, 2) + jnp.where(high, 0, 1), lane_pair)
    source_lane = jnp.where(at_edge, mirror_lane(edge_group, 5), mirror_lane(lane_i, 6 + lax.rem(lane, 2)))
    at_four = lane_s == 4
    takes_first = (odd_row == 1) & ((lane_s == 1) | (lane_s == 3) | (at_four & high))
    takes_last = (odd_row == 1) & ((lane_s == 6) | (at_four & mid))
    first_src = jnp.where(takes_first, mirror_lane(lane_i, jnp.where(at_four, 5, 6 + lane_s // 2)), 0)
    last_src = jnp.where(takes_last, mirror_lane(jnp.where(at_four, edge_group, lane_i), jnp.where(at_four, 5, 6 + sub // 4)), 0)
    low_group = lane_i - 6
    edge_back = [group_lane(lane_i, 7), group_lane(low_group, 7), group_lane(lane_i, 5), group_lane(low_group, 5)]
    msg_back = [jnp.where(lane_s >= 6, lane - 6 + 2 * j, jnp.where(edge_lane, edge_back[j], 0)) for j in range(4)]
    first_back = jnp.where(lane_s >= 6, lane + lane_s - 11, jnp.where(edge_lane, lane - 1, 0))
    last_back = jnp.where(lane_s >= 6, lane - lane_s + 6, jnp.where(edge_lane, group_lane(low_group, 4), 0))
    last_row = 1 + 2 * jnp.where((sub >= 4) & (lane_s < 7), odd_row, lax.rem(sub + 2 * (sub // 4), 4))

    def rows_by(arr, idx):
        return jnp.take_along_axis(arr, idx, axis=0, mode="promise_in_bounds")

    def lanes_by(arr, idx):
        return jnp.take_along_axis(arr, idx, axis=1, mode="promise_in_bounds")

    def by_number(number, parts):
        res = parts[0]
        for m, part in enumerate(parts):
            res = jnp.where(number == m, part, res) if m else res
        return res

    def peer(mirrored):
        return at(*(1 - b if m else b for b, m in zip((bx, by, bz), mirrored)))

    def strip_copy(axis, out, slot):
        return pltpu.make_async_remote_copy(
            send.at[out, pl.ds(2 * axis, 2)], recv.at[slot, pl.ds(2 * axis, 2)], ssem.at[slot, axis], rsem.at[slot, axis],
            device_id=peer(tuple(int(n == axis) for n in range(3))), device_id_type=MESH)

    def corner_copy(k, out, slot):
        n = k // 2
        return pltpu.make_async_remote_copy(
            csend.at[out, n], crecv.at[slot, n], ssem.at[slot, 3 + n], rsem.at[slot, 3 + n],
            device_id=peer(CORNERS[k]), device_id_type=MESH)

    def signed(sign, arr):
        return arr if sign == 1.0 else sign * arr

    def pack(arrs, k, out, sign):
        axis, n = STRIP_PLACE[k]
        a = tiles_of(arrs[k])

        def mirrored(i, sublane):
            return rows_by(a[(19 - i) % TILES], sublane)

        msg = [by_number(row_pair, [mirrored(i, (5 if i < 4 else 4) - odd_row) for i in range(4 * j, 4 * j + 4)])
               for j in range(4)]
        tail = [mirrored(i, 5 + 0 * sub) for i in range(EDGE, TILES)] + [mirrored(i, 3 + 0 * sub) for i in range(2)]
        msg = [signed(sign, part) for part in msg + [by_number(sub, tail)]]
        send[out, 2 * axis + n] = join(msg)
        return msg

    def pack_corner(k, packed, out, corner_sign):
        *msg, tail = packed
        block = by_number(source_vreg, [lanes_by(m, source_lane) for m in msg])
        first = lanes_by(rows_by(tail, row_pair), first_src)
        last = lanes_by(rows_by(tail, 4 + lax.rem(row_pair, 2)), last_src)
        block = jnp.where(takes_first, first, jnp.where(takes_last, last, block))
        csend[out, k // 2] = signed(corner_sign, block)

    def sender(arrs, out, slot, sign=1.0, corner_sign=1.0):
        packed = [pack(arrs, k, out, sign) for k in (1, 3)]
        strip_copy(2, out, slot).start()
        for k, msg in zip((1, 3), packed):
            pack_corner(k, msg, out, corner_sign)
        for k in (1, 3):
            corner_copy(k, out, slot).start()
        yield
        for k in (0, 2):
            pack(arrs, k, out, sign)
        yield
        pack_corner(4, pack(arrs, 4, out, sign), out, corner_sign)
        corner_copy(4, out, slot).start()
        pack(arrs, 5, out, sign)
        strip_copy(1, out, slot).start()
        strip_copy(0, out, slot).start()
        yield

    def strip(k, slot):
        axis, n = STRIP_PLACE[k]
        return tiles_of(recv[slot, 2 * axis + n])

    def halo_tiles(k, slot):
        *msg, tail = strip(k, slot)
        if k in CORNERS:
            block = crecv[slot, k // 2]
            msg = [jnp.where(halo_lane, lanes_by(block, msg_back[j]), msg[j]) for j in range(4)]
            last = rows_by(lanes_by(block, last_back), last_row)
            tail = jnp.where(halo_lane, jnp.where(sub < 4, rows_by(lanes_by(block, first_back), last_row), last), tail)
        res = [roll_rows(msg[i // 4], 6 - 2 * (i % 4)) for i in range(TILES)]
        for i in range(EDGE, TILES):
            res[i] = jnp.where(sub == 5, roll_rows(tail, 15 - i), res[i])
        return res

    def wait_all(out, slot):
        for axis in (0, 1):
            strip_copy(axis, out, slot).wait()
        for k in (3, 4, 1):
            corner_copy(k, out, slot).wait()
        strip_copy(2, out, slot).wait()

    def merge(arrs, k, rows, lanes):
        side = tiles_of(lanes)
        for i in range(TILES):
            own_rows = sub < (6 if i < EDGE else 5)
            sideways = halo_lane & own_rows if k in CORNERS else halo_lane
            arrs[k, tile(i)] = jnp.where(sideways, side[i], jnp.where(own_rows, arrs[k, tile(i)], rows[i]))

    def finish(slot):
        wait_all(0, slot)
        halos = {k: halo_tiles(k, slot) for k in (0, 2, 5, 1, 3, 4)}
        lanes = {TWIN[k]: turn(join(halos[k])) for k in (0, 2, 5, 1, 3, 4)}
        for k in (0, 2, 4, 1, 3, 5):
            merge(qa, k, halos[k], lanes[k])

    def scale_faces(first_step):
        def one(step, carry):
            scale = ws_ref[lax.rem(first_step + step, steps)]
            sw[step] = scale * wf[...]
            return carry
        lax.fori_loop(0, BLOCK_STEPS, one, 0)

    for f in (1, 2, 0):
        for slot in range(3):
            ox, oy, oz, quad = homes[slot]

            @pl.when(leaves[slot])
            def _():
                tile_copy(f, slot, quad, at(ox, oy, oz)).wait_send()
        for quad in range(3):
            @pl.when(comes[quad])
            def _():
                tile_copy(f, 0, quad, holder[quad]).wait_recv()
        for quad in range(3):
            loc = dot(dot(placing((SIZE, own), 0, row_to_idx, flip_a[quad]), tiles[f, quad]),
                      placing((own, SIZE), 1, lane_to_idx, flip_b[quad]))
            plain, turned = PLAIN[quad], TWIN[PLAIN[quad]]
            if f == 0:
                qa[plain] = loc
                qa[turned] = turn(loc)
            elif f == 1:
                loc = jnp.where(flip_a[quad] == 1, -1.0, 1.0) * loc
                qb[plain] = loc
                sw[0, turned] = turn(loc)
            else:
                loc = jnp.where(flip_b[quad] == 1, -1.0, 1.0) * loc
                sw[0, plain] = loc
                qb[turned] = turn(loc)
        if f == 2:
            list(sender(qb, 1, 2, sign=-1.0))
            list(sender(sw.at[0], 2, 3, corner_sign=-1.0))
    list(sender(qa, 0, 0))

    coef[1] = 1.0 - 4.0 * coef[0]
    coef[2] = 0.5 * coef[0]
    coef[3] = 0.5 - 2.0 * coef[0]

    wait_all(1, 2)
    wait_all(2, 3)
    for k in range(6):
        merge(qb, k, halo_tiles(k, 2), turn(join(halo_tiles(TWIN[k], 3))))
    for k in range(6):
        here = qb[k]
        scaled = 0.5 / (6.0 * C_SPEED)
        after = join([here[8:], roll_rows(here[:8], -1)])
        beyond = jnp.where(sub == 7, roll_rows(strip(k, 2)[-1], 1), after[-8:])
        wf[k] = scaled * (here + after)
        wf[k, row(15, 7)] = scaled * (here[:1] - qb[ACROSS[k], row(0)])
        wlast[k] = scaled * (here[-8:] + beyond)
    scale_faces(0)

    def x_part(a_ref, k, faces, ghosts=False, beyond=None):
        a = a_ref[k]
        first, last = a[:8], a[-8:]
        below, above = roll_rows(last, 1), roll_rows(first, -1)
        if ghosts:
            below = jnp.where(sub == 0, a_ref[ACROSS[k], tile(0)], below)
        if beyond is not None:
            above = jnp.where(sub == 7, roll_rows(beyond[0], 1), above)
        m = join([below, a[:-8]]) + join([a[8:], above])
        v = 8.0 * a - m
        v_above, here = roll_rows(v[:8], -1), faces
        if beyond is not None:
            v_above = 8.0 * above - (last + jnp.where(sub == 7, beyond[0], roll_rows(a[8:16], -1)))
            here = join([faces[:-8], beyond[1]])
        flux = here * (v + join([v[8:], v_above]))
        flux_below = roll_rows(flux[-8:], 1)
        if ghosts:
            v_below = 8.0 * below - (jnp.where(sub == 0, a_ref[ACROSS[k], tile(1)], roll_rows(a[-16:-8], 1)) + first)
            flux_below = roll_rows(faces[-8:], 1) * (v_below + v[:8])
        return (m - flux) + join([flux_below, flux[:-8]])

    def parts_of(src, dst, second, step, group, ghosts, scale, slot):
        part = {}
        for k in group:
            beyond = None if scale is None else (strip(k, slot)[-1], scale * wlast[k])
            part[k] = coef[2 if second else 0] * x_part(src, k, sw[step, k], ghosts, beyond)
            if k in PRIMARY:
                own_part = coef[3 if second else 1] * src[k]
                if second:
                    own_part = 0.5 * dst[k] + own_part
                part[k] = own_part + part[k]
        return part, {k: turn(part[k]) for k in group}

    def stage(src, dst, second, step, ghosts=False, scale=None, slot=None, sends=None):
        part, turned = {}, {}
        for group in GROUPS:
            more = parts_of(src, dst, second, step, group, ghosts, scale, slot)
            part.update(more[0])
            turned.update(more[1])
        new = {}
        for group in ((1, 3), (0, 2), (4, 5)):
            for k in group:
                new[k] = part[k] + turned[TWIN[k]]
            for k in group:
                dst[k] = new[k]
            if sends is not None:
                next(sends)
        if sends is None and scale is None:
            for k in range(6):
                near = new[ACROSS[k]]
                dst[k, row(14, 7)] = near[8:9]
                dst[k, row(15, 7)] = near[:1]

    def run_block(first_step, count, slot, sends):
        finish(slot)
        stage(qa, qb, False, 0, ghosts=True, scale=ws_ref[first_step], slot=slot)
        stage(qb, qa, True, 0, ghosts=True)

        def one_step(step, carry):
            stage(qa, qb, False, step)
            stage(qb, qa, True, step)
            return carry

        lax.fori_loop(1, count - 1, one_step, 0, unroll=True)
        stage(qa, qb, False, count - 1)
        stage(qb, qa, True, count - 1, sends=sends)

    full_blocks = (steps - 1) // BLOCK_STEPS

    def block(blk, carry):
        out_slot = lax.rem(blk + 1, 2)
        run_block(blk * BLOCK_STEPS, BLOCK_STEPS, lax.rem(blk, 2), sender(qa, 0, out_slot))
        scale_faces((blk + 1) * BLOCK_STEPS)
        return carry

    lax.fori_loop(0, full_blocks, block, 0)
    run_block(full_blocks * BLOCK_STEPS, steps - full_blocks * BLOCK_STEPS, full_blocks % 2, iter(range(3)))

    def result_copy(quad, slot, device, number):
        return pltpu.make_async_remote_copy(
            result.at[quad], out_ref.at[slot], osend.at[number], orecv.at[slot],
            device_id=device, device_id_type=MESH)

    for quad in range(3):
        result[quad] = dot(dot(placing((own, SIZE), 1, row_to_idx, flip_a[quad]), qa[PLAIN[quad]]),
                           placing((SIZE, own), 0, lane_to_idx, flip_b[quad]))

        @pl.when(comes[quad])
        def _():
            result_copy(quad, slot_of[quad], holder[quad], quad).start()

        @pl.when(jnp.logical_not(comes[quad]))
        def _():
            pltpu.make_async_copy(result.at[quad], out_ref.at[slot_of[quad]], osend.at[quad]).start()

    for quad in range(3):
        @pl.when(comes[quad])
        def _():
            result_copy(quad, slot_of[quad], holder[quad], quad).wait_send()

        @pl.when(jnp.logical_not(comes[quad]))
        def _():
            pltpu.make_async_copy(result.at[quad], out_ref.at[slot_of[quad]], osend.at[quad]).wait()
    for slot in range(3):
        ox, oy, oz, _ = homes[slot]

        @pl.when(leaves[slot])
        def _():
            result_copy(0, slot, at(ox, oy, oz), 0).wait_recv()
```

```python
import functools
import math

import jax
import jax.numpy as jnp
import numpy as np
from jax import lax
from jax.experimental import pallas as pl
from jax.experimental.pallas import tpu as pltpu
from jax.sharding import PartitionSpec as P

C_SPEED = 2.5
CFL_STEP = 0.12
MESH = pl.DeviceIdType.MESH
HIGHEST = lax.Precision.HIGHEST

TWIN = tuple(k ^ 1 for k in range(6))
ACROSS = (2, 4, 0, 5, 1, 3)
PRIMARY = (0, 2, 4)
STRIPS = ((2, 4), (0, 5), (1, 3))
STRIP_PLACE = {k: (axis, n) for axis, pair in enumerate(STRIPS) for n, k in enumerate(pair)}
CORNERS = {1: (0, 1, 1), 3: (1, 0, 1), 4: (1, 1, 0)}

SIZE = 128
TILES = 16
PITCH = SIZE + 16
CENTRE = 5
EDGE = 10
BLOCK_STEPS = 10
GROUPS = ((0, 2), (1, 3), (4, 5))


def row_idx(row):
    return TILES * (row % 8) + row // 8


def lane_group(b):
    half = (b + 1) // 2
    return np.where(b > 2 * CENTRE, b, CENTRE - half + 2 * half * (1 - b % 2))


LANE_ORDER = tuple(int(lane_group(b)) for b in range(TILES))


def tile(i):
    return pl.ds(8 * i, 8)


def row(i, sublane=0):
    return pl.ds(8 * i + sublane, 1)


def tiles_of(arr):
    return jnp.split(arr, arr.shape[0] // 8)


def join(tiles):
    return jnp.concatenate(tiles)


def roll_rows(tile, shift):
    return pltpu.roll(tile, shift % 8, 0)


def turn(arr):
    tiles = tiles_of(arr)
    turned = tiles_of(join([tiles[i] for i in LANE_ORDER]).T)
    return join([turned[LANE_ORDER.index(i)] for i in range(TILES)])


def solution(mesh):
    axis_names = mesh.axis_names

    def local_run(tracer, wind_a, wind_b, wind_scale):
        own = tracer.shape[1]
        cells = 2 * own
        steps = wind_scale.shape[0]
        dalpha = 0.5 * math.pi / cells
        place = np.arange(SIZE)
        lane_idx = TILES * (place % 8) + lane_group(place // 8)
        tan_a = np.tan((row_idx(place) + 0.5) * dalpha - 0.25 * math.pi)[:, None]
        tan_b = np.tan((lane_idx + 0.5) * dalpha - 0.25 * math.pi)[None, :]
        r_sq = 1.0 + tan_a * tan_a + tan_b * tan_b
        inv_sqrt_g = r_sq * np.sqrt(r_sq) / ((1.0 + tan_a * tan_a) * (1.0 + tan_b * tan_b))
        gain = (0.5 * C_SPEED * CFL_STEP * inv_sqrt_g).astype(np.float32)
        out = pl.pallas_call(
            functools.partial(kernel, own, steps, axis_names),
            out_shape=jax.ShapeDtypeStruct(tracer.shape, jnp.float32),
            in_specs=[pl.BlockSpec(memory_space=pl.ANY)] * 5,
            out_specs=pl.BlockSpec(memory_space=pl.ANY),
            scratch_shapes=[
                pltpu.SMEM((steps,), jnp.float32),
                pltpu.VMEM((3, 3, own, own), jnp.float32),
                pltpu.VMEM((6, PITCH, SIZE), jnp.float32),
                pltpu.VMEM((6, PITCH, SIZE), jnp.float32),
                pltpu.VMEM((BLOCK_STEPS, 6, SIZE, SIZE), jnp.float32),
                pltpu.VMEM((6, SIZE, SIZE), jnp.float32),
                pltpu.VMEM((6, 8, SIZE), jnp.float32),
                pltpu.VMEM((4, SIZE, SIZE), jnp.float32),
                pltpu.VMEM((3, 3, own, own), jnp.float32),
                pltpu.VMEM((3, own, own), jnp.float32),
                pltpu.VMEM((3, 6, 40, SIZE), jnp.float32),
                pltpu.VMEM((4, 6, 40, SIZE), jnp.float32),
                pltpu.VMEM((3, 3, 8, SIZE), jnp.float32),
                pltpu.VMEM((4, 3, 8, SIZE), jnp.float32),
            ] + [pltpu.SemaphoreType.DMA(shape) for shape in ((4, 6), (3, 3), (3,)) for _ in range(2)] + [
                pltpu.SemaphoreType.DMA((5,)),
            ],
            compiler_params=pltpu.CompilerParams(collective_id=0, has_side_effects=True),
            name="advect",
        )(wind_scale, tracer, wind_a, wind_b, gain)
        return out

    field_spec = P(('member', 'panel'), 'tx', 'ty')
    wind_spec = P('panel', 'tx', 'ty')
    return jax.shard_map(local_run, mesh=mesh, in_specs=(field_spec, wind_spec, wind_spec, P()),
                         out_specs=field_spec, check_vma=False)


def kernel(own, steps, axis_names, ws_in, q_in, wa_in, wb_in, gain_in, out_ref,
           ws_ref, fields, qa_rows, qb_rows, sw, wf, wlast, coef, tiles, result, send, recv, csend, crecv,
           ssem, rsem, tsend, trecv, osend, orecv, isem):
    tx, ty, core = lax.axis_index('tx'), lax.axis_index('ty'), lax.axis_index('panel')
    by, bz, bx = tx, ty, lax.rem(core + tx + 1, 2)
    qa, qb = (rows.at[:, pl.ds(0, SIZE)] for rows in (qa_rows, qb_rows))

    def place(kx, ky, kc):
        return {name: {'tx': kx, 'ty': ky, 'panel': kc}.get(name, 0) for name in axis_names}

    barrier = pltpu.get_barrier_semaphore()
    for other in range(1, 8):
        near = [1 - at if other & bit else at for at, bit in ((tx, 1), (ty, 2), (core, 4))]
        pl.semaphore_signal(barrier, inc=1, device_id=place(*near), device_id_type=MESH)
    loads = [pltpu.make_async_copy(src, dst, isem.at[n]) for n, (src, dst) in enumerate((
        (wa_in, fields.at[1]), (wb_in, fields.at[2]), (q_in, fields.at[0]), (gain_in, coef.at[0]), (ws_in, ws_ref)))]
    for load in loads:
        load.start()

    def at(ox, oy, oz):
        return place(oy, oz, lax.rem(ox + oy + 1, 2))

    def pick(first, second):
        return jnp.where(core == 0, first, second)

    homes = (
        (pick(1, tx), pick(tx, 0), ty, pick(0, 1)),
        (pick(1 - tx, 1 - ty), pick(1, tx), pick(ty, 1), pick(1, 2)),
        (pick(0, ty), pick(1 - tx, tx), pick(ty, 0), pick(0, 2)),
    )
    leaves = [jnp.logical_not((ox == bx) & (oy == by) & (oz == bz)) for ox, oy, oz, _ in homes]
    flip_a = (1 - lax.rem(bx + by, 2), lax.rem(bx + by, 2), by)
    flip_b = (bz, bz, jnp.where(bz == 1, 1 - bx, bx))
    panel = (jnp.where(bx == 1, 0, 2), jnp.where(by == 1, 1, 3), jnp.where(bz == 1, 4, 5))
    holder = [place(flip_a[n], flip_b[n], panel[n] // 3) for n in range(3)]
    slot_of = [lax.rem(panel[n], 3) for n in range(3)]
    comes = [jnp.logical_not((flip_a[n] == tx) & (flip_b[n] == ty) & (panel[n] // 3 == core)) for n in range(3)]

    def tile_copy(f, slot, quad, device):
        return pltpu.make_async_remote_copy(
            fields.at[f, slot], tiles.at[f, quad], tsend.at[f, slot], trecv.at[f, quad],
            device_id=device, device_id_type=MESH)

    for load in loads:
        load.wait()
    pl.semaphore_wait(barrier, 7)
    for f in (1, 2, 0):
        for slot in range(3):
            ox, oy, oz, quad = homes[slot]

            @pl.when(leaves[slot])
            def _():
                tile_copy(f, slot, quad, at(ox, oy, oz)).start()

            @pl.when(jnp.logical_not(leaves[slot]))
            def _():
                tiles[f, quad] = fields[f, slot]

    def placing(shape, spot_axis, to_idx, flip):
        dist = to_idx(lax.broadcasted_iota(jnp.int32, shape, spot_axis))
        cell = lax.broadcasted_iota(jnp.int32, shape, 1 - spot_axis)
        source = jnp.where(dist < own, jnp.where(flip == 1, own - 1 - dist, dist), -1)
        return jnp.where(source == cell, 1.0, 0.0)

    def row_to_idx(row):
        return TILES * lax.rem(row, 8) + row // 8

    def lane_to_idx(spot):
        b = spot // 8
        half = (b + 1) // 2
        group = jnp.where(b > 2 * CENTRE, b, CENTRE - half + 2 * half * (1 - lax.rem(b, 2)))
        return TILES * lax.rem(spot, 8) + group

    def dot(lhs, rhs):
        return jnp.dot(lhs, rhs, precision=HIGHEST, preferred_element_type=jnp.float32)

    PLAIN = (0, 2, 5)

    sub = lax.broadcasted_iota(jnp.int32, (8, SIZE), 0)
    lane = lax.broadcasted_iota(jnp.int32, (8, SIZE), 1)
    lane_s, lane_i = lax.rem(lane, 8), lax.rem(lane_to_idx(lane), TILES)
    edge_lane = (lane_s == 5) & (lane_i >= EDGE)
    halo_lane = (lane_s >= 6) | edge_lane

    def group_lane(group, number):
        turns = jnp.where(group < CENTRE, 2 * (CENTRE - group) - 1, 2 * (group - CENTRE))
        return 8 * jnp.where(group > 2 * CENTRE, group, turns) + number

    def mirror_lane(group, number):
        return group_lane(lax.rem(19 - group, TILES), jnp.where(group < 4, 11, EDGE) - number)

    odd_row = lax.rem(sub, 2)
    row_pair, lane_pair = sub // 2, lane_s // 2
    high, mid = lane_i >= EDGE, (lane_i >= 4) & (lane_i < EDGE)
    edge_group = jnp.where(mid, lane_i + 6, lane_i)
    at_edge = ((lane_s == 5) | (lane_s == 7)) & (high | mid)
    source_vreg = jnp.where(at_edge, jnp.where(lane_s == 7, 0, 2) + jnp.where(high, 0, 1), lane_pair)
    source_lane = jnp.where(at_edge, mirror_lane(edge_group, 5), mirror_lane(lane_i, 6 + lax.rem(lane, 2)))
    at_four = lane_s == 4
    takes_first = (odd_row == 1) & ((lane_s == 1) | (lane_s == 3) | (at_four & high))
    takes_last = (odd_row == 1) & ((lane_s == 6) | (at_four & mid))
    first_src = jnp.where(takes_first, mirror_lane(lane_i, jnp.where(at_four, 5, 6 + lane_s // 2)), 0)
    last_src = jnp.where(takes_last, mirror_lane(jnp.where(at_four, edge_group, lane_i), jnp.where(at_four, 5, 6 + sub // 4)), 0)
    low_group = lane_i - 6
    edge_back = [group_lane(lane_i, 7), group_lane(low_group, 7), group_lane(lane_i, 5), group_lane(low_group, 5)]
    msg_back = [jnp.where(lane_s >= 6, lane - 6 + 2 * j, jnp.where(edge_lane, edge_back[j], 0)) for j in range(4)]
    first_back = jnp.where(lane_s >= 6, lane + lane_s - 11, jnp.where(edge_lane, lane - 1, 0))
    last_back = jnp.where(lane_s >= 6, lane - lane_s + 6, jnp.where(edge_lane, group_lane(low_group, 4), 0))
    last_row = 1 + 2 * jnp.where((sub >= 4) & (lane_s < 7), odd_row, lax.rem(sub + 2 * (sub // 4), 4))

    def rows_by(arr, idx):
        return jnp.take_along_axis(arr, idx, axis=0, mode="promise_in_bounds")

    def lanes_by(arr, idx):
        return jnp.take_along_axis(arr, idx, axis=1, mode="promise_in_bounds")

    def by_number(number, parts):
        res = parts[0]
        for m, part in enumerate(parts):
            res = jnp.where(number == m, part, res) if m else res
        return res

    def peer(mirrored):
        return at(*(1 - b if m else b for b, m in zip((bx, by, bz), mirrored)))

    def strip_copy(axis, out, slot):
        return pltpu.make_async_remote_copy(
            send.at[out, pl.ds(2 * axis, 2)], recv.at[slot, pl.ds(2 * axis, 2)], ssem.at[slot, axis], rsem.at[slot, axis],
            device_id=peer(tuple(int(n == axis) for n in range(3))), device_id_type=MESH)

    def corner_copy(k, out, slot):
        n = k // 2
        return pltpu.make_async_remote_copy(
            csend.at[out, n], crecv.at[slot, n], ssem.at[slot, 3 + n], rsem.at[slot, 3 + n],
            device_id=peer(CORNERS[k]), device_id_type=MESH)

    def signed(sign, arr):
        return arr if sign == 1.0 else sign * arr

    def pack(arrs, k, out, sign):
        axis, n = STRIP_PLACE[k]
        a = tiles_of(arrs[k])

        def mirrored(i, sublane):
            return rows_by(a[(19 - i) % TILES], sublane)

        msg = [by_number(row_pair, [mirrored(i, (5 if i < 4 else 4) - odd_row) for i in range(4 * j, 4 * j + 4)])
               for j in range(4)]
        tail = [mirrored(i, 5 + 0 * sub) for i in range(EDGE, TILES)] + [mirrored(i, 3 + 0 * sub) for i in range(2)]
        msg = [signed(sign, part) for part in msg + [by_number(sub, tail)]]
        send[out, 2 * axis + n] = join(msg)
        return msg

    def pack_corner(k, packed, out, corner_sign):
        *msg, tail = packed
        block = by_number(source_vreg, [lanes_by(m, source_lane) for m in msg])
        first = lanes_by(rows_by(tail, row_pair), first_src)
        last = lanes_by(rows_by(tail, 4 + lax.rem(row_pair, 2)), last_src)
        block = jnp.where(takes_first, first, jnp.where(takes_last, last, block))
        csend[out, k // 2] = signed(corner_sign, block)

    def sender(arrs, out, slot, sign=1.0, corner_sign=1.0):
        packed = [pack(arrs, k, out, sign) for k in (1, 3)]
        strip_copy(2, out, slot).start()
        for k, msg in zip((1, 3), packed):
            pack_corner(k, msg, out, corner_sign)
        for k in (1, 3):
            corner_copy(k, out, slot).start()
        yield
        for k in (0, 2):
            pack(arrs, k, out, sign)
        yield
        pack_corner(4, pack(arrs, 4, out, sign), out, corner_sign)
        corner_copy(4, out, slot).start()
        pack(arrs, 5, out, sign)
        strip_copy(1, out, slot).start()
        strip_copy(0, out, slot).start()
        yield

    def strip(k, slot):
        axis, n = STRIP_PLACE[k]
        return tiles_of(recv[slot, 2 * axis + n])

    def halo_tiles(k, slot):
        *msg, tail = strip(k, slot)
        if k in CORNERS:
            block = crecv[slot, k // 2]
            msg = [jnp.where(halo_lane, lanes_by(block, msg_back[j]), msg[j]) for j in range(4)]
            last = rows_by(lanes_by(block, last_back), last_row)
            tail = jnp.where(halo_lane, jnp.where(sub < 4, rows_by(lanes_by(block, first_back), last_row), last), tail)
        res = [roll_rows(msg[i // 4], 6 - 2 * (i % 4)) for i in range(TILES)]
        for i in range(EDGE, TILES):
            res[i] = jnp.where(sub == 5, roll_rows(tail, 15 - i), res[i])
        return res

    def wait_all(out, slot):
        for axis in (0, 1):
            strip_copy(axis, out, slot).wait()
        for k in (3, 4, 1):
            corner_copy(k, out, slot).wait()
        strip_copy(2, out, slot).wait()

    def merge(arrs, k, rows, lanes):
        side = tiles_of(lanes)
        for i in range(TILES):
            own_rows = sub < (6 if i < EDGE else 5)
            sideways = halo_lane & own_rows if k in CORNERS else halo_lane
            arrs[k, tile(i)] = jnp.where(sideways, side[i], jnp.where(own_rows, arrs[k, tile(i)], rows[i]))

    def finish(slot):
        wait_all(0, slot)
        halos = {k: halo_tiles(k, slot) for k in (0, 2, 5, 1, 3, 4)}
        lanes = {TWIN[k]: turn(join(halos[k])) for k in (0, 2, 5, 1, 3, 4)}
        for k in (0, 2, 4, 1, 3, 5):
            merge(qa, k, halos[k], lanes[k])

    def scale_faces(first_step):
        def one(step, carry):
            scale = ws_ref[lax.rem(first_step + step, steps)]
            sw[step] = scale * wf[...]
            return carry
        lax.fori_loop(0, BLOCK_STEPS, one, 0)

    for f in (1, 2, 0):
        for slot in range(3):
            ox, oy, oz, quad = homes[slot]

            @pl.when(leaves[slot])
            def _():
                tile_copy(f, slot, quad, at(ox, oy, oz)).wait_send()
        for quad in range(3):
            @pl.when(comes[quad])
            def _():
                tile_copy(f, 0, quad, holder[quad]).wait_recv()
        for quad in range(3):
            loc = dot(dot(placing((SIZE, own), 0, row_to_idx, flip_a[quad]), tiles[f, quad]),
                      placing((own, SIZE), 1, lane_to_idx, flip_b[quad]))
            plain, turned = PLAIN[quad], TWIN[PLAIN[quad]]
            if f == 0:
                qa[plain] = loc
                qa[turned] = turn(loc)
            elif f == 1:
                loc = jnp.where(flip_a[quad] == 1, -1.0, 1.0) * loc
                qb[plain] = loc
                sw[0, turned] = turn(loc)
            else:
                loc = jnp.where(flip_b[quad] == 1, -1.0, 1.0) * loc
                sw[0, plain] = loc
                qb[turned] = turn(loc)
        if f == 2:
            list(sender(qb, 1, 2, sign=-1.0))
            list(sender(sw.at[0], 2, 3, corner_sign=-1.0))
    list(sender(qa, 0, 0))

    coef[1] = 1.0 - 4.0 * coef[0]
    coef[2] = 0.5 * coef[0]
    coef[3] = 0.5 - 2.0 * coef[0]

    wait_all(1, 2)
    wait_all(2, 3)
    for k in range(6):
        merge(qb, k, halo_tiles(k, 2), turn(join(halo_tiles(TWIN[k], 3))))
    for k in range(6):
        here = qb[k]
        scaled = 0.5 / (6.0 * C_SPEED)
        after = join([here[8:], roll_rows(here[:8], -1)])
        beyond = jnp.where(sub == 7, roll_rows(strip(k, 2)[-1], 1), after[-8:])
        wf[k] = scaled * (here + after)
        wf[k, row(15, 7)] = scaled * (here[:1] - qb[ACROSS[k], row(0)])
        wlast[k] = scaled * (here[-8:] + beyond)
    scale_faces(0)

    def x_part(a_ref, k, faces, ghosts=False, beyond=None):
        a = a_ref[k]
        first, last = a[:8], a[-8:]
        below, above = roll_rows(last, 1), roll_rows(first, -1)
        if ghosts:
            below = jnp.where(sub == 0, a_ref[ACROSS[k], tile(0)], below)
        if beyond is not None:
            above = jnp.where(sub == 7, roll_rows(beyond[0], 1), above)
        m = join([below, a[:-8]]) + join([a[8:], above])
        v = 8.0 * a - m
        v_above, here = roll_rows(v[:8], -1), faces
        if beyond is not None:
            v_above = 8.0 * above - (last + jnp.where(sub == 7, beyond[0], roll_rows(a[8:16], -1)))
            here = join([faces[:-8], beyond[1]])
        flux = here * (v + join([v[8:], v_above]))
        flux_below = roll_rows(flux[-8:], 1)
        if ghosts:
            v_below = 8.0 * below - (jnp.where(sub == 0, a_ref[ACROSS[k], tile(1)], roll_rows(a[-16:-8], 1)) + first)
            flux_below = roll_rows(faces[-8:], 1) * (v_below + v[:8])
        return (m - flux) + join([flux_below, flux[:-8]])

    def parts_of(src, dst, second, step, group, ghosts, scale, slot):
        part = {}
        for k in group:
            beyond = None if scale is None else (strip(k, slot)[-1], scale * wlast[k])
            part[k] = coef[2 if second else 0] * x_part(src, k, sw[step, k], ghosts, beyond)
            if k in PRIMARY:
                own_part = coef[3 if second else 1] * src[k]
                if second:
                    own_part = 0.5 * dst[k] + own_part
                part[k] = own_part + part[k]
        return part, {k: turn(part[k]) for k in group}

    def stage(src, dst, second, step, ghosts=False, scale=None, slot=None, sends=None):
        part, turned = {}, {}
        for group in GROUPS:
            more = parts_of(src, dst, second, step, group, ghosts, scale, slot)
            part.update(more[0])
            turned.update(more[1])
        new = {}
        for group in ((1, 3), (0, 2), (4, 5)):
            for k in group:
                new[k] = part[k] + turned[TWIN[k]]
            for k in group:
                dst[k] = new[k]
            if sends is not None:
                next(sends)
        if sends is None and scale is None:
            for k in range(6):
                near = new[ACROSS[k]]
                dst[k, row(14, 7)] = near[8:9]
                dst[k, row(15, 7)] = near[:1]

    def run_block(first_step, count, slot, sends):
        finish(slot)
        stage(qa, qb, False, 0, ghosts=True, scale=ws_ref[first_step], slot=slot)
        stage(qb, qa, True, 0, ghosts=True)

        def one_step(step, carry):
            stage(qa, qb, False, step)
            stage(qb, qa, True, step)
            return carry

        lax.fori_loop(1, count - 1, one_step, 0, unroll=True)
        stage(qa, qb, False, count - 1)
        stage(qb, qa, True, count - 1, sends=sends)

    full_blocks = (steps - 1) // BLOCK_STEPS

    def block(blk, carry):
        out_slot = lax.rem(blk + 1, 2)
        run_block(blk * BLOCK_STEPS, BLOCK_STEPS, lax.rem(blk, 2), sender(qa, 0, out_slot))
        scale_faces((blk + 1) * BLOCK_STEPS)
        return carry

    lax.fori_loop(0, full_blocks, block, 0)
    run_block(full_blocks * BLOCK_STEPS, steps - full_blocks * BLOCK_STEPS, full_blocks % 2, iter(range(3)))

    def result_copy(quad, slot, device, number):
        return pltpu.make_async_remote_copy(
            result.at[quad], out_ref.at[slot], osend.at[number], orecv.at[slot],
            device_id=device, device_id_type=MESH)

    for quad in range(3):
        result[quad] = dot(dot(placing((own, SIZE), 1, row_to_idx, flip_a[quad]), qa[PLAIN[quad]]),
                           placing((SIZE, own), 0, lane_to_idx, flip_b[quad]))

        @pl.when(comes[quad])
        def _():
            result_copy(quad, slot_of[quad], holder[quad], quad).start()

        @pl.when(jnp.logical_not(comes[quad]))
        def _():
            pltpu.make_async_copy(result.at[quad], out_ref.at[slot_of[quad]], osend.at[quad]).start()

    for quad in range(3):
        @pl.when(comes[quad])
        def _():
            result_copy(quad, slot_of[quad], holder[quad], quad).wait_send()

        @pl.when(jnp.logical_not(comes[quad]))
        def _():
            pltpu.make_async_copy(result.at[quad], out_ref.at[slot_of[quad]], osend.at[quad]).wait()
    for slot in range(3):
        ox, oy, oz, _ = homes[slot]

        @pl.when(leaves[slot])
        def _():
            result_copy(0, slot, at(ox, oy, oz), 0).wait_recv()
```

```python
import functools
import math

import jax
import jax.numpy as jnp
import numpy as np
from jax import lax
from jax.experimental import pallas as pl
from jax.experimental.pallas import tpu as pltpu
from jax.sharding import PartitionSpec as P

C_SPEED = 2.5
CFL_STEP = 0.12
MESH = pl.DeviceIdType.MESH
HIGHEST = lax.Precision.HIGHEST

ARRAYS = range(6)
TWIN = tuple(k ^ 1 for k in ARRAYS)
ACROSS = (2, 4, 0, 5, 1, 3)
PRIMARY = (0, 2, 4)
STRIPS = ((2, 4), (0, 5), (1, 3))
STRIP_PLACE = {k: (axis, n) for axis, pair in enumerate(STRIPS) for n, k in enumerate(pair)}
CORNERS = {1: (0, 1, 1), 3: (1, 0, 1), 4: (1, 1, 0)}

SIZE = 128
TILES = 16
PITCH = SIZE + 16
CENTRE = 5
EDGE = 10
BLOCK_STEPS = 10
GROUPS = ((0, 2), (1, 3), (4, 5))


def row_idx(row):
    return TILES * (row % 8) + row // 8


def lane_group(b):
    half = (b + 1) // 2
    return np.where(b > 2 * CENTRE, b, CENTRE - half + 2 * half * (1 - b % 2))


LANE_ORDER = tuple(int(lane_group(b)) for b in range(TILES))


def tile(i):
    return pl.ds(8 * i, 8)


def row(i, sublane=0):
    return pl.ds(8 * i + sublane, 1)


def tiles_of(arr):
    return jnp.split(arr, arr.shape[0] // 8)


def join(tiles):
    return jnp.concatenate(tiles)


def roll_rows(tile, shift):
    return pltpu.roll(tile, shift % 8, 0)


def turn(arr):
    tiles = tiles_of(arr)
    turned = tiles_of(join([tiles[i] for i in LANE_ORDER]).T)
    return join([turned[LANE_ORDER.index(i)] for i in range(TILES)])


def solution(mesh):
    axis_names = mesh.axis_names

    def local_run(tracer, wind_a, wind_b, wind_scale):
        own = tracer.shape[1]
        cells = 2 * own
        steps = wind_scale.shape[0]
        dalpha = 0.5 * math.pi / cells
        place = np.arange(SIZE)
        lane_idx = TILES * (place % 8) + lane_group(place // 8)
        tan_a = np.tan((row_idx(place) + 0.5) * dalpha - 0.25 * math.pi)[:, None]
        tan_b = np.tan((lane_idx + 0.5) * dalpha - 0.25 * math.pi)[None, :]
        r_sq = 1.0 + tan_a * tan_a + tan_b * tan_b
        inv_sqrt_g = r_sq * np.sqrt(r_sq) / ((1.0 + tan_a * tan_a) * (1.0 + tan_b * tan_b))
        gain = (0.5 * C_SPEED * CFL_STEP * inv_sqrt_g).astype(np.float32)
        out = pl.pallas_call(
            functools.partial(kernel, own, steps, axis_names),
            out_shape=jax.ShapeDtypeStruct(tracer.shape, jnp.float32),
            in_specs=[pl.BlockSpec(memory_space=pl.ANY)] * 5,
            out_specs=pl.BlockSpec(memory_space=pl.ANY),
            scratch_shapes=[
                pltpu.SMEM((steps,), jnp.float32),
                pltpu.VMEM((3, 3, own, own), jnp.float32),
                pltpu.VMEM((6, PITCH, SIZE), jnp.float32),
                pltpu.VMEM((6, PITCH, SIZE), jnp.float32),
                pltpu.VMEM((BLOCK_STEPS, 6, SIZE, SIZE), jnp.float32),
                pltpu.VMEM((6, SIZE, SIZE), jnp.float32),
                pltpu.VMEM((6, 8, SIZE), jnp.float32),
                pltpu.VMEM((4, SIZE, SIZE), jnp.float32),
                pltpu.VMEM((3, 3, own, own), jnp.float32),
                pltpu.VMEM((3, own, own), jnp.float32),
                pltpu.VMEM((3, 6, 40, SIZE), jnp.float32),
                pltpu.VMEM((4, 6, 40, SIZE), jnp.float32),
                pltpu.VMEM((3, 3, 8, SIZE), jnp.float32),
                pltpu.VMEM((4, 3, 8, SIZE), jnp.float32),
            ] + [pltpu.SemaphoreType.DMA(shape) for shape in ((4, 6), (3, 3), (3,)) for _ in range(2)] + [
                pltpu.SemaphoreType.DMA((5,)),
                pltpu.SemaphoreType.REGULAR,
            ],
            compiler_params=pltpu.CompilerParams(collective_id=0, has_side_effects=True),
            name="advect",
        )(wind_scale, tracer, wind_a, wind_b, gain)
        return out

    field_spec = P(('member', 'panel'), 'tx', 'ty')
    wind_spec = P('panel', 'tx', 'ty')
    return jax.shard_map(local_run, mesh=mesh, in_specs=(field_spec, wind_spec, wind_spec, P()),
                         out_specs=field_spec, check_vma=False)


def kernel(own, steps, axis_names, ws_in, q_in, wa_in, wb_in, gain_in, out_ref,
           ws_ref, fields, qa_rows, qb_rows, sw, wf, wlast, coef, tiles, result, send, recv, csend, crecv,
           ssem, rsem, tsend, trecv, osend, orecv, isem, second):
    tx, ty, core = lax.axis_index('tx'), lax.axis_index('ty'), lax.axis_index('panel')
    by, bz, bx = tx, ty, lax.rem(core + tx + 1, 2)
    qa, qb = (rows.at[:, pl.ds(0, SIZE)] for rows in (qa_rows, qb_rows))

    def place(kx, ky, kc):
        return {name: {'tx': kx, 'ty': ky, 'panel': kc}.get(name, 0) for name in axis_names}

    def greet(semaphore):
        for other in (1, 2, 4, 5, 6):
            near = [1 - at if other & bit else at for at, bit in ((tx, 1), (ty, 2), (core, 4))]
            pl.semaphore_signal(semaphore, inc=1, device_id=place(*near), device_id_type=MESH)

    barrier = pltpu.get_barrier_semaphore()
    greet(barrier)
    loads = [pltpu.make_async_copy(src, dst, isem.at[n]) for n, (src, dst) in enumerate((
        (wa_in, fields.at[1]), (wb_in, fields.at[2]), (q_in, fields.at[0]), (gain_in, coef.at[0]), (ws_in, ws_ref)))]
    for load in loads:
        load.start()

    def at(ox, oy, oz):
        return place(oy, oz, lax.rem(ox + oy + 1, 2))

    def pick(first, second):
        return jnp.where(core == 0, first, second)

    homes = (
        (pick(1, tx), pick(tx, 0), ty, pick(0, 1)),
        (pick(1 - tx, 1 - ty), pick(1, tx), pick(ty, 1), pick(1, 2)),
        (pick(0, ty), pick(1 - tx, tx), pick(ty, 0), pick(0, 2)),
    )
    leaves = [jnp.logical_not((ox == bx) & (oy == by) & (oz == bz)) for ox, oy, oz, _ in homes]
    flip_a = (1 - lax.rem(bx + by, 2), lax.rem(bx + by, 2), by)
    flip_b = (bz, bz, jnp.where(bz == 1, 1 - bx, bx))
    panel = (jnp.where(bx == 1, 0, 2), jnp.where(by == 1, 1, 3), jnp.where(bz == 1, 4, 5))
    holder = [place(flip_a[n], flip_b[n], panel[n] // 3) for n in range(3)]
    slot_of = [lax.rem(panel[n], 3) for n in range(3)]
    comes = [jnp.logical_not((flip_a[n] == tx) & (flip_b[n] == ty) & (panel[n] // 3 == core)) for n in range(3)]

    def tile_copy(f, slot, quad, device):
        return pltpu.make_async_remote_copy(
            fields.at[f, slot], tiles.at[f, quad], tsend.at[f, slot], trecv.at[f, quad],
            device_id=device, device_id_type=MESH)

    for load in loads:
        load.wait()
    pl.semaphore_wait(barrier, 5)
    greet(second)
    for f in (1, 2, 0):
        for slot in range(3):
            ox, oy, oz, quad = homes[slot]

            @pl.when(leaves[slot])
            def _():
                tile_copy(f, slot, quad, at(ox, oy, oz)).start()

            @pl.when(jnp.logical_not(leaves[slot]))
            def _():
                tiles[f, quad] = fields[f, slot]

    def placing(shape, spot_axis, to_idx, flip):
        dist = to_idx(lax.broadcasted_iota(jnp.int32, shape, spot_axis))
        cell = lax.broadcasted_iota(jnp.int32, shape, 1 - spot_axis)
        source = jnp.where(dist < own, jnp.where(flip == 1, own - 1 - dist, dist), -1)
        return jnp.where(source == cell, 1.0, 0.0)

    def row_to_idx(row):
        return TILES * lax.rem(row, 8) + row // 8

    def lane_to_idx(spot):
        b = spot // 8
        half = (b + 1) // 2
        group = jnp.where(b > 2 * CENTRE, b, CENTRE - half + 2 * half * (1 - lax.rem(b, 2)))
        return TILES * lax.rem(spot, 8) + group

    def dot(lhs, rhs):
        return jnp.dot(lhs, rhs, precision=HIGHEST, preferred_element_type=jnp.float32)

    PLAIN = (0, 2, 5)

    sub = lax.broadcasted_iota(jnp.int32, (8, SIZE), 0)
    lane = lax.broadcasted_iota(jnp.int32, (8, SIZE), 1)
    lane_s, lane_i = lax.rem(lane, 8), lax.rem(lane_to_idx(lane), TILES)
    edge_lane = (lane_s == 5) & (lane_i >= EDGE)
    halo_lane = (lane_s >= 6) | edge_lane

    def group_lane(group, number):
        turns = jnp.where(group < CENTRE, 2 * (CENTRE - group) - 1, 2 * (group - CENTRE))
        return 8 * jnp.where(group > 2 * CENTRE, group, turns) + number

    def mirror_lane(group, number):
        return group_lane(lax.rem(19 - group, TILES), jnp.where(group < 4, 11, EDGE) - number)

    odd_row = lax.rem(sub, 2)
    row_pair, lane_pair = sub // 2, lane_s // 2
    high, mid = lane_i >= EDGE, (lane_i >= 4) & (lane_i < EDGE)
    edge_group = jnp.where(mid, lane_i + 6, lane_i)
    at_edge = ((lane_s == 5) | (lane_s == 7)) & (high | mid)
    source_vreg = jnp.where(at_edge, jnp.where(lane_s == 7, 0, 2) + jnp.where(high, 0, 1), lane_pair)
    source_lane = jnp.where(at_edge, mirror_lane(edge_group, 5), mirror_lane(lane_i, 6 + lax.rem(lane, 2)))
    at_four = lane_s == 4
    takes_first = (odd_row == 1) & ((lane_s == 1) | (lane_s == 3) | (at_four & high))
    takes_last = (odd_row == 1) & ((lane_s == 6) | (at_four & mid))
    first_src = jnp.where(takes_first, mirror_lane(lane_i, jnp.where(at_four, 5, 6 + lane_s // 2)), 0)
    last_src = jnp.where(takes_last, mirror_lane(jnp.where(at_four, edge_group, lane_i), jnp.where(at_four, 5, 6 + sub // 4)), 0)
    low_group = lane_i - 6
    edge_back = [group_lane(lane_i, 7), group_lane(low_group, 7), group_lane(lane_i, 5), group_lane(low_group, 5)]
    msg_back = [jnp.where(lane_s >= 6, lane - 6 + 2 * j, jnp.where(edge_lane, edge_back[j], 0)) for j in range(4)]
    first_back = jnp.where(lane_s >= 6, lane + lane_s - 11, jnp.where(edge_lane, lane - 1, 0))
    last_back = jnp.where(lane_s >= 6, lane - lane_s + 6, jnp.where(edge_lane, group_lane(low_group, 4), 0))
    last_row = 1 + 2 * jnp.where((sub >= 4) & (lane_s < 7), odd_row, lax.rem(sub + 2 * (sub // 4), 4))

    def rows_by(arr, idx):
        return jnp.take_along_axis(arr, idx, axis=0, mode="promise_in_bounds")

    def lanes_by(arr, idx):
        return jnp.take_along_axis(arr, idx, axis=1, mode="promise_in_bounds")

    def by_number(number, parts):
        res = parts[0]
        for m, part in enumerate(parts):
            res = jnp.where(number == m, part, res) if m else res
        return res

    def peer(mirrored):
        return at(*(1 - b if m else b for b, m in zip((bx, by, bz), mirrored)))

    def strip_copy(axis, out, slot):
        return pltpu.make_async_remote_copy(
            send.at[out, pl.ds(2 * axis, 2)], recv.at[slot, pl.ds(2 * axis, 2)], ssem.at[slot, axis], rsem.at[slot, axis],
            device_id=peer(tuple(int(n == axis) for n in range(3))), device_id_type=MESH)

    def corner_copy(k, out, slot):
        n = k // 2
        return pltpu.make_async_remote_copy(
            csend.at[out, n], crecv.at[slot, n], ssem.at[slot, 3 + n], rsem.at[slot, 3 + n],
            device_id=peer(CORNERS[k]), device_id_type=MESH)

    def signed(sign, arr):
        return arr if sign == 1.0 else sign * arr

    def pack(arrs, k, out, sign):
        axis, n = STRIP_PLACE[k]
        a = tiles_of(arrs[k])

        def mirrored(i, sublane):
            return rows_by(a[(19 - i) % TILES], sublane)

        msg = [by_number(row_pair, [mirrored(i, (5 if i < 4 else 4) - odd_row) for i in range(4 * j, 4 * j + 4)])
               for j in range(4)]
        tail = [mirrored(i, 5 + 0 * sub) for i in range(EDGE, TILES)] + [mirrored(i, 3 + 0 * sub) for i in range(2)]
        msg = [signed(sign, part) for part in msg + [by_number(sub, tail)]]
        send[out, 2 * axis + n] = join(msg)
        return msg

    def pack_corner(k, packed, out, corner_sign):
        *msg, tail = packed
        block = by_number(source_vreg, [lanes_by(m, source_lane) for m in msg])
        first = lanes_by(rows_by(tail, row_pair), first_src)
        last = lanes_by(rows_by(tail, 4 + lax.rem(row_pair, 2)), last_src)
        block = jnp.where(takes_first, first, jnp.where(takes_last, last, block))
        csend[out, k // 2] = signed(corner_sign, block)

    def sender(arrs, out, slot, sign=1.0, corner_sign=1.0):
        packed = [pack(arrs, k, out, sign) for k in (1, 3)]
        strip_copy(2, out, slot).start()
        for k, msg in zip((1, 3), packed):
            pack_corner(k, msg, out, corner_sign)
        for k in (1, 3):
            corner_copy(k, out, slot).start()
        yield
        for k in (0, 2):
            pack(arrs, k, out, sign)
        yield
        pack_corner(4, pack(arrs, 4, out, sign), out, corner_sign)
        corner_copy(4, out, slot).start()
        pack(arrs, 5, out, sign)
        strip_copy(1, out, slot).start()
        strip_copy(0, out, slot).start()
        yield

    def strip(k, slot):
        axis, n = STRIP_PLACE[k]
        return tiles_of(recv[slot, 2 * axis + n])

    def halo_tiles(k, slot):
        *msg, tail = strip(k, slot)
        if k in CORNERS:
            block = crecv[slot, k // 2]
            msg = [jnp.where(halo_lane, lanes_by(block, msg_back[j]), msg[j]) for j in range(4)]
            last = rows_by(lanes_by(block, last_back), last_row)
            tail = jnp.where(halo_lane, jnp.where(sub < 4, rows_by(lanes_by(block, first_back), last_row), last), tail)
        res = [roll_rows(msg[i // 4], 6 - 2 * (i % 4)) for i in range(TILES)]
        for i in range(EDGE, TILES):
            res[i] = jnp.where(sub == 5, roll_rows(tail, 15 - i), res[i])
        return res

    def wait_all(out, slot):
        for axis in (0, 1):
            strip_copy(axis, out, slot).wait()
        for k in (3, 4, 1):
            corner_copy(k, out, slot).wait()
        strip_copy(2, out, slot).wait()

    def merge(arrs, k, rows, lanes):
        side = tiles_of(lanes)
        for i in range(TILES):
            own_rows = sub < (6 if i < EDGE else 5)
            sideways = halo_lane & own_rows if k in CORNERS else halo_lane
            arrs[k, tile(i)] = jnp.where(sideways, side[i], jnp.where(own_rows, arrs[k, tile(i)], rows[i]))

    def finish(slot):
        wait_all(0, slot)
        halos = {k: halo_tiles(k, slot) for k in (0, 2, 5, 1, 3, 4)}
        lanes = {TWIN[k]: turn(join(halos[k])) for k in (0, 2, 5, 1, 3, 4)}
        for k in (0, 2, 4, 1, 3, 5):
            merge(qa, k, halos[k], lanes[k])

    def scale_faces(first_step):
        def one(step, carry):
            scale = ws_ref[lax.rem(first_step + step, steps)]
            sw[step] = scale * wf[...]
            return carry
        lax.fori_loop(0, BLOCK_STEPS, one, 0)

    for f in (1, 2, 0):
        for slot in range(3):
            ox, oy, oz, quad = homes[slot]

            @pl.when(leaves[slot])
            def _():
                tile_copy(f, slot, quad, at(ox, oy, oz)).wait_send()
        for quad in range(3):
            @pl.when(comes[quad])
            def _():
                tile_copy(f, 0, quad, holder[quad]).wait_recv()
        for quad in range(3):
            loc = dot(dot(placing((SIZE, own), 0, row_to_idx, flip_a[quad]), tiles[f, quad]),
                      placing((own, SIZE), 1, lane_to_idx, flip_b[quad]))
            plain, turned = PLAIN[quad], TWIN[PLAIN[quad]]
            if f == 0:
                qa[plain] = loc
                qa[turned] = turn(loc)
            elif f == 1:
                loc = jnp.where(flip_a[quad] == 1, -1.0, 1.0) * loc
                qb[plain] = loc
                sw[0, turned] = turn(loc)
            else:
                loc = jnp.where(flip_b[quad] == 1, -1.0, 1.0) * loc
                sw[0, plain] = loc
                qb[turned] = turn(loc)
        if f == 2:
            pl.semaphore_wait(second, 5)
            list(sender(qb, 1, 2, sign=-1.0))
            list(sender(sw.at[0], 2, 3, corner_sign=-1.0))
    list(sender(qa, 0, 0))

    coef[1] = 1.0 - 4.0 * coef[0]
    coef[2] = 0.5 * coef[0]
    coef[3] = 0.5 - 2.0 * coef[0]

    wait_all(1, 2)
    wait_all(2, 3)
    for k in ARRAYS:
        merge(qb, k, halo_tiles(k, 2), turn(join(halo_tiles(TWIN[k], 3))))
    for k in ARRAYS:
        here = qb[k]
        scaled = 0.5 / (6.0 * C_SPEED)
        after = join([here[8:], roll_rows(here[:8], -1)])
        beyond = jnp.where(sub == 7, roll_rows(strip(k, 2)[-1], 1), after[-8:])
        wf[k] = scaled * (here + after)
        wf[k, row(15, 7)] = scaled * (here[:1] - qb[ACROSS[k], row(0)])
        wlast[k] = scaled * (here[-8:] + beyond)
    scale_faces(0)

    def x_part(a_ref, k, faces, ghosts=False, beyond=None):
        a = a_ref[k]
        first, last = a[:8], a[-8:]
        below, above = roll_rows(last, 1), roll_rows(first, -1)
        if ghosts:
            below = jnp.where(sub == 0, a_ref[ACROSS[k], tile(0)], below)
        if beyond is not None:
            above = jnp.where(sub == 7, roll_rows(beyond[0], 1), above)
        m = join([below, a[:-8]]) + join([a[8:], above])
        v = 8.0 * a - m
        v_above, here = roll_rows(v[:8], -1), faces
        if beyond is not None:
            v_above = 8.0 * above - (last + jnp.where(sub == 7, beyond[0], roll_rows(a[8:16], -1)))
            here = join([faces[:-8], beyond[1]])
        flux = here * (v + join([v[8:], v_above]))
        flux_below = roll_rows(flux[-8:], 1)
        if ghosts:
            v_below = 8.0 * below - (jnp.where(sub == 0, a_ref[ACROSS[k], tile(1)], roll_rows(a[-16:-8], 1)) + first)
            flux_below = roll_rows(faces[-8:], 1) * (v_below + v[:8])
        return (m - flux) + join([flux_below, flux[:-8]])

    def parts_of(src, dst, second, step, group, ghosts, scale, slot):
        part = {}
        for k in group:
            beyond = None if scale is None else (strip(k, slot)[-1], scale * wlast[k])
            part[k] = coef[2 if second else 0] * x_part(src, k, sw[step, k], ghosts, beyond)
            if k in PRIMARY:
                own_part = coef[3 if second else 1] * src[k]
                if second:
                    own_part = 0.5 * dst[k] + own_part
                part[k] = own_part + part[k]
        return part, {k: turn(part[k]) for k in group}

    def stage(src, dst, second, step, ghosts=False, scale=None, slot=None, sends=None):
        part, turned = {}, {}
        for group in GROUPS:
            more = parts_of(src, dst, second, step, group, ghosts, scale, slot)
            part.update(more[0])
            turned.update(more[1])
        new = {}
        for group in ((1, 3), (0, 2), (4, 5)):
            for k in group:
                new[k] = part[k] + turned[TWIN[k]]
            for k in group:
                dst[k] = new[k]
            if sends is not None:
                next(sends)
        if sends is None and scale is None:
            for k in ARRAYS:
                near = new[ACROSS[k]]
                dst[k, row(14, 7)] = near[8:9]
                dst[k, row(15, 7)] = near[:1]

    def run_block(first_step, count, slot, sends):
        finish(slot)
        stage(qa, qb, False, 0, ghosts=True, scale=ws_ref[first_step], slot=slot)
        stage(qb, qa, True, 0, ghosts=True)

        def one_step(step, carry):
            stage(qa, qb, False, step)
            stage(qb, qa, True, step)
            return carry

        lax.fori_loop(1, count - 1, one_step, 0, unroll=True)
        stage(qa, qb, False, count - 1)
        stage(qb, qa, True, count - 1, sends=sends)

    full_blocks = (steps - 1) // BLOCK_STEPS

    def block(blk, carry):
        out_slot = lax.rem(blk + 1, 2)
        run_block(blk * BLOCK_STEPS, BLOCK_STEPS, lax.rem(blk, 2), sender(qa, 0, out_slot))
        scale_faces((blk + 1) * BLOCK_STEPS)
        return carry

    lax.fori_loop(0, full_blocks, block, 0)
    run_block(full_blocks * BLOCK_STEPS, steps - full_blocks * BLOCK_STEPS, full_blocks % 2, iter(range(3)))

    def result_copy(quad, slot, device, number):
        return pltpu.make_async_remote_copy(
            result.at[quad], out_ref.at[slot], osend.at[number], orecv.at[slot],
            device_id=device, device_id_type=MESH)

    for quad in range(3):
        result[quad] = dot(dot(placing((own, SIZE), 1, row_to_idx, flip_a[quad]), qa[PLAIN[quad]]),
                           placing((SIZE, own), 0, lane_to_idx, flip_b[quad]))

        @pl.when(comes[quad])
        def _():
            result_copy(quad, slot_of[quad], holder[quad], quad).start()

        @pl.when(jnp.logical_not(comes[quad]))
        def _():
            pltpu.make_async_copy(result.at[quad], out_ref.at[slot_of[quad]], osend.at[quad]).start()

    for quad in range(3):
        @pl.when(comes[quad])
        def _():
            result_copy(quad, slot_of[quad], holder[quad], quad).wait_send()

        @pl.when(jnp.logical_not(comes[quad]))
        def _():
            pltpu.make_async_copy(result.at[quad], out_ref.at[slot_of[quad]], osend.at[quad]).wait()
    for slot in range(3):
        ox, oy, oz, _ = homes[slot]

        @pl.when(leaves[slot])
        def _():
            result_copy(0, slot, at(ox, oy, oz), 0).wait_recv()
```

```python
import functools
import math

import jax
import jax.numpy as jnp
import numpy as np
from jax import lax
from jax.experimental import pallas as pl
from jax.experimental.pallas import tpu as pltpu
from jax.sharding import PartitionSpec as P

C_SPEED = 2.5
CFL_STEP = 0.12
MESH = pl.DeviceIdType.MESH
HIGHEST = lax.Precision.HIGHEST

ARRAYS = range(6)
TWIN = tuple(k ^ 1 for k in ARRAYS)
ACROSS = (2, 4, 0, 5, 1, 3)
PRIMARY = (0, 2, 4)
STRIPS = ((2, 4), (0, 5), (1, 3))
STRIP_PLACE = {k: (axis, n) for axis, pair in enumerate(STRIPS) for n, k in enumerate(pair)}
CORNERS = {1: (0, 1, 1), 3: (1, 0, 1), 4: (1, 1, 0)}

SIZE = 128
TILES = 16
PITCH = SIZE + 48
CENTRE = 7
EDGE = 10
BLOCK_STEPS = 10
FIRST, SECOND, THIRD = GROUPS = ((0, 2), (1, 3), (5, 4))


def row_idx(row):
    return TILES * (row % 8) + row // 8


def lane_group(b):
    half = (b + 1) // 2
    return np.where(b > 2 * CENTRE, b, CENTRE - half + 2 * half * (1 - b % 2))


LANE_ORDER = tuple(int(lane_group(b)) for b in range(TILES))


def tile(i):
    return pl.ds(8 * i, 8)


def row(i, sublane=0):
    return pl.ds(8 * i + sublane, 1)


def tiles_of(arr):
    return jnp.split(arr, arr.shape[0] // 8)


def join(tiles):
    return jnp.concatenate(tiles)


def roll_rows(tile, shift):
    return pltpu.roll(tile, shift % 8, 0)


def turn(arr):
    tiles = tiles_of(arr)
    turned = tiles_of(join([tiles[i] for i in LANE_ORDER]).T)
    return join([turned[LANE_ORDER.index(i)] for i in range(TILES)])


def solution(mesh):
    axis_names = mesh.axis_names

    def local_run(tracer, wind_a, wind_b, wind_scale):
        own = tracer.shape[1]
        cells = 2 * own
        steps = wind_scale.shape[0]
        dalpha = 0.5 * math.pi / cells
        place = np.arange(SIZE)
        lane_idx = TILES * (place % 8) + lane_group(place // 8)
        tan_a = np.tan((row_idx(place) + 0.5) * dalpha - 0.25 * math.pi)[:, None]
        tan_b = np.tan((lane_idx + 0.5) * dalpha - 0.25 * math.pi)[None, :]
        r_sq = 1.0 + tan_a * tan_a + tan_b * tan_b
        inv_sqrt_g = r_sq * np.sqrt(r_sq) / ((1.0 + tan_a * tan_a) * (1.0 + tan_b * tan_b))
        gain = (0.5 * C_SPEED * CFL_STEP * inv_sqrt_g).astype(np.float32)
        out = pl.pallas_call(
            functools.partial(kernel, own, steps, axis_names),
            out_shape=jax.ShapeDtypeStruct(tracer.shape, jnp.float32),
            in_specs=[pl.BlockSpec(memory_space=pl.ANY)] * 5,
            out_specs=pl.BlockSpec(memory_space=pl.ANY),
            scratch_shapes=[
                pltpu.SMEM((steps,), jnp.float32),
                pltpu.VMEM((3, 3, own, own), jnp.float32),
                pltpu.VMEM((6, PITCH, SIZE), jnp.float32),
                pltpu.VMEM((6, PITCH, SIZE), jnp.float32),
                pltpu.VMEM((BLOCK_STEPS, 6, SIZE, SIZE), jnp.float32),
                pltpu.VMEM((6, SIZE, SIZE), jnp.float32),
                pltpu.VMEM((6, 8, SIZE), jnp.float32),
                pltpu.VMEM((4, SIZE, SIZE), jnp.float32),
                pltpu.VMEM((3, 3, own, own), jnp.float32),
                pltpu.VMEM((3, own, own), jnp.float32),
                pltpu.VMEM((3, 6, 40, SIZE), jnp.float32),
                pltpu.VMEM((4, 6, 40, SIZE), jnp.float32),
                pltpu.VMEM((3, 3, 8, SIZE), jnp.float32),
                pltpu.VMEM((4, 3, 8, SIZE), jnp.float32),
            ] + [pltpu.SemaphoreType.DMA(shape) for shape in ((4, 6), (3, 3), (3,)) for _ in range(2)] + [
                pltpu.SemaphoreType.DMA((5,)),
                pltpu.SemaphoreType.REGULAR,
            ],
            compiler_params=pltpu.CompilerParams(collective_id=0, has_side_effects=True),
            name="advect",
        )(wind_scale, tracer, wind_a, wind_b, gain)
        return out

    field_spec = P(('member', 'panel'), 'tx', 'ty')
    wind_spec = P('panel', 'tx', 'ty')
    return jax.shard_map(local_run, mesh=mesh, in_specs=(field_spec, wind_spec, wind_spec, P()),
                         out_specs=field_spec, check_vma=False)


def kernel(own, steps, axis_names, ws_in, q_in, wa_in, wb_in, gain_in, out_ref,
           ws_ref, fields, qa_rows, qb_rows, sw, wf, wlast, coef, tiles, result, send, recv, csend, crecv,
           ssem, rsem, tsend, trecv, osend, orecv, isem, second):
    tx, ty, core = lax.axis_index('tx'), lax.axis_index('ty'), lax.axis_index('panel')
    by, bz, bx = tx, ty, lax.rem(core + tx + 1, 2)
    qa, qb = (rows.at[:, pl.ds(0, SIZE)] for rows in (qa_rows, qb_rows))

    def place(kx, ky, kc):
        return {name: {'tx': kx, 'ty': ky, 'panel': kc}.get(name, 0) for name in axis_names}

    def greet(semaphore):
        for other in (1, 2, 4, 5, 6):
            near = [1 - at if other & bit else at for at, bit in ((tx, 1), (ty, 2), (core, 4))]
            pl.semaphore_signal(semaphore, inc=1, device_id=place(*near), device_id_type=MESH)

    barrier = pltpu.get_barrier_semaphore()
    greet(barrier)
    loads = [pltpu.make_async_copy(src, dst, isem.at[n]) for n, (src, dst) in enumerate((
        (wa_in, fields.at[1]), (wb_in, fields.at[2]), (q_in, fields.at[0]), (gain_in, coef.at[0]), (ws_in, ws_ref)))]
    for load in loads:
        load.start()

    def at(ox, oy, oz):
        return place(oy, oz, lax.rem(ox + oy + 1, 2))

    def pick(first, second):
        return jnp.where(core == 0, first, second)

    homes = (
        (pick(1, tx), pick(tx, 0), ty, pick(0, 1)),
        (pick(1 - tx, 1 - ty), pick(1, tx), pick(ty, 1), pick(1, 2)),
        (pick(0, ty), pick(1 - tx, tx), pick(ty, 0), pick(0, 2)),
    )
    leaves = [jnp.logical_not((ox == bx) & (oy == by) & (oz == bz)) for ox, oy, oz, _ in homes]
    flip_a = (1 - lax.rem(bx + by, 2), lax.rem(bx + by, 2), by)
    flip_b = (bz, bz, jnp.where(bz == 1, 1 - bx, bx))
    panel = (jnp.where(bx == 1, 0, 2), jnp.where(by == 1, 1, 3), jnp.where(bz == 1, 4, 5))
    holder = [place(flip_a[n], flip_b[n], panel[n] // 3) for n in range(3)]
    slot_of = [lax.rem(panel[n], 3) for n in range(3)]
    comes = [jnp.logical_not((flip_a[n] == tx) & (flip_b[n] == ty) & (panel[n] // 3 == core)) for n in range(3)]

    def tile_copy(f, slot, quad, device):
        return pltpu.make_async_remote_copy(
            fields.at[f, slot], tiles.at[f, quad], tsend.at[f, slot], trecv.at[f, quad],
            device_id=device, device_id_type=MESH)

    for load in loads:
        load.wait()
    pl.semaphore_wait(barrier, 5)
    greet(second)
    for f in (1, 2, 0):
        for slot in range(3):
            ox, oy, oz, quad = homes[slot]

            @pl.when(leaves[slot])
            def _():
                tile_copy(f, slot, quad, at(ox, oy, oz)).start()

            @pl.when(jnp.logical_not(leaves[slot]))
            def _():
                tiles[f, quad] = fields[f, slot]

    def placing(shape, spot_axis, to_idx, flip):
        dist = to_idx(lax.broadcasted_iota(jnp.int32, shape, spot_axis))
        cell = lax.broadcasted_iota(jnp.int32, shape, 1 - spot_axis)
        source = jnp.where(dist < own, jnp.where(flip == 1, own - 1 - dist, dist), -1)
        return jnp.where(source == cell, 1.0, 0.0)

    def row_to_idx(row):
        return TILES * lax.rem(row, 8) + row // 8

    def lane_to_idx(spot):
        b = spot // 8
        half = (b + 1) // 2
        group = jnp.where(b > 2 * CENTRE, b, CENTRE - half + 2 * half * (1 - lax.rem(b, 2)))
        return TILES * lax.rem(spot, 8) + group

    def dot(lhs, rhs):
        return jnp.dot(lhs, rhs, precision=HIGHEST, preferred_element_type=jnp.float32)

    PLAIN = (0, 2, 5)

    sub = lax.broadcasted_iota(jnp.int32, (8, SIZE), 0)
    lane = lax.broadcasted_iota(jnp.int32, (8, SIZE), 1)
    lane_s, lane_i = lax.rem(lane, 8), lax.rem(lane_to_idx(lane), TILES)
    edge_lane = (lane_s == 5) & (lane_i >= EDGE)
    halo_lane = (lane_s >= 6) | edge_lane

    def group_lane(group, number):
        turns = jnp.where(group < CENTRE, 2 * (CENTRE - group) - 1, 2 * (group - CENTRE))
        return 8 * jnp.where(group > 2 * CENTRE, group, turns) + number

    def mirror_lane(group, number):
        return group_lane(lax.rem(19 - group, TILES), jnp.where(group < 4, 11, EDGE) - number)

    odd_row = lax.rem(sub, 2)
    row_pair, lane_pair = sub // 2, lane_s // 2
    high, mid = lane_i >= EDGE, (lane_i >= 4) & (lane_i < EDGE)
    edge_group = jnp.where(mid, lane_i + 6, lane_i)
    at_edge = ((lane_s == 5) | (lane_s == 7)) & (high | mid)
    source_vreg = jnp.where(at_edge, jnp.where(lane_s == 7, 0, 2) + jnp.where(high, 0, 1), lane_pair)
    source_lane = jnp.where(at_edge, mirror_lane(edge_group, 5), mirror_lane(lane_i, 6 + lax.rem(lane, 2)))
    at_four = lane_s == 4
    takes_first = (odd_row == 1) & ((lane_s == 1) | (lane_s == 3) | (at_four & high))
    takes_last = (odd_row == 1) & ((lane_s == 6) | (at_four & mid))
    first_src = jnp.where(takes_first, mirror_lane(lane_i, jnp.where(at_four, 5, 6 + lane_s // 2)), 0)
    last_src = jnp.where(takes_last, mirror_lane(jnp.where(at_four, edge_group, lane_i), jnp.where(at_four, 5, 6 + sub // 4)), 0)
    low_group = lane_i - 6
    edge_back = [group_lane(lane_i, 7), group_lane(low_group, 7), group_lane(lane_i, 5), group_lane(low_group, 5)]
    msg_back = [jnp.where(lane_s >= 6, lane - 6 + 2 * j, jnp.where(edge_lane, edge_back[j], 0)) for j in range(4)]
    first_back = jnp.where(lane_s >= 6, lane + lane_s - 11, jnp.where(edge_lane, lane - 1, 0))
    last_back = jnp.where(lane_s >= 6, lane - lane_s + 6, jnp.where(edge_lane, group_lane(low_group, 4), 0))
    last_row = 1 + 2 * jnp.where((sub >= 4) & (lane_s < 7), odd_row, lax.rem(sub + 2 * (sub // 4), 4))

    def rows_by(arr, idx):
        return jnp.take_along_axis(arr, idx, axis=0, mode="promise_in_bounds")

    def lanes_by(arr, idx):
        return jnp.take_along_axis(arr, idx, axis=1, mode="promise_in_bounds")

    def by_number(number, parts):
        res = parts[0]
        for m, part in enumerate(parts):
            res = jnp.where(number == m, part, res) if m else res
        return res

    def peer(mirrored):
        return at(*(1 - b if m else b for b, m in zip((bx, by, bz), mirrored)))

    def strip_copy(axis, out, slot):
        return pltpu.make_async_remote_copy(
            send.at[out, pl.ds(2 * axis, 2)], recv.at[slot, pl.ds(2 * axis, 2)], ssem.at[slot, axis], rsem.at[slot, axis],
            device_id=peer(tuple(int(n == axis) for n in range(3))), device_id_type=MESH)

    def corner_copy(k, out, slot):
        n = k // 2
        return pltpu.make_async_remote_copy(
            csend.at[out, n], crecv.at[slot, n], ssem.at[slot, 3 + n], rsem.at[slot, 3 + n],
            device_id=peer(CORNERS[k]), device_id_type=MESH)

    def signed(sign, arr):
        return arr if sign == 1.0 else sign * arr

    def pack(arrs, k, out, sign):
        axis, n = STRIP_PLACE[k]
        a = tiles_of(arrs[k])

        def mirrored(i, sublane):
            return rows_by(a[(19 - i) % TILES], sublane)

        msg = [by_number(row_pair, [mirrored(i, (5 if i < 4 else 4) - odd_row) for i in range(4 * j, 4 * j + 4)])
               for j in range(4)]
        tail = [mirrored(i, 5 + 0 * sub) for i in range(EDGE, TILES)] + [mirrored(i, 3 + 0 * sub) for i in range(2)]
        msg = [signed(sign, part) for part in msg + [by_number(sub, tail)]]
        send[out, 2 * axis + n] = join(msg)
        return msg

    def pack_corner(k, packed, out, corner_sign):
        *msg, tail = packed
        block = by_number(source_vreg, [lanes_by(m, source_lane) for m in msg])
        first = lanes_by(rows_by(tail, row_pair), first_src)
        last = lanes_by(rows_by(tail, 4 + lax.rem(row_pair, 2)), last_src)
        block = jnp.where(takes_first, first, jnp.where(takes_last, last, block))
        csend[out, k // 2] = signed(corner_sign, block)

    def sender(arrs, out, slot, sign=1.0, corner_sign=1.0):
        packed = [pack(arrs, k, out, sign) for k in (1, 3)]
        strip_copy(2, out, slot).start()
        for k, msg in zip((1, 3), packed):
            pack_corner(k, msg, out, corner_sign)
        for k in (1, 3):
            corner_copy(k, out, slot).start()
        yield
        for k in (0, 2):
            pack(arrs, k, out, sign)
        yield
        pack_corner(4, pack(arrs, 4, out, sign), out, corner_sign)
        corner_copy(4, out, slot).start()
        pack(arrs, 5, out, sign)
        strip_copy(1, out, slot).start()
        strip_copy(0, out, slot).start()
        yield

    def strip(k, slot):
        axis, n = STRIP_PLACE[k]
        return tiles_of(recv[slot, 2 * axis + n])

    def halo_tiles(k, slot):
        *msg, tail = strip(k, slot)
        if k in CORNERS:
            block = crecv[slot, k // 2]
            msg = [jnp.where(halo_lane, lanes_by(block, msg_back[j]), msg[j]) for j in range(4)]
            last = rows_by(lanes_by(block, last_back), last_row)
            tail = jnp.where(halo_lane, jnp.where(sub < 4, rows_by(lanes_by(block, first_back), last_row), last), tail)
        res = [roll_rows(msg[i // 4], 6 - 2 * (i % 4)) for i in range(TILES)]
        for i in range(EDGE, TILES):
            res[i] = jnp.where(sub == 5, roll_rows(tail, 15 - i), res[i])
        return res

    def wait_all(out, slot):
        for axis in (0, 1):
            strip_copy(axis, out, slot).wait()
        for k in (3, 4, 1):
            corner_copy(k, out, slot).wait()
        strip_copy(2, out, slot).wait()

    def merge(arrs, k, rows, lanes):
        side = tiles_of(lanes)
        for i in range(TILES):
            own_rows = sub < (6 if i < EDGE else 5)
            sideways = halo_lane & own_rows if k in CORNERS else halo_lane
            arrs[k, tile(i)] = jnp.where(sideways, side[i], jnp.where(own_rows, arrs[k, tile(i)], rows[i]))

    def finish(slot):
        wait_all(0, slot)
        halos = {k: halo_tiles(k, slot) for k in (0, 2, 5, 1, 3, 4)}
        lanes = {TWIN[k]: turn(join(halos[k])) for k in (0, 2, 5, 1, 3, 4)}
        for k in (*SECOND, *FIRST, 4, 5):
            merge(qa, k, halos[k], lanes[k])

    def scale_faces(first_step):
        def one(step, carry):
            scale = ws_ref[lax.rem(first_step + step, steps)]
            sw[step] = scale * wf[...]
            return carry
        lax.fori_loop(0, BLOCK_STEPS, one, 0)

    for f in (1, 2, 0):
        for slot in range(3):
            ox, oy, oz, quad = homes[slot]

            @pl.when(leaves[slot])
            def _():
                tile_copy(f, slot, quad, at(ox, oy, oz)).wait_send()
        for quad in range(3):
            @pl.when(comes[quad])
            def _():
                tile_copy(f, 0, quad, holder[quad]).wait_recv()
        for quad in range(3):
            loc = dot(dot(placing((SIZE, own), 0, row_to_idx, flip_a[quad]), tiles[f, quad]),
                      placing((own, SIZE), 1, lane_to_idx, flip_b[quad]))
            plain, turned = PLAIN[quad], TWIN[PLAIN[quad]]
            if f == 0:
                qa[plain] = loc
                qa[turned] = turn(loc)
            elif f == 1:
                loc = jnp.where(flip_a[quad] == 1, -1.0, 1.0) * loc
                qb[plain] = loc
                sw[0, turned] = turn(loc)
            else:
                loc = jnp.where(flip_b[quad] == 1, -1.0, 1.0) * loc
                sw[0, plain] = loc
                qb[turned] = turn(loc)
        if f == 2:
            pl.semaphore_wait(second, 5)
            list(sender(qb, 1, 2, sign=-1.0))
            list(sender(sw.at[0], 2, 3, corner_sign=-1.0))
    list(sender(qa, 0, 0))

    coef[1] = 1.0 - 4.0 * coef[0]
    coef[2] = 0.5 * coef[0]
    coef[3] = 0.5 - 2.0 * coef[0]

    wait_all(1, 2)
    wait_all(2, 3)
    for k in ARRAYS:
        merge(qb, k, halo_tiles(k, 2), turn(join(halo_tiles(TWIN[k], 3))))
    for k in ARRAYS:
        here = qb[k]
        scaled = 0.5 / (6.0 * C_SPEED)
        after = join([here[8:], roll_rows(here[:8], -1)])
        beyond = jnp.where(sub == 7, roll_rows(strip(k, 2)[-1], 1), after[-8:])
        wf[k] = scaled * (here + after)
        wf[k, row(15, 7)] = scaled * (here[:1] - qb[ACROSS[k], row(0)])
        wlast[k] = scaled * (here[-8:] + beyond)
    scale_faces(0)

    def x_part(a_ref, k, faces, ghosts=False, beyond=None):
        a = a_ref[k]
        first, last = a[:8], a[-8:]
        below, above = roll_rows(last, 1), roll_rows(first, -1)
        if ghosts:
            below = jnp.where(sub == 0, a_ref[ACROSS[k], tile(0)], below)
        if beyond is not None:
            above = jnp.where(sub == 7, roll_rows(beyond[0], 1), above)
        m = join([below, a[:-8]]) + join([a[8:], above])
        v = 8.0 * a - m
        v_above, here = roll_rows(v[:8], -1), faces
        if beyond is not None:
            v_above = 8.0 * above - (last + jnp.where(sub == 7, beyond[0], roll_rows(a[8:16], -1)))
            here = join([faces[:-8], beyond[1]])
        flux = here * (v + join([v[8:], v_above]))
        flux_below = roll_rows(flux[-8:], 1)
        if ghosts:
            v_below = 8.0 * below - (jnp.where(sub == 0, a_ref[ACROSS[k], tile(1)], roll_rows(a[-16:-8], 1)) + first)
            flux_below = roll_rows(faces[-8:], 1) * (v_below + v[:8])
        return (m - flux) + join([flux_below, flux[:-8]])

    def parts_of(src, dst, second, step, group, ghosts, scale, slot):
        part = {}
        for k in group:
            beyond = None if scale is None else (strip(k, slot)[-1], scale * wlast[k])
            part[k] = coef[2 if second else 0] * x_part(src, k, sw[step, k], ghosts, beyond)
            if k in PRIMARY:
                own_part = coef[3 if second else 1] * src[k]
                if second:
                    own_part = 0.5 * dst[k] + own_part
                part[k] = own_part + part[k]
        return part, {k: turn(part[k]) for k in group}

    def stage(src, dst, second, step, ghosts=False, scale=None, slot=None, sends=None):
        part, turned = {}, {}
        for group in GROUPS:
            more = parts_of(src, dst, second, step, group, ghosts, scale, slot)
            part.update(more[0])
            turned.update(more[1])
            if group is FIRST:
                for k in group:
                    dst[k] = part[k]
        new = {}
        for group in (SECOND, FIRST, THIRD):
            for k in group:
                new[k] = (dst[k] if group is FIRST else part[k]) + turned[TWIN[k]]
            for k in group:
                dst[k] = new[k]
            if sends is not None:
                next(sends)
        if sends is None and scale is None:
            for k in ARRAYS:
                near = new[ACROSS[k]]
                dst[k, row(14, 7)] = near[8:9]
                dst[k, row(15, 7)] = near[:1]

    def run_block(first_step, count, slot, sends):
        finish(slot)
        stage(qa, qb, False, 0, ghosts=True, scale=ws_ref[first_step], slot=slot)
        stage(qb, qa, True, 0, ghosts=True)

        def one_step(step, carry):
            stage(qa, qb, False, step)
            stage(qb, qa, True, step)
            return carry

        lax.fori_loop(1, count - 1, one_step, 0, unroll=True)
        stage(qa, qb, False, count - 1)
        stage(qb, qa, True, count - 1, sends=sends)

    full_blocks = (steps - 1) // BLOCK_STEPS

    def block(blk, carry):
        out_slot = lax.rem(blk + 1, 2)
        run_block(blk * BLOCK_STEPS, BLOCK_STEPS, lax.rem(blk, 2), sender(qa, 0, out_slot))
        scale_faces((blk + 1) * BLOCK_STEPS)
        return carry

    lax.fori_loop(0, full_blocks, block, 0)
    run_block(full_blocks * BLOCK_STEPS, steps - full_blocks * BLOCK_STEPS, full_blocks % 2, iter(range(3)))

    def result_copy(quad, slot, device, number):
        return pltpu.make_async_remote_copy(
            result.at[quad], out_ref.at[slot], osend.at[number], orecv.at[slot],
            device_id=device, device_id_type=MESH)

    for quad in range(3):
        result[quad] = dot(dot(placing((own, SIZE), 1, row_to_idx, flip_a[quad]), qa[PLAIN[quad]]),
                           placing((SIZE, own), 0, lane_to_idx, flip_b[quad]))

        @pl.when(comes[quad])
        def _():
            result_copy(quad, slot_of[quad], holder[quad], quad).start()

        @pl.when(jnp.logical_not(comes[quad]))
        def _():
            pltpu.make_async_copy(result.at[quad], out_ref.at[slot_of[quad]], osend.at[quad]).start()

    for quad in range(3):
        @pl.when(comes[quad])
        def _():
            result_copy(quad, slot_of[quad], holder[quad], quad).wait_send()

        @pl.when(jnp.logical_not(comes[quad]))
        def _():
            pltpu.make_async_copy(result.at[quad], out_ref.at[slot_of[quad]], osend.at[quad]).wait()
    for slot in range(3):
        ox, oy, oz, _ = homes[slot]

        @pl.when(leaves[slot])
        def _():
            result_copy(0, slot, at(ox, oy, oz), 0).wait_recv()
```

```python
import functools
import math

import jax
import jax.numpy as jnp
import numpy as np
from jax import lax
from jax.experimental import pallas as pl
from jax.experimental.pallas import tpu as pltpu
from jax.sharding import PartitionSpec as P

C_SPEED = 2.5
CFL_STEP = 0.12
MESH = pl.DeviceIdType.MESH
HIGHEST = lax.Precision.HIGHEST

ARRAYS = range(6)
TWIN = tuple(k ^ 1 for k in ARRAYS)
ACROSS = (2, 4, 0, 5, 1, 3)
PRIMARY = (0, 2, 4)
STRIPS = ((2, 4), (0, 5), (1, 3))
STRIP_PLACE = {k: (axis, n) for axis, pair in enumerate(STRIPS) for n, k in enumerate(pair)}
CORNERS = {1: (0, 1, 1), 3: (1, 0, 1), 4: (1, 1, 0)}

SIZE = 128
TILES = 16
PITCH = SIZE + 48
CENTRE = 7
EDGE = 10
BLOCK_STEPS = 10
FIRST, SECOND, THIRD = GROUPS = ((0, 2), (1, 3), (5, 4))


def row_idx(row):
    return TILES * (row % 8) + row // 8


def lane_group(b):
    half = (b + 1) // 2
    return np.where(b > 2 * CENTRE, b, CENTRE - half + 2 * half * (1 - b % 2))


LANE_ORDER = tuple(int(lane_group(b)) for b in range(TILES))


def tile(i):
    return pl.ds(8 * i, 8)


def row(i, sublane=0):
    return pl.ds(8 * i + sublane, 1)


def tiles_of(arr):
    return jnp.split(arr, arr.shape[0] // 8)


def join(tiles):
    return jnp.concatenate(tiles)


def roll_rows(tile, shift):
    return pltpu.roll(tile, shift % 8, 0)


def turn(arr):
    tiles = tiles_of(arr)
    turned = tiles_of(join([tiles[i] for i in LANE_ORDER]).T)
    return join([turned[LANE_ORDER.index(i)] for i in range(TILES)])


def solution(mesh):
    axis_names = mesh.axis_names

    def local_run(tracer, wind_a, wind_b, wind_scale):
        own = tracer.shape[1]
        cells = 2 * own
        steps = wind_scale.shape[0]
        dalpha = 0.5 * math.pi / cells
        place = np.arange(SIZE)
        lane_idx = TILES * (place % 8) + lane_group(place // 8)
        tan_a = np.tan((row_idx(place) + 0.5) * dalpha - 0.25 * math.pi)[:, None]
        tan_b = np.tan((lane_idx + 0.5) * dalpha - 0.25 * math.pi)[None, :]
        r_sq = 1.0 + tan_a * tan_a + tan_b * tan_b
        inv_sqrt_g = r_sq * np.sqrt(r_sq) / ((1.0 + tan_a * tan_a) * (1.0 + tan_b * tan_b))
        gain = (0.5 * C_SPEED * CFL_STEP * inv_sqrt_g).astype(np.float32)
        out = pl.pallas_call(
            functools.partial(kernel, own, steps, axis_names),
            out_shape=jax.ShapeDtypeStruct(tracer.shape, jnp.float32),
            in_specs=[pl.BlockSpec(memory_space=pl.ANY)] * 5,
            out_specs=pl.BlockSpec(memory_space=pl.ANY),
            scratch_shapes=[
                pltpu.SMEM((steps,), jnp.float32),
                pltpu.VMEM((3, 3, own, own), jnp.float32),
                pltpu.VMEM((6, PITCH, SIZE), jnp.float32),
                pltpu.VMEM((6, PITCH, SIZE), jnp.float32),
                pltpu.VMEM((BLOCK_STEPS, 6, SIZE, SIZE), jnp.float32),
                pltpu.VMEM((6, SIZE, SIZE), jnp.float32),
                pltpu.VMEM((6, 8, SIZE), jnp.float32),
                pltpu.VMEM((4, SIZE, SIZE), jnp.float32),
                pltpu.VMEM((3, 3, own, own), jnp.float32),
                pltpu.VMEM((3, own, own), jnp.float32),
                pltpu.VMEM((3, 6, 40, SIZE), jnp.float32),
                pltpu.VMEM((4, 6, 40, SIZE), jnp.float32),
                pltpu.VMEM((3, 3, 8, SIZE), jnp.float32),
                pltpu.VMEM((4, 3, 8, SIZE), jnp.float32),
            ] + [pltpu.SemaphoreType.DMA(shape) for shape in ((4, 6), (3, 3), (3,)) for _ in range(2)] + [
                pltpu.SemaphoreType.DMA((5,)),
                pltpu.SemaphoreType.REGULAR,
            ],
            compiler_params=pltpu.CompilerParams(collective_id=0, has_side_effects=True),
            name="advect",
        )(wind_scale, tracer, wind_a, wind_b, gain)
        return out

    field_spec = P(('member', 'panel'), 'tx', 'ty')
    wind_spec = P('panel', 'tx', 'ty')
    return jax.shard_map(local_run, mesh=mesh, in_specs=(field_spec, wind_spec, wind_spec, P()),
                         out_specs=field_spec, check_vma=False)


def kernel(own, steps, axis_names, ws_in, q_in, wa_in, wb_in, gain_in, out_ref,
           ws_ref, fields, qa_rows, qb_rows, sw, wf, wlast, coef, tiles, result, send, recv, csend, crecv,
           ssem, rsem, tsend, trecv, osend, orecv, isem, second):
    tx, ty, core = lax.axis_index('tx'), lax.axis_index('ty'), lax.axis_index('panel')
    by, bz, bx = tx, ty, lax.rem(core + tx + 1, 2)
    qa, qb = (rows.at[:, pl.ds(0, SIZE)] for rows in (qa_rows, qb_rows))

    def place(kx, ky, kc):
        return {name: {'tx': kx, 'ty': ky, 'panel': kc}.get(name, 0) for name in axis_names}

    def greet(semaphore):
        for other in (1, 2, 4, 5, 6):
            near = [1 - at if other & bit else at for at, bit in ((tx, 1), (ty, 2), (core, 4))]
            pl.semaphore_signal(semaphore, inc=1, device_id=place(*near), device_id_type=MESH)

    barrier = pltpu.get_barrier_semaphore()
    greet(barrier)
    loads = [pltpu.make_async_copy(src, dst, isem.at[n]) for n, (src, dst) in enumerate((
        (wa_in, fields.at[1]), (wb_in, fields.at[2]), (q_in, fields.at[0]), (gain_in, coef.at[0]), (ws_in, ws_ref)))]
    for load in loads:
        load.start()

    def at(ox, oy, oz):
        return place(oy, oz, lax.rem(ox + oy + 1, 2))

    def pick(first, second):
        return jnp.where(core == 0, first, second)

    homes = (
        (pick(1, tx), pick(tx, 0), ty, pick(0, 1)),
        (pick(1 - tx, 1 - ty), pick(1, tx), pick(ty, 1), pick(1, 2)),
        (pick(0, ty), pick(1 - tx, tx), pick(ty, 0), pick(0, 2)),
    )
    leaves = [jnp.logical_not((ox == bx) & (oy == by) & (oz == bz)) for ox, oy, oz, _ in homes]
    flip_a = (1 - lax.rem(bx + by, 2), lax.rem(bx + by, 2), by)
    flip_b = (bz, bz, jnp.where(bz == 1, 1 - bx, bx))
    panel = (jnp.where(bx == 1, 0, 2), jnp.where(by == 1, 1, 3), jnp.where(bz == 1, 4, 5))
    holder = [place(flip_a[n], flip_b[n], panel[n] // 3) for n in range(3)]
    slot_of = [lax.rem(panel[n], 3) for n in range(3)]
    comes = [jnp.logical_not((flip_a[n] == tx) & (flip_b[n] == ty) & (panel[n] // 3 == core)) for n in range(3)]

    def tile_copy(f, slot, quad, device):
        return pltpu.make_async_remote_copy(
            fields.at[f, slot], tiles.at[f, quad], tsend.at[f, slot], trecv.at[f, quad],
            device_id=device, device_id_type=MESH)

    for load in loads:
        load.wait()
    pl.semaphore_wait(barrier, 5)
    greet(second)
    for f in (1, 2, 0):
        for slot in range(3):
            ox, oy, oz, quad = homes[slot]

            @pl.when(leaves[slot])
            def _():
                tile_copy(f, slot, quad, at(ox, oy, oz)).start()

            @pl.when(jnp.logical_not(leaves[slot]))
            def _():
                tiles[f, quad] = fields[f, slot]

    def placing(shape, spot_axis, to_idx, flip):
        dist = to_idx(lax.broadcasted_iota(jnp.int32, shape, spot_axis))
        cell = lax.broadcasted_iota(jnp.int32, shape, 1 - spot_axis)
        source = jnp.where(dist < own, jnp.where(flip == 1, own - 1 - dist, dist), -1)
        return jnp.where(source == cell, 1.0, 0.0)

    def row_to_idx(row):
        return TILES * lax.rem(row, 8) + row // 8

    def lane_to_idx(spot):
        b = spot // 8
        half = (b + 1) // 2
        group = jnp.where(b > 2 * CENTRE, b, CENTRE - half + 2 * half * (1 - lax.rem(b, 2)))
        return TILES * lax.rem(spot, 8) + group

    def dot(lhs, rhs):
        return jnp.dot(lhs, rhs, precision=HIGHEST, preferred_element_type=jnp.float32)

    PLAIN = (0, 2, 5)

    sub = lax.broadcasted_iota(jnp.int32, (8, SIZE), 0)
    lane = lax.broadcasted_iota(jnp.int32, (8, SIZE), 1)
    lane_s, lane_i = lax.rem(lane, 8), lax.rem(lane_to_idx(lane), TILES)
    edge_lane = (lane_s == 5) & (lane_i >= EDGE)
    halo_lane = (lane_s >= 6) | edge_lane

    def group_lane(group, number):
        turns = jnp.where(group < CENTRE, 2 * (CENTRE - group) - 1, 2 * (group - CENTRE))
        return 8 * jnp.where(group > 2 * CENTRE, group, turns) + number

    def mirror_lane(group, number):
        return group_lane(lax.rem(19 - group, TILES), jnp.where(group < 4, 11, EDGE) - number)

    odd_row = lax.rem(sub, 2)
    row_pair, lane_pair = sub // 2, lane_s // 2
    high, mid = lane_i >= EDGE, (lane_i >= 4) & (lane_i < EDGE)
    edge_group = jnp.where(mid, lane_i + 6, lane_i)
    at_edge = ((lane_s == 5) | (lane_s == 7)) & (high | mid)
    source_vreg = jnp.where(at_edge, jnp.where(lane_s == 7, 0, 2) + jnp.where(high, 0, 1), lane_pair)
    source_lane = jnp.where(at_edge, mirror_lane(edge_group, 5), mirror_lane(lane_i, 6 + lax.rem(lane, 2)))
    at_four = lane_s == 4
    takes_first = (odd_row == 1) & ((lane_s == 1) | (lane_s == 3) | (at_four & high))
    takes_last = (odd_row == 1) & ((lane_s == 6) | (at_four & mid))
    first_src = jnp.where(takes_first, mirror_lane(lane_i, jnp.where(at_four, 5, 6 + lane_s // 2)), 0)
    last_src = jnp.where(takes_last, mirror_lane(jnp.where(at_four, edge_group, lane_i), jnp.where(at_four, 5, 6 + sub // 4)), 0)
    low_group = lane_i - 6
    edge_back = [group_lane(lane_i, 7), group_lane(low_group, 7), group_lane(lane_i, 5), group_lane(low_group, 5)]
    msg_back = [jnp.where(lane_s >= 6, lane - 6 + 2 * j, jnp.where(edge_lane, edge_back[j], 0)) for j in range(4)]
    first_back = jnp.where(lane_s >= 6, lane + lane_s - 11, jnp.where(edge_lane, lane - 1, 0))
    last_back = jnp.where(lane_s >= 6, lane - lane_s + 6, jnp.where(edge_lane, group_lane(low_group, 4), 0))
    last_row = 1 + 2 * jnp.where((sub >= 4) & (lane_s < 7), odd_row, lax.rem(sub + 2 * (sub // 4), 4))

    def rows_by(arr, idx):
        return jnp.take_along_axis(arr, idx, axis=0, mode="promise_in_bounds")

    def lanes_by(arr, idx):
        return jnp.take_along_axis(arr, idx, axis=1, mode="promise_in_bounds")

    def by_number(number, parts):
        res = parts[0]
        for m, part in enumerate(parts):
            res = jnp.where(number == m, part, res) if m else res
        return res

    def peer(mirrored):
        return at(*(1 - b if m else b for b, m in zip((bx, by, bz), mirrored)))

    def strip_copy(axis, out, slot):
        return pltpu.make_async_remote_copy(
            send.at[out, pl.ds(2 * axis, 2)], recv.at[slot, pl.ds(2 * axis, 2)], ssem.at[slot, axis], rsem.at[slot, axis],
            device_id=peer(tuple(int(n == axis) for n in range(3))), device_id_type=MESH)

    def corner_copy(k, out, slot):
        n = k // 2
        return pltpu.make_async_remote_copy(
            csend.at[out, n], crecv.at[slot, n], ssem.at[slot, 3 + n], rsem.at[slot, 3 + n],
            device_id=peer(CORNERS[k]), device_id_type=MESH)

    def signed(sign, arr):
        return arr if sign == 1.0 else sign * arr

    def pack(arrs, k, out, sign):
        axis, n = STRIP_PLACE[k]
        a = tiles_of(arrs[k])

        def mirrored(i, sublane):
            return rows_by(a[(19 - i) % TILES], sublane)

        msg = [by_number(row_pair, [mirrored(i, (5 if i < 4 else 4) - odd_row) for i in range(4 * j, 4 * j + 4)])
               for j in range(4)]
        tail = [mirrored(i, 5 + 0 * sub) for i in range(EDGE, TILES)] + [mirrored(i, 3 + 0 * sub) for i in range(2)]
        msg = [signed(sign, part) for part in msg + [by_number(sub, tail)]]
        send[out, 2 * axis + n] = join(msg)
        return msg

    def pack_corner(k, packed, out, corner_sign):
        *msg, tail = packed
        block = by_number(source_vreg, [lanes_by(m, source_lane) for m in msg])
        first = lanes_by(rows_by(tail, row_pair), first_src)
        last = lanes_by(rows_by(tail, 4 + lax.rem(row_pair, 2)), last_src)
        block = jnp.where(takes_first, first, jnp.where(takes_last, last, block))
        csend[out, k // 2] = signed(corner_sign, block)

    def sender(arrs, out, slot, sign=1.0, corner_sign=1.0):
        packed = [pack(arrs, k, out, sign) for k in (1, 3)]
        strip_copy(2, out, slot).start()
        for k, msg in zip((1, 3), packed):
            pack_corner(k, msg, out, corner_sign)
            corner_copy(k, out, slot).start()
        yield
        for k in (0, 2):
            pack(arrs, k, out, sign)
        yield
        pack_corner(4, pack(arrs, 4, out, sign), out, corner_sign)
        corner_copy(4, out, slot).start()
        pack(arrs, 5, out, sign)
        strip_copy(1, out, slot).start()
        strip_copy(0, out, slot).start()
        yield

    def strip(k, slot):
        axis, n = STRIP_PLACE[k]
        return tiles_of(recv[slot, 2 * axis + n])

    def halo_tiles(k, slot):
        *msg, tail = strip(k, slot)
        if k in CORNERS:
            block = crecv[slot, k // 2]
            msg = [jnp.where(halo_lane, lanes_by(block, msg_back[j]), msg[j]) for j in range(4)]
            last = rows_by(lanes_by(block, last_back), last_row)
            tail = jnp.where(halo_lane, jnp.where(sub < 4, rows_by(lanes_by(block, first_back), last_row), last), tail)
        res = [roll_rows(msg[i // 4], 6 - 2 * (i % 4)) for i in range(TILES)]
        for i in range(EDGE, TILES):
            res[i] = jnp.where(sub == 5, roll_rows(tail, 15 - i), res[i])
        return res

    def wait_all(out, slot):
        for axis in (0, 1):
            strip_copy(axis, out, slot).wait()
        for k in (3, 4, 1):
            corner_copy(k, out, slot).wait()
        strip_copy(2, out, slot).wait()

    def merge(arrs, k, rows, lanes):
        side = tiles_of(lanes)
        for i in range(TILES):
            own_rows = sub < (6 if i < EDGE else 5)
            sideways = halo_lane & own_rows if k in CORNERS else halo_lane
            arrs[k, tile(i)] = jnp.where(sideways, side[i], jnp.where(own_rows, arrs[k, tile(i)], rows[i]))

    def finish(slot):
        wait_all(0, slot)
        halos = {k: halo_tiles(k, slot) for k in (0, 2, 5, 1, 3, 4)}
        lanes = {TWIN[k]: turn(join(halos[k])) for k in (0, 2, 5, 1, 3, 4)}
        for k in (*SECOND, *FIRST, 4, 5):
            merge(qa, k, halos[k], lanes[k])

    def scale_faces(first_step):
        def one(step, carry):
            scale = ws_ref[lax.rem(first_step + step, steps)]
            sw[step] = scale * wf[...]
            return carry
        lax.fori_loop(0, BLOCK_STEPS, one, 0)

    for f in (1, 2, 0):
        for slot in range(3):
            ox, oy, oz, quad = homes[slot]

            @pl.when(leaves[slot])
            def _():
                tile_copy(f, slot, quad, at(ox, oy, oz)).wait_send()
        for quad in range(3):
            @pl.when(comes[quad])
            def _():
                tile_copy(f, 0, quad, holder[quad]).wait_recv()
        for quad in range(3):
            loc = dot(dot(placing((SIZE, own), 0, row_to_idx, flip_a[quad]), tiles[f, quad]),
                      placing((own, SIZE), 1, lane_to_idx, flip_b[quad]))
            plain, turned = PLAIN[quad], TWIN[PLAIN[quad]]
            if f == 0:
                qa[plain] = loc
                qa[turned] = turn(loc)
            elif f == 1:
                loc = jnp.where(flip_a[quad] == 1, -1.0, 1.0) * loc
                qb[plain] = loc
                sw[0, turned] = turn(loc)
            else:
                loc = jnp.where(flip_b[quad] == 1, -1.0, 1.0) * loc
                sw[0, plain] = loc
                qb[turned] = turn(loc)
        if f == 2:
            pl.semaphore_wait(second, 5)
            list(sender(qb, 1, 2, sign=-1.0))
            list(sender(sw.at[0], 2, 3, corner_sign=-1.0))
    list(sender(qa, 0, 0))

    coef[1] = 1.0 - 4.0 * coef[0]
    coef[2] = 0.5 * coef[0]
    coef[3] = 0.5 - 2.0 * coef[0]

    wait_all(1, 2)
    wait_all(2, 3)
    for k in ARRAYS:
        merge(qb, k, halo_tiles(k, 2), turn(join(halo_tiles(TWIN[k], 3))))
    for k in ARRAYS:
        here = qb[k]
        scaled = 0.5 / (6.0 * C_SPEED)
        after = join([here[8:], roll_rows(here[:8], -1)])
        beyond = jnp.where(sub == 7, roll_rows(strip(k, 2)[-1], 1), after[-8:])
        wf[k] = scaled * (here + after)
        wf[k, row(15, 7)] = scaled * (here[:1] - qb[ACROSS[k], row(0)])
        wlast[k] = scaled * (here[-8:] + beyond)
    scale_faces(0)

    def x_part(a_ref, k, faces, ghosts=False, beyond=None):
        a = a_ref[k]
        first, last = a[:8], a[-8:]
        below, above = roll_rows(last, 1), roll_rows(first, -1)
        if ghosts:
            below = jnp.where(sub == 0, a_ref[ACROSS[k], tile(0)], below)
        if beyond is not None:
            above = jnp.where(sub == 7, roll_rows(beyond[0], 1), above)
        m = join([below, a[:-8]]) + join([a[8:], above])
        v = 8.0 * a - m
        v_above, here = roll_rows(v[:8], -1), faces
        if beyond is not None:
            v_above = 8.0 * above - (last + jnp.where(sub == 7, beyond[0], roll_rows(a[8:16], -1)))
            here = join([faces[:-8], beyond[1]])
        flux = here * (v + join([v[8:], v_above]))
        flux_below = roll_rows(flux[-8:], 1)
        if ghosts:
            v_below = 8.0 * below - (jnp.where(sub == 0, a_ref[ACROSS[k], tile(1)], roll_rows(a[-16:-8], 1)) + first)
            flux_below = roll_rows(faces[-8:], 1) * (v_below + v[:8])
        return (m - flux) + join([flux_below, flux[:-8]])

    def parts_of(src, dst, second, step, group, ghosts, scale, slot):
        part = {}
        for k in group:
            beyond = None if scale is None else (strip(k, slot)[-1], scale * wlast[k])
            part[k] = coef[2 if second else 0] * x_part(src, k, sw[step, k], ghosts, beyond)
            if k in PRIMARY:
                own_part = coef[3 if second else 1] * src[k]
                if second:
                    own_part = 0.5 * dst[k] + own_part
                part[k] = own_part + part[k]
        return part, {k: turn(part[k]) for k in group}

    def stage(src, dst, second, step, ghosts=False, scale=None, slot=None, sends=None):
        part, turned = {}, {}
        for group in GROUPS:
            more = parts_of(src, dst, second, step, group, ghosts, scale, slot)
            part.update(more[0])
            turned.update(more[1])
            if group is FIRST:
                for k in group:
                    dst[k] = part[k]
        new = {}
        for group in (SECOND, FIRST, THIRD):
            for k in group:
                new[k] = (dst[k] if group is FIRST else part[k]) + turned[TWIN[k]]
            for k in group:
                dst[k] = new[k]
            if sends is not None:
                next(sends)
        if sends is None and scale is None:
            for k in ARRAYS:
                near = new[ACROSS[k]]
                dst[k, row(14, 7)] = near[8:9]
                dst[k, row(15, 7)] = near[:1]

    def run_block(first_step, count, slot, sends):
        finish(slot)
        stage(qa, qb, False, 0, ghosts=True, scale=ws_ref[first_step], slot=slot)
        stage(qb, qa, True, 0, ghosts=True)

        def one_step(step, carry):
            stage(qa, qb, False, step)
            stage(qb, qa, True, step)
            return carry

        lax.fori_loop(1, count - 1, one_step, 0, unroll=True)
        stage(qa, qb, False, count - 1)
        stage(qb, qa, True, count - 1, sends=sends)

    full_blocks = (steps - 1) // BLOCK_STEPS

    def block(blk, carry):
        out_slot = lax.rem(blk + 1, 2)
        run_block(blk * BLOCK_STEPS, BLOCK_STEPS, lax.rem(blk, 2), sender(qa, 0, out_slot))
        scale_faces((blk + 1) * BLOCK_STEPS)
        return carry

    lax.fori_loop(0, full_blocks, block, 0)
    run_block(full_blocks * BLOCK_STEPS, steps - full_blocks * BLOCK_STEPS, full_blocks % 2, iter(range(3)))

    def result_copy(quad, slot, device, number):
        return pltpu.make_async_remote_copy(
            result.at[quad], out_ref.at[slot], osend.at[number], orecv.at[slot],
            device_id=device, device_id_type=MESH)

    for quad in range(3):
        result[quad] = dot(dot(placing((own, SIZE), 1, row_to_idx, flip_a[quad]), qa[PLAIN[quad]]),
                           placing((SIZE, own), 0, lane_to_idx, flip_b[quad]))

        @pl.when(comes[quad])
        def _():
            result_copy(quad, slot_of[quad], holder[quad], quad).start()

        @pl.when(jnp.logical_not(comes[quad]))
        def _():
            pltpu.make_async_copy(result.at[quad], out_ref.at[slot_of[quad]], osend.at[quad]).start()

    for quad in range(3):
        @pl.when(comes[quad])
        def _():
            result_copy(quad, slot_of[quad], holder[quad], quad).wait_send()

        @pl.when(jnp.logical_not(comes[quad]))
        def _():
            pltpu.make_async_copy(result.at[quad], out_ref.at[slot_of[quad]], osend.at[quad]).wait()
    for slot in range(3):
        ox, oy, oz, _ = homes[slot]

        @pl.when(leaves[slot])
        def _():
            result_copy(0, slot, at(ox, oy, oz), 0).wait_recv()
```
